32 devices in a mesh: gx: 4 (over y, x), gy: 4 (over z), gz: 2 (over core).
Axes of the slice: x: 2, y: 2, z: 4, core: 2. Of those that a mesh axis runs over, the one named last changes fastest.
Arguments:
- estimate: float32 [16, 256, 512], P('gz', 'gx', 'gy'), may hold values from 0.25 to 4
- view_data: float32 [16, 256, 512], P('gz', 'gx', 'gy'), may hold values from 0.25 to 4
- psf_stack: float32 [6, 31, 31, 31], replicated, may hold values from 0.01 to 1.53, as said below
- view_index: int32 [1], replicated, may hold values from 0 to 5
Outputs:
- updated_estimate: float32 [16, 256, 512], P('gz', 'gx', 'gy')
- level_one: float32 [8, 128, 256], P('gz', 'gx', 'gy')
- level_two: float32 [4, 64, 128], P('gz', 'gx', 'gy')
- level_three: float32 [2, 32, 64], P('gz', 'gx', 'gy')
- level_four: float32 [1, 16, 32], P(None, 'gx', 'gy')
- level_five: float32 [1, 8, 16], replicated
The draws below stay inside these ranges and needn't reach their ends.
Inputs may be any that keep to these rules, and one draw needn't show every extreme that they name: `psf_stack`: every entry of every view's point spread function is positive.
All inputs are finite; a program needn't handle non-finite values.
Results may differ from the reference program's by a relative error of at most 0.000075.
Values sent between devices are 32-bit elements; how exact they have to be, the bound alone decides.
No kernel may reach another device: no remote copies, remote signals or barrier semaphores. Data moves between devices by JAX's collectives and lax.ppermute only.
A program may use at most 128 MiB of HBM per device.

```python
import math
import jax
import jax.numpy as jnp
from jax import lax

HALO = 15
VIEWS = 6
NX = 256
NY = 512
NZ = 16


def draw_psf_stack(key, part):
    extent = 2 * HALO + 1
    first, second, third = jax.random.split(jax.random.fold_in(key, 7), 3)
    widths = jax.random.uniform(first, (VIEWS, 3), jnp.float32, 1.0, 4.5)
    offsets = jnp.arange(extent, dtype=jnp.float32) - HALO
    depth_term = offsets[None, :, None, None] / widths[:, 0, None, None, None]
    row_term = offsets[None, None, :, None] / widths[:, 1, None, None, None]
    column_term = offsets[None, None, None, :] / widths[:, 2, None, None, None]
    exponent = depth_term * depth_term + row_term * row_term + column_term * column_term
    roughness = jax.random.uniform(second, (VIEWS, extent, extent, extent), jnp.float32, 0.5, 1.5)
    floor_part = 0.02 * jax.random.uniform(third, (VIEWS, extent, extent, extent), jnp.float32, 0.5, 1.5)
    return jnp.exp(-0.5 * exponent) * roughness + floor_part


def levels(own_key, shape, cuts, least, high):
    def one(position, parts):
        steps = jax.random.uniform(jax.random.fold_in(jax.random.fold_in(own_key, 6), position), (parts,), jnp.float32, least / len(cuts), high / len(cuts))
        return jnp.repeat(jnp.exp(steps), shape[position] // parts).reshape((-1,) + (1,) * (len(shape) - position - 1))

    loudness = one(*cuts[0])
    for cut in cuts[1:]:
        loudness = loudness * one(*cut)
    return loudness


def setup_inputs(seed: int = 0) -> dict:
    streams_of = jax.random.split(jax.random.key(seed), 5)
    return {
        "estimate": jnp.clip(jnp.exp(math.log(4.0) - 2.7725887 * jax.random.uniform(streams_of[0], (NZ, NX, NY), jnp.float32) ** levels(streams_of[0], (NZ, NX, NY), ((0, 2), (1, 4), (2, 4)), -0.2, 0.2)), 0.25, 4.0),
        "view_data": jnp.clip(jnp.exp(math.log(4.0) - 2.7725887 * jax.random.uniform(streams_of[1], (NZ, NX, NY), jnp.float32) ** levels(streams_of[1], (NZ, NX, NY), ((0, 2), (1, 4), (2, 4)), -0.2, 0.2)), 0.25, 4.0),
        "psf_stack": draw_psf_stack(jax.random.fold_in(streams_of[4], 71), 0),
        "view_index": jax.random.randint(streams_of[3], (1,), 0, VIEWS).astype(jnp.int32),
    }


def convolve(volume, kernel):
    radius = (kernel.shape[0] - 1) // 2
    fft_sizes = tuple(((extent + 2 * radius + 15) // 16) * 16 for extent in volume.shape)
    product = jnp.fft.rfftn(volume, fft_sizes) * jnp.fft.rfftn(kernel, fft_sizes)
    full_conv = jnp.fft.irfftn(product, fft_sizes)
    plane_count, row_count, column_count = volume.shape
    return full_conv[radius:radius + plane_count, radius:radius + row_count, radius:radius + column_count].astype(jnp.float32)


def average_blocks(volume, depth):
    plane_count, row_count, column_count = volume.shape
    if depth:
        blocks = volume.reshape(plane_count // 2, 2, row_count // 2, 2, column_count // 2, 2)
        return jnp.mean(blocks, axis=(1, 3, 5))
    blocks = volume.reshape(plane_count, row_count // 2, 2, column_count // 2, 2)
    return jnp.mean(blocks, axis=(2, 4))


def reference(estimate, view_data, psf_stack, view_index):
    kernel = lax.dynamic_index_in_dim(psf_stack, view_index[0], 0, keepdims=False)
    kernel = kernel / jnp.sum(kernel)
    blurred = convolve(estimate, kernel)
    ratio_field = view_data / blurred
    correction = convolve(ratio_field, jnp.flip(kernel))
    updated = estimate * correction
    level_one = average_blocks(updated, True)
    level_two = average_blocks(level_one, True)
    level_three = average_blocks(level_two, True)
    level_four = average_blocks(level_three, True)
    level_five = average_blocks(level_four, False)
    return updated, level_one, level_two, level_three, level_four, level_five
```

```python
import functools

import jax
import jax.numpy as jnp
import ml_dtypes
import numpy as np
from jax import lax
from jax.experimental import pallas as pl
from jax.experimental.pallas import tpu as pltpu
from jax.sharding import PartitionSpec as P

F32 = jnp.float32
BF16 = jnp.bfloat16
ALL = ("gx", "gy", "gz")
VMEM_LIMIT = 40 * 1024 * 1024


def up8(count):
    return (count + 7) // 8 * 8


class Sizes:
    def __init__(self, estimate_shape, psf_shape, gx, gy):
        self.planes, self.rows, self.cols = estimate_shape
        self.extent = psf_shape[1]
        self.radius = (self.extent - 1) // 2
        self.depth = 2 * self.planes
        self.half = self.cols // 2
        self.wide = up8(2 * self.radius)
        self.near = up8(self.radius)
        self.length = self.rows + 2 * self.wide
        self.view_rows = self.rows + 2 * self.near
        self.stack_rows = self.length + self.view_rows
        self.freqs = self.cols // 2
        self.q_wide = self.cols // self.wide
        self.r_wide = self.length // self.q_wide
        self.q_near = self.cols // self.near
        self.r_near = self.view_rows * 2 // self.q_near
        self.pack_e = self.planes * self.r_wide
        self.pack_v = self.planes // 2 * self.r_near
        self.gx, self.gy = gx, gy
        assert self.half + 2 * self.wide == self.cols == 128
        assert self.wide <= self.rows and self.r_wide % 8 == 0 and self.r_near % 8 == 0
        assert self.depth == 16


def split_np(matrix):
    high = matrix.astype(np.float32).astype(ml_dtypes.bfloat16)
    low = (matrix - high.astype(np.float64)).astype(np.float32).astype(ml_dtypes.bfloat16)
    return high, low


def lane_positions(s, core):
    lanes = np.arange(s.cols)
    return (lanes + s.wide) % s.cols if core == 0 else (lanes - s.wide) % s.cols


def right_pair(matrix):
    high, low = split_np(matrix)
    return np.block([[high, low], [high, np.zeros_like(low)]])


def tables(s):
    y_freq = 2.0 * np.pi * (np.arange(s.freqs) + 0.5) / s.cols
    x_freq = 2.0 * np.pi * np.arange(s.length) / s.length
    y_forward, y_inverse = [], []
    for core in (0, 1):
        angle = lane_positions(s, core)[:, None] * y_freq[None, :]
        y_forward.append(right_pair(np.concatenate([np.cos(angle), -np.sin(angle)], 1)))
        back = np.concatenate([np.cos(angle), -np.sin(angle)], 1).T * (2.0 / s.cols / s.length)
        y_inverse.append(right_pair(back))
    offset = np.zeros(s.cols)
    offset[: s.extent] = np.arange(s.extent) - s.radius
    angle = offset[:, None] * y_freq[None, :]
    y_kernel = np.concatenate([np.cos(angle), -np.sin(angle)], 1)
    y_kernel[s.extent :] = 0.0

    def x_matrix(positions):
        angle = x_freq[:, None] * positions[None, :]
        return np.cos(angle), np.sin(angle)

    def stacked(cosine, sine):
        high, low = split_np(np.concatenate([cosine, sine], 1))
        return np.concatenate([high, low], 0)

    window = np.arange(s.length) - s.wide
    near = np.arange(s.view_rows) - s.near
    own = np.arange(s.rows)
    taps = np.arange(up8(s.extent)) - s.radius
    x_window = stacked(*x_matrix(window))
    x_near = stacked(*x_matrix(near))
    cosine, sine = x_matrix(near)
    x_back_near = stacked(cosine.T, sine.T)
    cosine, sine = x_matrix(own)
    x_back_own = stacked(cosine.T, sine.T)
    high, low = split_np(np.concatenate(x_matrix(taps), 1))
    x_kernel = np.concatenate([high, low, high], 1)
    return dict(
        y_forward=np.stack(y_forward),
        y_inverse=np.stack(y_inverse),
        y_kernel=right_pair(y_kernel),
        x_window=x_window,
        x_near=x_near,
        x_back_near=x_back_near,
        x_back_own=x_back_own,
        x_kernel=x_kernel,
    )


def split(x):
    high = x.astype(BF16)
    return high, (x - high.astype(F32)).astype(BF16)


def dot(a, b):
    return lax.dot_general(a, b, (((1,), (0,)), ((), ())), preferred_element_type=F32)


def lane_iota(rows, cols):
    return lax.broadcasted_iota(jnp.int32, (rows, cols), 1)


def turn(x, shift):
    shift %= x.shape[1]
    return pltpu.roll(x, shift, 1) if shift else x


def times_right(x, pair):
    width = x.shape[1]
    both = dot(jnp.concatenate(split(x), 1), pair)
    return both[:, :width] + both[:, width:]


def times_left(matrix, x):
    count = matrix.shape[0] // 2
    high, low = split(x)
    both = dot(matrix, high)
    return both[:count] + both[count:] + dot(matrix[:count], low)


def quarter_turn(x, sign):
    half = x.shape[1] // 2
    lanes = lane_iota(*x.shape)
    moved = turn(x, half)
    return jnp.where((lanes < half) == (sign > 0), moved, -moved)


def pack_kernel(s, where_ref, e_ref, v_ref, below_ref, above_ref, stack_ref, same_ref, other_ref):
    w, n, length = s.wide, s.near, s.length
    stack_ref[:, :w] = below_ref[:, :w]
    stack_ref[:, w : w + s.rows] = e_ref[...]
    stack_ref[:, w + s.rows : length] = above_ref[:, :w]
    stack_ref[:, length : length + n] = below_ref[:, w:]
    stack_ref[:, length + n : length + n + s.rows] = v_ref[...]
    stack_ref[:, length + n + s.rows :] = above_ref[:, w:]
    first_core = where_ref[1] == 0

    def put(start, count, last, first):
        same_ref[pl.ds(start, count)] = jnp.where(first_core, last, first)
        other_ref[pl.ds(start, count)] = jnp.where(first_core, first, last)

    group = lane_iota(s.r_wide, s.cols) // w
    for z in range(s.planes):
        last = first = jnp.zeros((s.r_wide, s.cols), F32)
        for q in range(s.q_wide):
            moved = turn(stack_ref[z, q * s.r_wide : (q + 1) * s.r_wide], q * w)
            last = jnp.where(group == (q - 1) % s.q_wide, moved, last)
            first = jnp.where(group == q, moved, first)
        put(z * s.r_wide, s.r_wide, last, first)
    group = lane_iota(s.r_near, s.cols) // n
    per_plane = s.q_near // 2
    for low in range(s.planes // 2):
        last = first = jnp.zeros((s.r_near, s.cols), F32)
        for j in range(s.q_near):
            plane = j // per_plane * (s.planes // 2) + low
            start = length + j % per_plane * s.r_near
            moved = turn(stack_ref[plane, start : start + s.r_near], j * n)
            last = jnp.where(group == (j - 1) % s.q_near, moved, last)
            first = jnp.where(group == j, moved, first)
        put(s.pack_e + low * s.r_near, s.r_near, last, first)


def kernel_spectrum(s, where_ref, psf_ref, y_ref, x_ref, k1_ref, k2_ref, pad_ref, a_ref):
    taps = up8(s.extent)
    pad_ref[...] = jnp.zeros_like(pad_ref)
    total = jnp.zeros((s.extent, s.extent), F32)
    for a in range(s.extent):
        total = total + psf_ref[0, a]
    total = jnp.sum(total)
    for a in range(s.extent):
        pad_ref[a * taps : a * taps + s.extent, : s.extent] = psf_ref[0, a] / total
    a_ref[...] = times_right(pad_ref[...], y_ref[...])
    lanes = lane_iota(s.length, s.cols)
    half = s.cols // 2
    for pair in range((s.extent + 1) // 2):
        one = a_ref[2 * pair * taps : (2 * pair + 1) * taps]
        two = a_ref[(2 * pair + 1) * taps : (2 * pair + 2) * taps]
        right = jnp.concatenate(
            [
                jnp.concatenate([one, two], 1),
                jnp.concatenate([quarter_turn(one, 1), quarter_turn(two, 1)], 1),
            ],
            0,
        )
        high, low = split(right)
        out = dot(x_ref[...], jnp.concatenate([high, high, low], 0))
        for side in (0, 1):
            a = 2 * pair + side
            if a < s.extent:
                value = out[:, side * s.cols : (side + 1) * s.cols]
                moved = turn(value, half)
                k1_ref[a] = jnp.where(lanes < half, value, moved)
                k2_ref[a] = jnp.where(lanes < half, -moved, value)


def main_kernel(
    s,
    where_ref,
    own_ref,
    partner_ref,
    same_ref,
    other_ref,
    k1_ref,
    k2_ref,
    yf_ref,
    yi_ref,
    xw_ref,
    xn_ref,
    xbn_ref,
    xbo_ref,
    mine_ref,
    theirs_ref,
    five_ref,
    e_ref,
    v_ref,
    x1_ref,
    x2_ref,
    p_ref,
    u_ref,
    t_ref,
):
    core, gx, gy = where_ref[1], where_ref[2], where_ref[3]
    half = s.cols // 2
    depth = s.depth
    for source_ref, halo_ref, base in (
        (own_ref, same_ref, core * s.planes),
        (partner_ref, other_ref, (1 - core) * s.planes),
    ):
        lanes = lane_iota(s.r_wide, s.cols)
        from_halo = jnp.where(core == 0, lanes - (s.cols - s.wide), s.wide - 1 - lanes) >= 0
        for z in range(s.planes):
            packed = halo_ref[z * s.r_wide : (z + 1) * s.r_wide]
            for q in range(s.q_wide):
                rows = slice(q * s.r_wide, (q + 1) * s.r_wide)
                e_ref[base + z, rows] = jnp.where(from_halo, turn(packed, -q * s.wide), source_ref[z, rows])
        lanes = lane_iota(s.r_near, s.cols)
        from_halo = jnp.where(core == 0, lanes - (s.cols - s.near), s.near - 1 - lanes) >= 0
        per_plane = s.q_near // 2
        for low in range(s.planes // 2):
            packed = halo_ref[s.pack_e + low * s.r_near : s.pack_e + (low + 1) * s.r_near]
            for j in range(s.q_near):
                plane = j // per_plane * (s.planes // 2) + low
                start = j % per_plane * s.r_near
                v_ref[base + plane, start : start + s.r_near] = jnp.where(
                    from_halo,
                    turn(packed, -j * s.near),
                    source_ref[plane, s.length + start : s.length + start + s.r_near],
                )

    def forward(load, x_table, sign):
        for pair in range(depth // 2):
            parts = [times_right(load(2 * pair + side), yf_ref[0]) for side in (0, 1)]
            right = jnp.concatenate(
                [
                    jnp.concatenate(parts, 1),
                    jnp.concatenate([quarter_turn(part, 1) for part in parts], 1),
                ],
                0,
            )
            out = times_left(x_table[...], right)
            for side in (0, 1):
                value = out[:, side * s.cols : (side + 1) * s.cols]
                moved = turn(value, half)
                x1_ref[2 * pair + side] = value
                x2_ref[2 * pair + side] = moved if sign > 0 else -moved

    def along_z(flip):
        block = 4

        def tile(t, carry):
            rows = pl.ds(t * 8, 8)
            ones = [x1_ref[z, rows] for z in range(depth)]
            twos = [x2_ref[z, rows] for z in range(depth)]
            for start in range(0, depth, block):
                sums = [None] * block
                for d in range(2 * depth - 1):
                    hits = []
                    for k in range(block):
                        zi = start + k + (d - (depth - 1)) * (1 if flip else -1)
                        if 0 <= zi < depth:
                            hits.append((k, zi))
                    if not hits:
                        continue
                    tap = d - (depth - 1) + s.radius
                    k1, k2 = k1_ref[tap, rows], k2_ref[tap, rows]
                    for k, zi in hits:
                        term = k1 * ones[zi] + k2 * twos[zi]
                        sums[k] = term if sums[k] is None else sums[k] + term
                for k in range(block):
                    p_ref[start + k, rows] = sums[k]
            return carry

        lax.fori_loop(0, s.length // 8, tile, 0)

    def backward(x_table, use):
        for pair in range(depth // 2):
            parts = [p_ref[2 * pair + side] for side in (0, 1)]
            right = jnp.concatenate(
                [
                    jnp.concatenate(parts, 1),
                    jnp.concatenate([quarter_turn(part, -1) for part in parts], 1),
                ],
                0,
            )
            out = times_left(x_table[...], right)
            for side in (0, 1):
                use(2 * pair + side, times_right(out[:, side * s.cols : (side + 1) * s.cols], yi_ref[0]))

    forward(lambda z: e_ref[z], xw_ref, 1)
    along_z(False)

    shape = (s.view_rows, s.cols)
    row = lax.broadcasted_iota(jnp.int32, shape, 0) - s.near
    lane = lane_iota(*shape)
    column = lane + jnp.where(core == 0, jnp.where(lane < s.cols - s.near, 0, -s.cols), jnp.where(lane < s.near, s.cols, 0))
    first_row, last_row = -gx * s.rows, (s.gx - gx) * s.rows
    first_column, last_column = -gy * s.cols, (s.gy - gy) * s.cols
    inside = (row >= first_row) & (row < last_row) & (column >= first_column) & (column < last_column)
    begin = core * half - s.near
    inside = inside & (column >= begin) & (column < begin + half + 2 * s.near)

    def to_ratio(z, blurred):
        safe = jnp.where(inside, blurred, 1.0)
        v_ref[z] = jnp.where(inside, v_ref[z] / safe, 0.0)

    backward(xbn_ref, to_ratio)
    forward(lambda z: v_ref[z], xn_ref, -1)
    along_z(True)

    lane = lane_iota(s.rows, s.cols)
    owned = (lane // half) == core

    def to_update(z, correction):
        u_ref[z] = jnp.where(owned, e_ref[z, s.wide : s.wide + s.rows] * correction, 0.0)

    backward(xbo_ref, to_update)

    def pooled(x, factor, scale):
        count = s.cols // factor
        weights = jnp.where(
            lax.broadcasted_iota(jnp.int32, (s.cols, count), 0) // factor
            == lax.broadcasted_iota(jnp.int32, (s.cols, count), 1),
            scale,
            0.0,
        ).astype(BF16)
        high, rest = split(x)
        middle = x - high.astype(F32)
        low = (middle - rest.astype(F32)).astype(BF16)
        return dot(high, weights) + dot(rest, weights) + dot(low, weights)

    u_rows = s.planes * s.rows
    source = u_ref
    planes, rows, start = depth, s.rows, u_rows
    levels = []
    for level in (1, 2, 3, 4):
        planes, rows = planes // 2, rows // 2
        here = t_ref.at[level - 1]
        for z in range(planes):
            here[z, : 2 * rows] = source[2 * z, : 2 * rows] + source[2 * z + 1, : 2 * rows]
        sums = [
            here[z, pl.ds(0, rows, stride=2)] + here[z, pl.ds(1, rows, stride=2)] for z in range(planes)
        ]
        for z in range(planes):
            here[z, :rows] = sums[z]
        factor = 2**level
        value = pooled(jnp.concatenate(sums, 0), factor, 1.0 / factor**3)
        levels.append((value, planes, rows, s.cols // factor))
        source = here
    for half_index in (0, 1):
        for mine, out_ref in ((True, mine_ref), (False, theirs_ref)):

            @pl.when((core == half_index) == mine)
            def _():
                for z in range(s.planes):
                    out_ref[z * s.rows : (z + 1) * s.rows] = u_ref[half_index * s.planes + z]
                start = u_rows
                for value, planes, rows, columns in levels:
                    count = max(planes * rows // 2, rows)
                    begin = half_index * count if planes > 1 else 0
                    out_ref[start : start + count, :columns] = value[begin : begin + count]
                    start += up8(count)
    top = sums[0]
    rows5, columns5 = five_ref.shape[1:]
    own_rows = top.shape[0] // 2
    row = lax.broadcasted_iota(jnp.int32, (rows5, s.cols), 0)
    spread = jnp.zeros((rows5, s.cols), F32)
    for i in range(own_rows):
        spread = jnp.where(row == gx * own_rows + i, top[2 * i : 2 * i + 1] + top[2 * i + 1 : 2 * i + 2], spread)
    factor = 32
    per_chip = s.cols // factor
    weights = jnp.where(
        lax.broadcasted_iota(jnp.int32, (s.cols, columns5), 0) // factor + gy * per_chip
        == lax.broadcasted_iota(jnp.int32, (s.cols, columns5), 1),
        1.0 / (factor * factor * depth),
        0.0,
    ).astype(BF16)
    high, rest = split(spread)
    low = (spread - high.astype(F32) - rest.astype(F32)).astype(BF16)
    five = dot(high, weights) + dot(rest, weights) + dot(low, weights)
    for k in range(five_ref.shape[0]):
        five_ref[k] = five


def last_kernel(s, mine_ref, got_ref, fives_ref, u_ref, one_ref, two_ref, three_ref, four_ref, five_ref):
    for z in range(s.planes):
        part = slice(z * s.rows, (z + 1) * s.rows)
        u_ref[z] = mine_ref[part] + got_ref[part]
    start = s.planes * s.rows
    for out_ref in (one_ref, two_ref, three_ref, four_ref):
        planes, rows, columns = out_ref.shape
        for z in range(planes):
            part = slice(start + z * rows, start + (z + 1) * rows)
            out_ref[z] = mine_ref[part, :columns] + got_ref[part, :columns]
        start += up8(planes * rows)
    total = fives_ref[0]
    for k in range(1, fives_ref.shape[0]):
        total = total + fives_ref[k]
    five_ref[0] = total


def whole(shape):
    return pl.BlockSpec(shape, lambda *_: (0,) * len(shape))


def call(body, where, arrays, in_specs, outs, scratch=(), name=None):
    grid_spec = pltpu.PrefetchScalarGridSpec(
        num_scalar_prefetch=1,
        grid=(1,),
        in_specs=in_specs,
        out_specs=[whole(shape) for shape in outs],
        scratch_shapes=[pltpu.VMEM(shape, F32) for shape in scratch],
    )
    return pl.pallas_call(
        body,
        grid_spec=grid_spec,
        out_shape=[jax.ShapeDtypeStruct(shape, F32) for shape in outs],
        compiler_params=pltpu.CompilerParams(vmem_limit_bytes=VMEM_LIMIT),
        name=name,
    )(where, *arrays)


def shift(axis, step):
    count = lax.axis_size(axis)
    return [(i, i + step) for i in range(count) if 0 <= i + step < count]


def to_side(same):
    pairs = []
    for h in range(lax.axis_size("gy")):
        sender_up, sender_down = (0, 1) if same else (1, 0)
        if h + 1 < lax.axis_size("gy"):
            pairs.append((2 * h + sender_up, 2 * (h + 1)))
        if h > 0:
            pairs.append((2 * h + sender_down, 2 * (h - 1) + 1))
    return pairs


def local(estimate, view_data, psf_stack, view_index):
    assert lax.axis_size("gz") == 2
    gx, gy = lax.axis_size("gx"), lax.axis_size("gy")
    s = Sizes(estimate.shape, psf_stack.shape, gx, gy)
    t = {key: jnp.asarray(value) for key, value in tables(s).items()}
    where = jnp.stack(
        [view_index[0], lax.axis_index("gz"), lax.axis_index("gx"), lax.axis_index("gy")]
    ).astype(jnp.int32)

    below = lax.ppermute(
        jnp.concatenate([estimate[:, s.rows - s.wide :], view_data[:, s.rows - s.near :]], 1), "gx", shift("gx", 1)
    )
    above = lax.ppermute(
        jnp.concatenate([estimate[:, : s.wide], view_data[:, : s.near]], 1), "gx", shift("gx", -1)
    )
    psf_shape = (1,) + psf_stack.shape[1:]
    taps = up8(s.extent)
    k1, k2 = call(
        functools.partial(kernel_spectrum, s),
        where,
        (psf_stack, t["y_kernel"], t["x_kernel"]),
        [pl.BlockSpec(psf_shape, lambda i, w: (w[0], 0, 0, 0)), whole(t["y_kernel"].shape), whole(t["x_kernel"].shape)],
        [(s.extent, s.length, s.cols)] * 2,
        scratch=[((s.extent + 1) // 2 * 2 * taps, s.cols)] * 2,
        name="kernel_spectrum",
    )
    stack_shape = (s.planes, s.stack_rows, s.cols)
    slab_shape = (s.pack_e + s.pack_v, s.cols)
    arrays = (estimate, view_data, below, above)
    stack, same, other = call(
        functools.partial(pack_kernel, s),
        where,
        arrays,
        [whole(a.shape) for a in arrays],
        [stack_shape, slab_shape, slab_shape],
        name="pack",
    )
    partner = lax.ppermute(stack, "gz", [(0, 1), (1, 0)])
    same = lax.ppermute(same, ("gy", "gz"), to_side(True))
    other = lax.ppermute(other, ("gy", "gz"), to_side(False))

    u_rows = s.planes * s.rows
    out_rows = u_rows
    level_shapes = []
    planes, rows, columns = s.depth, s.rows, s.cols
    for _ in range(4):
        planes, rows, columns = planes // 2, rows // 2, columns // 2
        level_shapes.append((max(planes // 2, 1), rows, columns))
        out_rows += up8(level_shapes[-1][0] * rows)
    devices = 2 * gx * gy
    five_shape = (rows // 2 * gx, columns // 2 * gy)
    arrays = (
        stack,
        partner,
        same,
        other,
        k1,
        k2,
        t["y_forward"],
        t["y_inverse"],
        t["x_window"],
        t["x_near"],
        t["x_back_near"],
        t["x_back_own"],
    )
    specs = [whole(a.shape) for a in arrays]
    for k in (6, 7):
        specs[k] = pl.BlockSpec((1,) + arrays[k].shape[1:], lambda i, w: (w[1], 0, 0))
    spectrum = (s.depth, s.length, s.cols)
    mine, theirs, five = call(
        functools.partial(main_kernel, s),
        where,
        arrays,
        specs,
        [(out_rows, s.cols), (out_rows, s.cols), (devices,) + five_shape],
        scratch=[
            spectrum,
            (s.depth, s.view_rows, s.cols),
            spectrum,
            spectrum,
            spectrum,
            (s.depth, s.rows, s.cols),
            (4, s.depth // 2, s.rows, s.cols),
        ],
        name="update",
    )
    got = lax.ppermute(theirs, "gz", [(0, 1), (1, 0)])
    fives = lax.all_to_all(five, ALL, split_axis=0, concat_axis=0, tiled=True)
    outs = [estimate.shape] + level_shapes + [(1,) + five_shape]
    arrays = (mine, got, fives)
    return tuple(
        pl.pallas_call(
            functools.partial(last_kernel, s),
            in_specs=[whole(a.shape) for a in arrays],
            out_specs=[whole(shape) for shape in outs],
            out_shape=[jax.ShapeDtypeStruct(shape, F32) for shape in outs],
            grid=(1,),
            compiler_params=pltpu.CompilerParams(vmem_limit_bytes=VMEM_LIMIT),
            name="assemble",
        )(*arrays)
    )


def solution(mesh):
    return jax.shard_map(
        local,
        mesh=mesh,
        in_specs=(P("gz", "gx", "gy"), P("gz", "gx", "gy"), P(), P()),
        out_specs=(
            P("gz", "gx", "gy"),
            P("gz", "gx", "gy"),
            P("gz", "gx", "gy"),
            P("gz", "gx", "gy"),
            P(None, "gx", "gy"),
            P(),
        ),
        check_vma=False,
    )
```

```python
import functools

import jax
import jax.numpy as jnp
import ml_dtypes
import numpy as np
from jax import lax
from jax.experimental import pallas as pl
from jax.experimental.pallas import tpu as pltpu
from jax.sharding import PartitionSpec as P

F32 = jnp.float32
BF16 = jnp.bfloat16
ALL = ("gx", "gy", "gz")
MIB = 1024 * 1024


def up8(count):
    return (count + 7) // 8 * 8


class Sizes:
    def __init__(self, estimate_shape, psf_shape, gx, gy):
        self.planes, self.rows, self.cols = estimate_shape
        self.extent = psf_shape[1]
        self.radius = (self.extent - 1) // 2
        self.depth = 2 * self.planes
        self.half = self.cols // 2
        self.wide = up8(2 * self.radius)
        self.near = up8(self.radius)
        self.length = self.rows + 2 * self.wide
        self.view_rows = self.rows + 2 * self.near
        self.stack_rows = self.length + self.view_rows
        self.freqs = self.cols // 2
        self.q_wide = self.cols // self.wide
        self.r_wide = self.length // self.q_wide
        self.q_near = self.cols // self.near
        self.r_near = self.view_rows * 2 // self.q_near
        self.pack_e = self.planes * self.r_wide
        self.pack_v = self.planes // 2 * self.r_near
        self.gx, self.gy = gx, gy
        assert self.half + 2 * self.wide == self.cols == 128
        assert self.wide <= self.rows and self.r_wide % 8 == 0 and self.r_near % 8 == 0
        assert self.depth == 16


def split_np(matrix):
    high = matrix.astype(np.float32).astype(ml_dtypes.bfloat16)
    low = (matrix - high.astype(np.float64)).astype(np.float32).astype(ml_dtypes.bfloat16)
    return high, low


def lane_positions(s, core):
    lanes = np.arange(s.cols)
    return (lanes + s.wide) % s.cols if core == 0 else (lanes - s.wide) % s.cols


def right_pair(matrix):
    high, low = split_np(matrix)
    return np.block([[high, low], [high, np.zeros_like(low)]])


def tables(s):
    y_freq = 2.0 * np.pi * (np.arange(s.freqs) + 0.5) / s.cols
    x_freq = 2.0 * np.pi * np.arange(s.length) / s.length
    y_forward, y_inverse = [], []
    for core in (0, 1):
        angle = lane_positions(s, core)[:, None] * y_freq[None, :]
        y_forward.append(right_pair(np.concatenate([np.cos(angle), -np.sin(angle)], 1)))
        back = np.concatenate([np.cos(angle), -np.sin(angle)], 1).T * (2.0 / s.cols / s.length)
        y_inverse.append(right_pair(back))
    offset = np.zeros(s.cols)
    offset[: s.extent] = np.arange(s.extent) - s.radius
    angle = offset[:, None] * y_freq[None, :]
    y_kernel = np.concatenate([np.cos(angle), -np.sin(angle)], 1)
    y_kernel[s.extent :] = 0.0

    def x_matrix(positions):
        angle = x_freq[:, None] * positions[None, :]
        return np.cos(angle), np.sin(angle)

    def stacked(cosine, sine):
        high, low = split_np(np.concatenate([cosine, sine], 0))
        return np.concatenate([high, high, low], 1)

    window = np.arange(s.length) - s.wide
    near = np.arange(s.view_rows) - s.near
    own = np.arange(s.rows)
    taps = np.arange(up8(s.extent)) - s.radius
    x_window = stacked(*x_matrix(window))
    x_near = stacked(*x_matrix(near))
    cosine, sine = x_matrix(near)
    x_back_near = stacked(cosine.T, sine.T)
    cosine, sine = x_matrix(own)
    x_back_own = stacked(cosine.T, sine.T)
    high, low = split_np(np.concatenate(x_matrix(taps), 1))
    x_kernel = np.concatenate([high, low, high], 1)
    return dict(
        y_forward=np.stack(y_forward),
        y_inverse=np.stack(y_inverse),
        y_kernel=right_pair(y_kernel),
        x_window=x_window,
        x_near=x_near,
        x_back_near=x_back_near,
        x_back_own=x_back_own,
        x_kernel=x_kernel,
    )


def split(x):
    high = x.astype(BF16)
    return high, (x - high.astype(F32)).astype(BF16)


def dot(a, b):
    return lax.dot_general(a, b, (((1,), (0,)), ((), ())), preferred_element_type=F32)


def lane_iota(rows, cols):
    return lax.broadcasted_iota(jnp.int32, (rows, cols), 1)


def turn(x, shift):
    shift %= x.shape[1]
    return pltpu.roll(x, shift, 1) if shift else x


def wide_split(x):
    return jnp.concatenate(split(x), 1)


def fold(both):
    width = both.shape[1] // 2
    return both[:, :width] + both[:, width:]


def signs(rows, cols, left):
    return jnp.where(lane_iota(rows, cols) < cols // 2, left, -left).astype(F32)


def quarter_turn(x, sign):
    half = x.shape[1] // 2
    lanes = lane_iota(*x.shape)
    moved = turn(x, half)
    return jnp.where((lanes < half) == (sign > 0), moved, -moved)


def send_kernel(s, e_in, v_in, e_ref, v_ref, up_ref, down_ref, sem_ref):
    moves = [
        pltpu.make_async_copy(e_in, e_ref, sem_ref.at[0]),
        pltpu.make_async_copy(v_in, v_ref, sem_ref.at[1]),
    ]
    for move in moves:
        move.start()
    for move in moves:
        move.wait()
    up_ref[:, : s.wide] = e_ref[:, s.rows - s.wide :]
    up_ref[:, s.wide :] = v_ref[:, s.rows - s.near :]
    down_ref[:, : s.wide] = e_ref[:, : s.wide]
    down_ref[:, s.wide :] = v_ref[:, : s.near]


def pack_kernel(s, where_ref, e_ref, v_ref, below_ref, above_ref, k_ref, stack_ref, same_ref, other_ref):
    w, n, length = s.wide, s.near, s.length
    stack_ref[:, :w] = below_ref[:, :w]
    stack_ref[:, w : w + s.rows] = e_ref[...]
    stack_ref[:, w + s.rows : length] = above_ref[:, :w]
    stack_ref[:, length : length + n] = below_ref[:, w:]
    stack_ref[:, length + n : length + n + s.rows] = v_ref[...]
    stack_ref[:, length + n + s.rows :] = above_ref[:, w:]
    first_core = where_ref[1] == 0

    def put(start, count, last, first):
        same_ref[pl.ds(start, count)] = jnp.where(first_core, last, first)
        other_ref[pl.ds(start, count)] = jnp.where(first_core, first, last)

    group = lane_iota(s.r_wide, s.cols) // w
    for z in range(s.planes):
        last = first = jnp.zeros((s.r_wide, s.cols), F32)
        for q in range(s.q_wide):
            moved = turn(stack_ref[z, q * s.r_wide : (q + 1) * s.r_wide], q * w)
            last = jnp.where(group == (q - 1) % s.q_wide, moved, last)
            first = jnp.where(group == q, moved, first)
        put(z * s.r_wide, s.r_wide, last, first)
    group = lane_iota(s.r_near, s.cols) // n
    per_plane = s.q_near // 2
    for low in range(s.planes // 2):
        last = first = jnp.zeros((s.r_near, s.cols), F32)
        for j in range(s.q_near):
            plane = j // per_plane * (s.planes // 2) + low
            start = length + j % per_plane * s.r_near
            moved = turn(stack_ref[plane, start : start + s.r_near], j * n)
            last = jnp.where(group == (j - 1) % s.q_near, moved, last)
            first = jnp.where(group == j, moved, first)
        put(s.pack_e + low * s.r_near, s.r_near, last, first)


def toeplitz_parts(taps, size):
    half = size // 2
    middle = size - 1
    parts = [[], [], []]
    for d in range(-half + 1, half):
        centre = taps[middle + d]
        parts[0].append(centre)
        for part, other in ((1, taps[middle + d - half]), (2, taps[middle + d + half])):
            parts[part].append([other, centre])
    return parts


def combine(load, expression):
    if isinstance(expression, int):
        return load(expression)
    return combine(load, expression[0]) - combine(load, expression[1])


def leaves(s):
    found = []
    first = s.radius - (s.depth - 1)
    for part in toeplitz_parts(list(range(first, first + 2 * s.depth - 1)), s.depth):
        found += toeplitz_parts(part, s.depth // 2)
    return found


def kernel_spectrum(
    s, where_ref, psf_in, y_in, x_in, k1_ref, k2_ref, pad_ref, a_ref, k_ref, psf_ref, y_ref, x_ref, sem_ref
):
    taps = up8(s.extent)
    moves = [
        pltpu.make_async_copy(psf_in.at[pl.ds(where_ref[0], 1)], psf_ref, sem_ref.at[0]),
        pltpu.make_async_copy(y_in, y_ref, sem_ref.at[1]),
        pltpu.make_async_copy(x_in, x_ref, sem_ref.at[2]),
    ]
    for move in moves:
        move.start()
    pad_ref[...] = jnp.zeros_like(pad_ref)
    for move in moves:
        move.wait()
    total = jnp.zeros((s.extent, s.extent), F32)
    for a in range(s.extent):
        total = total + psf_ref[0, a]
    total = jnp.sum(total)
    for a in range(s.extent):
        pad_ref[a * taps : a * taps + s.extent, : s.extent] = psf_ref[0, a] / total
    a_ref[...] = fold(dot(wide_split(pad_ref[...]), y_ref[...]))
    for pair in range((s.extent + 1) // 2):
        one = a_ref[2 * pair * taps : (2 * pair + 1) * taps]
        two = a_ref[(2 * pair + 1) * taps : (2 * pair + 2) * taps]
        right = jnp.concatenate(
            [
                jnp.concatenate([one, two], 1),
                jnp.concatenate([quarter_turn(one, 1), quarter_turn(two, 1)], 1),
            ],
            0,
        )
        high, low = split(right)
        out = dot(x_ref[...], jnp.concatenate([high, high, low], 0))
        for side in (0, 1):
            if 2 * pair + side < s.extent:
                k_ref[2 * pair + side] = out[:, side * s.cols : (side + 1) * s.cols]
    per_leaf = s.depth // 2 - 1
    lanes = lane_iota(8, s.cols)
    half = s.cols // 2

    def tile(t, carry):
        rows = pl.ds(t * 8, 8)
        planes = {}

        def load(a):
            if a not in planes:
                planes[a] = k_ref[a, rows]
            return planes[a]

        for leaf, diagonals in enumerate(leaves(s)):
            for d, expression in enumerate(diagonals):
                value = combine(load, expression)
                moved = turn(value, half)
                k1_ref[leaf * per_leaf + d, rows] = jnp.where(lanes < half, value, moved)
                k2_ref[leaf * per_leaf + d, rows] = jnp.where(lanes < half, -moved, value)
        return carry

    lax.fori_loop(0, s.length // 8, tile, 0)


def main_kernel(
    s,
    where_ref,
    own_ref,
    partner_ref,
    same_ref,
    other_ref,
    k1_ref,
    k2_ref,
    yf_ref,
    yi_ref,
    xw_ref,
    xn_ref,
    xbn_ref,
    xbo_ref,
    mine_ref,
    theirs_ref,
    five_ref,
    e_ref,
    v_ref,
    x1_ref,
    x2_ref,
    p_ref,
    u_ref,
    t_ref,
    l_ref,
    a_ref,
    b_ref,
):
    core, gx, gy = where_ref[1], where_ref[2], where_ref[3]
    half = s.cols // 2
    depth = s.depth
    group = 4
    for source_ref, halo_ref, base in (
        (own_ref, same_ref, core * s.planes),
        (partner_ref, other_ref, (1 - core) * s.planes),
    ):
        lanes = lane_iota(s.r_wide, s.cols)
        from_halo = jnp.where(core == 0, lanes - (s.cols - s.wide), s.wide - 1 - lanes) >= 0
        for z in range(s.planes):
            packed = halo_ref[z * s.r_wide : (z + 1) * s.r_wide]
            for q in range(s.q_wide):
                first = q * s.r_wide
                rows = slice(first, first + s.r_wide)
                value = jnp.where(from_halo, turn(packed, -q * s.wide), source_ref[z, rows])
                l_ref[base + z, rows] = wide_split(value)
                if s.wide <= first < s.wide + s.rows:
                    e_ref[base + z, first - s.wide : first - s.wide + s.r_wide] = value
        lanes = lane_iota(s.r_near, s.cols)
        from_halo = jnp.where(core == 0, lanes - (s.cols - s.near), s.near - 1 - lanes) >= 0
        per_plane = s.q_near // 2
        for low in range(s.planes // 2):
            packed = halo_ref[s.pack_e + low * s.r_near : s.pack_e + (low + 1) * s.r_near]
            for j in range(s.q_near):
                plane = j // per_plane * (s.planes // 2) + low
                start = j % per_plane * s.r_near
                v_ref[base + plane, start : start + s.r_near] = jnp.where(
                    from_halo,
                    turn(packed, -j * s.near),
                    source_ref[plane, s.length + start : s.length + start + s.r_near],
                )

    def forward(rows, x_table, sign):
        for z in range(0, depth, group):
            left = l_ref[z : z + group, :rows].reshape(group * rows, 2 * s.cols)
            high, low = split(fold(dot(left, yf_ref[0])))
            a_ref[z : z + group, :rows] = high.reshape(group, rows, s.cols)
            a_ref[z : z + group, s.length : s.length + rows] = low.reshape(group, rows, s.cols)
        turned = signs(s.length, s.cols, 1.0)
        for z in range(0, depth, 2):
            columns = []
            for side in (z, z + 1):
                high, low = a_ref[side, :rows], a_ref[side, s.length : s.length + rows]
                columns.append(jnp.concatenate([high, low, high], 0))
            out = dot(x_table[...], jnp.concatenate(columns, 1))
            for side in (0, 1):
                value = out[:, side * s.cols : (side + 1) * s.cols]
                value = value[: s.length] + turned * turn(value[s.length :], half)
                moved = turn(value, half)
                x1_ref[z + side] = value
                x2_ref[z + side] = moved if sign > 0 else -moved

    def along_z(flip):
        quarter = depth // 4

        def tile(t, carry):
            rows = pl.ds(t * 8, 8)
            order = (lambda z: depth - 1 - z) if flip else (lambda z: z)
            sources = [[ref[order(z), rows] for z in range(depth)] for ref in (x1_ref, x2_ref)]
            middle = 2 * quarter

            def parts(x):
                n = len(x) // 2
                return [[p + q for p, q in zip(x[:n], x[n:])], x[n:], x[:n]]

            def small(leaf, first, second):
                out = []
                for i in range(quarter):
                    total = None
                    for j in range(quarter):
                        d = leaf * (2 * quarter - 1) + i - j + quarter - 1
                        term = k1_ref[d, rows] * first[j] + k2_ref[d, rows] * second[j]
                        total = term if total is None else total + term
                    out.append(total)
                return out

            ones, twos = parts(sources[0]), parts(sources[1])
            kept = None
            for part in range(3):
                inner_ones, inner_twos = parts(ones[part]), parts(twos[part])
                whole_part, upper, lower = (
                    small(3 * part + k, inner_ones[k], inner_twos[k]) for k in range(3)
                )
                value = [p + q for p, q in zip(whole_part, upper)] + [p + q for p, q in zip(whole_part, lower)]
                if part == 0:
                    kept = value
                else:
                    start = 0 if part == 1 else middle
                    for i in range(middle):
                        p_ref[order(start + i), rows] = kept[i] + value[i]
            return carry

        lax.fori_loop(0, s.length // 8, tile, 0)

    def backward(rows, x_table, use):
        turned = signs(rows, s.cols, -1.0)
        for z in range(0, depth, 2):
            columns = []
            for side in (z, z + 1):
                high, low = split(p_ref[side])
                columns.append(jnp.concatenate([high, low, high], 0))
            out = dot(x_table[...], jnp.concatenate(columns, 1))
            for side in (0, 1):
                value = out[:, side * s.cols : (side + 1) * s.cols]
                value = value[:rows] + turned * turn(value[rows:], half)
                b_ref[z + side, :rows] = wide_split(value)
        for z in range(0, depth, group):
            left = b_ref[z : z + group, :rows].reshape(group * rows, 2 * s.cols)
            out = fold(dot(left, yi_ref[0]))
            for k in range(group):
                use(z + k, out[k * rows : (k + 1) * rows])

    forward(s.length, xw_ref, 1)
    along_z(False)

    shape = (s.view_rows, s.cols)
    row = lax.broadcasted_iota(jnp.int32, shape, 0) - s.near
    lane = lane_iota(*shape)
    column = lane + jnp.where(core == 0, jnp.where(lane < s.cols - s.near, 0, -s.cols), jnp.where(lane < s.near, s.cols, 0))
    first_row, last_row = -gx * s.rows, (s.gx - gx) * s.rows
    first_column, last_column = -gy * s.cols, (s.gy - gy) * s.cols
    inside = (row >= first_row) & (row < last_row) & (column >= first_column) & (column < last_column)
    begin = core * half - s.near
    inside = inside & (column >= begin) & (column < begin + half + 2 * s.near)

    def to_ratio(z, blurred):
        safe = jnp.where(inside, blurred, 1.0)
        l_ref[z, : s.view_rows] = wide_split(jnp.where(inside, v_ref[z] / safe, 0.0))

    backward(s.view_rows, xbn_ref, to_ratio)
    forward(s.view_rows, xn_ref, -1)
    along_z(True)

    lane = lane_iota(s.rows, s.cols)
    owned = (lane // half) == core

    def to_update(z, correction):
        value = jnp.where(owned, e_ref[z] * correction, 0.0)
        u_ref[z] = value

    backward(s.rows, xbo_ref, to_update)

    def three(x):
        high, rest = split(x)
        return high, rest, (x - high.astype(F32) - rest.astype(F32)).astype(BF16)

    def pooled(x, factor, scale):
        count = s.cols // factor
        weights = jnp.where(
            lax.broadcasted_iota(jnp.int32, (s.cols, count), 0) // factor
            == lax.broadcasted_iota(jnp.int32, (s.cols, count), 1),
            scale,
            0.0,
        ).astype(BF16)
        return dot(jnp.concatenate(three(x), 1), jnp.concatenate([weights] * 3, 0))

    u_rows = s.planes * s.rows
    source = u_ref
    planes, rows = depth, s.rows
    sums_of = []
    for level in (1, 2, 3, 4):
        planes, rows = planes // 2, rows // 2
        here = t_ref.at[level - 1]
        for z in range(planes):
            here[z, : 2 * rows] = source[2 * z, : 2 * rows] + source[2 * z + 1, : 2 * rows]
        sums = [
            here[z, pl.ds(0, rows, stride=2)] + here[z, pl.ds(1, rows, stride=2)] for z in range(planes)
        ]
        for z in range(planes):
            here[z, :rows] = sums[z]
        sums_of.append(sums)
        source = here
    levels = []
    for level, sums in enumerate(sums_of, 1):
        factor = 2**level
        value = pooled(jnp.concatenate(sums, 0), factor, 1.0 / factor**3)
        levels.append((value, len(sums), sums[0].shape[0], s.cols // factor))
    top = sums_of[-1][0]
    own_rows = top.shape[0] // 2
    per_chip = s.cols // 32
    line = jnp.concatenate([top[2 * i : 2 * i + 1] + top[2 * i + 1 : 2 * i + 2] for i in range(own_rows)], 1)
    cells = five_ref.shape[2]
    source_lane = lax.broadcasted_iota(jnp.int32, (line.shape[1], cells), 0)
    place = (gx * own_rows + source_lane // s.cols) * (s.gy * per_chip) + gy * per_chip + source_lane % s.cols // 32
    weights = jnp.where(
        place == lax.broadcasted_iota(jnp.int32, place.shape, 1), 1.0 / (32 * 32 * depth), 0.0
    ).astype(BF16)
    five = dot(jnp.concatenate(three(line), 1), jnp.concatenate([weights] * 3, 0))
    five_ref[...] = jnp.broadcast_to(five[None], five_ref.shape)
    for half_index in (0, 1):
        for mine, out_ref in ((True, mine_ref), (False, theirs_ref)):

            @pl.when((core == half_index) == mine)
            def _():
                for z in range(s.planes):
                    out_ref[z * s.rows : (z + 1) * s.rows] = u_ref[half_index * s.planes + z]
                start = u_rows
                for value, planes, rows, columns in levels:
                    count = max(planes * rows // 2, rows)
                    begin = half_index * count if planes > 1 else 0
                    out_ref[start : start + count, :columns] = value[begin : begin + count]
                    start += up8(count)


def last_kernel(s, mine_ref, got_ref, fives_ref, u_ref, one_ref, two_ref, three_ref, four_ref, five_ref):
    for z in range(s.planes):
        part = slice(z * s.rows, (z + 1) * s.rows)
        u_ref[z] = mine_ref[part] + got_ref[part]
    start = s.planes * s.rows
    for out_ref in (one_ref, two_ref, three_ref, four_ref):
        planes, rows, columns = out_ref.shape
        for z in range(planes):
            part = slice(start + z * rows, start + (z + 1) * rows)
            out_ref[z] = mine_ref[part, :columns] + got_ref[part, :columns]
        start += up8(planes * rows)
    rows, columns = five_ref.shape[1:]
    total = jnp.sum(fives_ref[...], axis=0)
    cells = rows * columns
    shape = (rows, cells)
    lane = lane_iota(*shape)
    spread = jnp.where(lane // columns == lax.broadcasted_iota(jnp.int32, shape, 0), jnp.broadcast_to(total, shape), 0.0)
    shape = (cells, columns)
    ones = (lax.broadcasted_iota(jnp.int32, shape, 0) % columns == lane_iota(*shape)).astype(BF16)
    high, rest = split(spread)
    low = (spread - high.astype(F32) - rest.astype(F32)).astype(BF16)
    five_ref[0] = dot(jnp.concatenate([high, rest, low], 1), jnp.concatenate([ones] * 3, 0))


def in_hbm(x):
    return pltpu.with_memory_space_constraint(x, pltpu.HBM)


def whole(shape):
    return pl.BlockSpec(shape, lambda *_: (0,) * len(shape))


def call(body, where, arrays, in_specs, outs, scratch=(), narrow=(), name=None, flops=0, mib=16, copies=()):
    grid_spec = pltpu.PrefetchScalarGridSpec(
        num_scalar_prefetch=1,
        grid=(1,),
        in_specs=in_specs,
        out_specs=[whole(shape) for shape in outs],
        scratch_shapes=[pltpu.VMEM(shape, F32) for shape in scratch] + [pltpu.VMEM(shape, BF16) for shape in narrow] + list(copies),
    )
    return pl.pallas_call(
        body,
        grid_spec=grid_spec,
        out_shape=[jax.ShapeDtypeStruct(shape, F32) for shape in outs],
        compiler_params=pltpu.CompilerParams(vmem_limit_bytes=mib * MIB),
        cost_estimate=pl.CostEstimate(flops=flops, bytes_accessed=0, transcendentals=0) if flops else None,
        name=name,
    )(where, *arrays)


def shift(axis, step):
    count = lax.axis_size(axis)
    return [(i, i + step) for i in range(count) if 0 <= i + step < count]


def to_side(same):
    pairs = []
    for h in range(lax.axis_size("gy")):
        sender_up, sender_down = (0, 1) if same else (1, 0)
        if h + 1 < lax.axis_size("gy"):
            pairs.append((2 * h + sender_up, 2 * (h + 1)))
        if h > 0:
            pairs.append((2 * h + sender_down, 2 * (h - 1) + 1))
    return pairs


def local(estimate, view_data, psf_stack, view_index):
    assert lax.axis_size("gz") == 2
    gx, gy = lax.axis_size("gx"), lax.axis_size("gy")
    s = Sizes(estimate.shape, psf_stack.shape, gx, gy)
    t = {key: jnp.asarray(value) for key, value in tables(s).items()}
    where = jnp.stack(
        [view_index[0], lax.axis_index("gz"), lax.axis_index("gx"), lax.axis_index("gy")]
    ).astype(jnp.int32)

    slab = (s.planes, s.wide + s.near, s.cols)
    outs = [estimate.shape, view_data.shape, slab, slab]
    arrays = (in_hbm(estimate), in_hbm(view_data))
    estimate_here, view_here, up, down = pl.pallas_call(
        functools.partial(send_kernel, s),
        in_specs=[pl.BlockSpec(memory_space=pltpu.HBM)] * 2,
        out_specs=[pl.BlockSpec(memory_space=pltpu.VMEM)] * len(outs),
        out_shape=[jax.ShapeDtypeStruct(shape, F32) for shape in outs],
        scratch_shapes=[pltpu.SemaphoreType.DMA((2,))],
        compiler_params=pltpu.CompilerParams(vmem_limit_bytes=8 * MIB),
        name="send",
    )(*arrays)
    below = lax.ppermute(up, "gx", shift("gx", 1))
    above = lax.ppermute(down, "gx", shift("gx", -1))
    psf_shape = (1,) + psf_stack.shape[1:]
    taps = up8(s.extent)
    k1, k2 = call(
        functools.partial(kernel_spectrum, s),
        where,
        (in_hbm(psf_stack), in_hbm(t["y_kernel"]), in_hbm(t["x_kernel"])),
        [pl.BlockSpec(memory_space=pltpu.HBM)] * 3,
        [(9 * (s.depth // 2 - 1), s.length, s.cols)] * 2,
        scratch=[((s.extent + 1) // 2 * 2 * taps, s.cols)] * 2 + [(s.extent, s.length, s.cols), psf_shape],
        narrow=[t["y_kernel"].shape, t["x_kernel"].shape],
        copies=[pltpu.SemaphoreType.DMA((3,))],
        name="kernel_spectrum",
        flops=10**8,
    )
    stack_shape = (s.planes, s.stack_rows, s.cols)
    slab_shape = (s.pack_e + s.pack_v, s.cols)
    arrays = (estimate_here, view_here, below, above)
    stack, same, other = call(
        functools.partial(pack_kernel, s),
        where,
        arrays + (k1,),
        [whole(a.shape) for a in arrays] + [pl.BlockSpec(memory_space=pl.ANY)],
        [stack_shape, slab_shape, slab_shape],
        name="pack",
    )
    partner = lax.ppermute(stack, "gz", [(0, 1), (1, 0)])
    same = lax.ppermute(same, ("gy", "gz"), to_side(True))
    other = lax.ppermute(other, ("gy", "gz"), to_side(False))

    u_rows = s.planes * s.rows
    out_rows = u_rows
    level_shapes = []
    planes, rows, columns = s.depth, s.rows, s.cols
    for _ in range(4):
        planes, rows, columns = planes // 2, rows // 2, columns // 2
        level_shapes.append((max(planes // 2, 1), rows, columns))
        out_rows += up8(level_shapes[-1][0] * rows)
    devices = 2 * gx * gy
    five_shape = (rows // 2 * gx, columns // 2 * gy)
    arrays = (
        stack,
        partner,
        same,
        other,
        k1,
        k2,
        t["y_forward"],
        t["y_inverse"],
        t["x_window"],
        t["x_near"],
        t["x_back_near"],
        t["x_back_own"],
    )
    specs = [whole(a.shape) for a in arrays]
    for k in (6, 7):
        specs[k] = pl.BlockSpec((1,) + arrays[k].shape[1:], lambda i, w: (w[1], 0, 0))
    spectrum = (s.depth, s.length, s.cols)
    mine, theirs, five = call(
        functools.partial(main_kernel, s),
        where,
        arrays,
        specs,
        [(out_rows, s.cols), (out_rows, s.cols), (devices, 1, five_shape[0] * five_shape[1])],
        scratch=[
            (s.depth, s.rows, s.cols),
            (s.depth, s.view_rows, s.cols),
            spectrum,
            spectrum,
            spectrum,
            (s.depth, s.rows, s.cols),
            (4, s.depth // 2, s.rows, s.cols),
        ],
        narrow=[
            (s.depth, s.length, 2 * s.cols),
            (s.depth, 2 * s.length, s.cols),
            (s.depth, s.view_rows, 2 * s.cols),
        ],
        name="update",
        mib=24,
    )
    got = lax.ppermute(theirs, "gz", [(0, 1), (1, 0)])
    fives = lax.all_to_all(five, ALL, split_axis=0, concat_axis=0, tiled=True)
    outs = [estimate.shape] + level_shapes + [(1,) + five_shape]
    arrays = (mine, got, fives)
    return tuple(
        pl.pallas_call(
            functools.partial(last_kernel, s),
            in_specs=[whole(a.shape) for a in arrays],
            out_specs=[whole(shape) for shape in outs],
            out_shape=[jax.ShapeDtypeStruct(shape, F32) for shape in outs],
            grid=(1,),
            compiler_params=pltpu.CompilerParams(vmem_limit_bytes=8 * MIB),
            name="assemble",
        )(*arrays)
    )


def solution(mesh):
    return jax.shard_map(
        local,
        mesh=mesh,
        in_specs=(P("gz", "gx", "gy"), P("gz", "gx", "gy"), P(), P()),
        out_specs=(
            P("gz", "gx", "gy"),
            P("gz", "gx", "gy"),
            P("gz", "gx", "gy"),
            P("gz", "gx", "gy"),
            P(None, "gx", "gy"),
            P(),
        ),
        check_vma=False,
    )
```

```python
import functools

import jax
import jax.numpy as jnp
import ml_dtypes
import numpy as np
from jax import lax
from jax.experimental import pallas as pl
from jax.experimental.pallas import tpu as pltpu
from jax.sharding import PartitionSpec as P

F32 = jnp.float32
BF16 = jnp.bfloat16
ALL = ("gx", "gy", "gz")
MIB = 1024 * 1024


def up8(count):
    return (count + 7) // 8 * 8


class Sizes:
    def __init__(self, estimate_shape, psf_shape, gx, gy):
        self.planes, self.rows, self.cols = estimate_shape
        self.extent = psf_shape[1]
        self.radius = (self.extent - 1) // 2
        self.depth = 2 * self.planes
        self.half = self.cols // 2
        self.wide = up8(2 * self.radius)
        self.near = up8(self.radius)
        self.length = self.rows + 2 * self.wide
        self.view_rows = self.rows + 2 * self.near
        self.stack_rows = self.length + self.view_rows
        self.freqs = self.cols // 2
        self.q_wide = self.cols // self.wide
        self.r_wide = self.length // self.q_wide
        self.q_near = self.cols // self.near
        self.r_near = self.view_rows * 2 // self.q_near
        self.pack_e = self.planes * self.r_wide
        self.pack_v = self.planes // 2 * self.r_near
        self.gx, self.gy = gx, gy
        assert self.half + 2 * self.wide == self.cols == 128
        assert self.wide <= self.rows and self.r_wide % 8 == 0 and self.r_near % 8 == 0
        assert self.depth == 16


def split_np(matrix):
    high = matrix.astype(np.float32).astype(ml_dtypes.bfloat16)
    low = (matrix - high.astype(np.float64)).astype(np.float32).astype(ml_dtypes.bfloat16)
    return high, low


def lane_positions(s, core):
    lanes = np.arange(s.cols)
    return (lanes + s.wide) % s.cols if core == 0 else (lanes - s.wide) % s.cols


def right_pair(matrix):
    high, low = split_np(matrix)
    return np.block([[high, low], [high, np.zeros_like(low)]])


def left_pair(matrix):
    high, low = split_np(matrix)
    return np.block([[high, high], [low, np.zeros_like(low)]])


def tables(s):
    y_freq = 2.0 * np.pi * (np.arange(s.freqs) + 0.5) / s.cols
    x_freq = 2.0 * np.pi * (np.arange(s.length // 2) + 0.5) / s.length
    y_forward, y_inverse = [], []
    for core in (0, 1):
        angle = lane_positions(s, core)[:, None] * y_freq[None, :]
        both = np.concatenate([np.cos(angle), np.sin(angle)], 1)
        y_forward.append(right_pair(both))
        y_inverse.append(right_pair(both.T * (2.0 / s.cols / s.length)))
    offset = np.arange(s.cols) - s.radius
    angle = offset[:, None] * y_freq[None, :]
    y_kernel = np.concatenate([np.cos(angle), np.sin(angle)], 1)
    y_kernel[s.extent :] = 0.0

    def x_forward(positions):
        angle = x_freq[:, None] * positions[None, :]
        return np.concatenate([np.cos(angle), np.sin(angle)], 0)

    def x_inverse(positions):
        angle = positions[:, None] * x_freq[None, :]
        return np.concatenate([np.cos(angle), -np.sin(angle)], 1)

    window = np.arange(s.length) - s.wide
    near = np.arange(s.view_rows) - s.near
    own = np.arange(s.rows)
    taps = np.arange(up8(s.extent)) - s.radius
    high, low = split_np(x_forward(taps))
    x_kernel = np.concatenate([high, high, low], 1)
    return dict(
        y_forward=np.stack(y_forward),
        y_inverse=np.stack(y_inverse),
        y_kernel=right_pair(y_kernel),
        x_window=left_pair(x_forward(window)),
        x_near=left_pair(x_forward(near)),
        x_back_near=left_pair(x_inverse(near)),
        x_back_own=left_pair(x_inverse(own)),
        x_kernel=x_kernel,
    )


def split(x):
    high = x.astype(BF16)
    return high, (x - high.astype(F32)).astype(BF16)


def dot(a, b):
    return lax.dot_general(a, b, (((1,), (0,)), ((), ())), preferred_element_type=F32)


def lane_iota(rows, cols):
    return lax.broadcasted_iota(jnp.int32, (rows, cols), 1)


def turn(x, shift):
    shift %= x.shape[1]
    return pltpu.roll(x, shift, 1) if shift else x


def wide_split(x):
    return jnp.concatenate(split(x), 1)


def tall_split(x):
    return jnp.concatenate(split(x), 0)


def fold(both):
    width = both.shape[1] // 2
    return both[:, :width] + both[:, width:]


def fold_rows(both):
    count = both.shape[0] // 2
    return both[:count] + both[count:]


def spectrum_of(cosine, sine):
    half = cosine.shape[1] // 2
    left = lane_iota(*cosine.shape) < half
    moved = turn(sine, half)
    minus, plus = cosine - moved, turn(cosine + moved, half)
    return jnp.where(left, minus, plus), jnp.where(left, -plus, minus)


def send_kernel(s, e_in, v_in, e_ref, v_ref, up_ref, down_ref, sem_ref):
    moves = [
        pltpu.make_async_copy(e_in, e_ref, sem_ref.at[0]),
        pltpu.make_async_copy(v_in, v_ref, sem_ref.at[1]),
    ]
    for move in moves:
        move.start()
    for move in moves:
        move.wait()
    up_ref[:, : s.wide] = e_ref[:, s.rows - s.wide :]
    up_ref[:, s.wide :] = v_ref[:, s.rows - s.near :]
    down_ref[:, : s.wide] = e_ref[:, : s.wide]
    down_ref[:, s.wide :] = v_ref[:, : s.near]


def pack_kernel(s, where_ref, e_ref, v_ref, below_ref, above_ref, k_ref, stack_ref, same_ref, other_ref):
    w, n, length = s.wide, s.near, s.length
    stack_ref[:, :w] = below_ref[:, :w]
    stack_ref[:, w : w + s.rows] = e_ref[...]
    stack_ref[:, w + s.rows : length] = above_ref[:, :w]
    stack_ref[:, length : length + n] = below_ref[:, w:]
    stack_ref[:, length + n : length + n + s.rows] = v_ref[...]
    stack_ref[:, length + n + s.rows :] = above_ref[:, w:]
    first_core = where_ref[1] == 0

    def put(start, count, last, first):
        same_ref[pl.ds(start, count)] = jnp.where(first_core, last, first)
        other_ref[pl.ds(start, count)] = jnp.where(first_core, first, last)

    group = lane_iota(s.r_wide, s.cols) // w
    for z in range(s.planes):
        last = first = jnp.zeros((s.r_wide, s.cols), F32)
        for q in range(s.q_wide):
            moved = turn(stack_ref[z, q * s.r_wide : (q + 1) * s.r_wide], q * w)
            last = jnp.where(group == (q - 1) % s.q_wide, moved, last)
            first = jnp.where(group == q, moved, first)
        put(z * s.r_wide, s.r_wide, last, first)
    group = lane_iota(s.r_near, s.cols) // n
    per_plane = s.q_near // 2
    for low in range(s.planes // 2):
        last = first = jnp.zeros((s.r_near, s.cols), F32)
        for j in range(s.q_near):
            plane = j // per_plane * (s.planes // 2) + low
            start = length + j % per_plane * s.r_near
            moved = turn(stack_ref[plane, start : start + s.r_near], j * n)
            last = jnp.where(group == (j - 1) % s.q_near, moved, last)
            first = jnp.where(group == j, moved, first)
        put(s.pack_e + low * s.r_near, s.r_near, last, first)


def toeplitz_parts(taps):
    middle = len(taps) // 2
    half = (middle + 1) // 2
    centre = taps[middle - half + 1 : middle + half]
    upper = [p - q for p, q in zip(taps[middle - 2 * half + 1 : middle], centre)]
    lower = [p - q for p, q in zip(taps[middle + 1 : middle + 2 * half], centre)]
    return centre, upper, lower


def kernel_spectrum(
    s, where_ref, psf_in, y_in, x_in, k_ref, ks_ref, kd_ref, pad_ref, a_ref, re_ref, im_ref, psf_ref, y_ref, x_ref, sem_ref
):
    taps = up8(s.extent)
    moves = [
        pltpu.make_async_copy(psf_in.at[pl.ds(where_ref[0], 1)], psf_ref, sem_ref.at[0]),
        pltpu.make_async_copy(y_in, y_ref, sem_ref.at[1]),
        pltpu.make_async_copy(x_in, x_ref, sem_ref.at[2]),
    ]
    for move in moves:
        move.start()
    pad_ref[...] = jnp.zeros_like(pad_ref)
    for move in moves:
        move.wait()
    total = jnp.zeros((s.extent, s.extent), F32)
    for a in range(s.extent):
        total = total + psf_ref[0, a]
    total = jnp.sum(total)
    for a in range(s.extent):
        pad_ref[a * taps : a * taps + s.extent, : s.extent] = psf_ref[0, a] / total
    a_ref[...] = fold(dot(wide_split(pad_ref[...]), y_ref[...]))
    for pair in range((s.extent + 1) // 2):
        columns = []
        for side in (0, 1):
            a = 2 * pair + side
            high, low = split(a_ref[a * taps : (a + 1) * taps])
            columns.append(jnp.concatenate([high, low, high], 0))
        out = dot(x_ref[...], jnp.concatenate(columns, 1))
        for side in (0, 1):
            if 2 * pair + side < s.extent:
                value = out[:, side * s.cols : (side + 1) * s.cols]
                re_ref[2 * pair + side], im_ref[2 * pair + side] = spectrum_of(value[: s.length // 2], value[s.length // 2 :])
    first = s.radius - (s.depth - 1)

    def tile(t, carry):
        rows = pl.ds(t * 8, 8)
        real = [re_ref[a, rows] for a in range(first, first + 2 * s.depth - 1)]
        imag = [im_ref[a, rows] for a in range(first, first + 2 * s.depth - 1)]
        total = [p + q for p, q in zip(real, imag)]
        change = [q - p for p, q in zip(real, imag)]
        for out_ref, values in ((k_ref, real), (ks_ref, total), (kd_ref, change)):
            place = 0
            for part in toeplitz_parts(values):
                for inner in toeplitz_parts(part):
                    for value in inner:
                        out_ref[place, rows] = value
                        place += 1
        return carry

    lax.fori_loop(0, s.length // 16, tile, 0)


def main_kernel(
    s,
    where_ref,
    own_ref,
    partner_ref,
    same_ref,
    other_ref,
    k_ref,
    ks_ref,
    kd_ref,
    yf_ref,
    yi_ref,
    xw_ref,
    xn_ref,
    xbn_ref,
    xbo_ref,
    mine_ref,
    theirs_ref,
    five_ref,
    e_ref,
    v_ref,
    re_ref,
    im_ref,
    pr_ref,
    pi_ref,
    u_ref,
    t_ref,
    l_ref,
    a_ref,
    b_ref,
):
    core, gx, gy = where_ref[1], where_ref[2], where_ref[3]
    half = s.cols // 2
    depth = s.depth
    group = 4
    for source_ref, halo_ref, base in (
        (own_ref, same_ref, core * s.planes),
        (partner_ref, other_ref, (1 - core) * s.planes),
    ):
        lanes = lane_iota(s.r_wide, s.cols)
        from_halo = jnp.where(core == 0, lanes - (s.cols - s.wide), s.wide - 1 - lanes) >= 0
        for z in range(s.planes):
            packed = halo_ref[z * s.r_wide : (z + 1) * s.r_wide]
            for q in range(s.q_wide):
                first = q * s.r_wide
                rows = slice(first, first + s.r_wide)
                value = jnp.where(from_halo, turn(packed, -q * s.wide), source_ref[z, rows])
                high, low = split(value)
                l_ref[base + z, rows] = high
                l_ref[base + z, s.length + first : s.length + first + s.r_wide] = low
                if s.wide <= first < s.wide + s.rows:
                    e_ref[base + z, first - s.wide : first - s.wide + s.r_wide] = value
        lanes = lane_iota(s.r_near, s.cols)
        from_halo = jnp.where(core == 0, lanes - (s.cols - s.near), s.near - 1 - lanes) >= 0
        per_plane = s.q_near // 2
        for low in range(s.planes // 2):
            packed = halo_ref[s.pack_e + low * s.r_near : s.pack_e + (low + 1) * s.r_near]
            for j in range(s.q_near):
                plane = j // per_plane * (s.planes // 2) + low
                start = j % per_plane * s.r_near
                v_ref[base + plane, start : start + s.r_near] = jnp.where(
                    from_halo,
                    turn(packed, -j * s.near),
                    source_ref[plane, s.length + start : s.length + start + s.r_near],
                )

    freqs = s.length // 2

    def forward(rows, x_table):
        for z in range(0, depth, 2):
            both = jnp.concatenate([l_ref[z, : 2 * rows], l_ref[z + 1, : 2 * rows]], 1)
            out = fold_rows(dot(x_table[...], both))
            for side in (0, 1):
                a_ref[z + side] = wide_split(out[:, side * s.cols : (side + 1) * s.cols])
        for z in range(0, depth, group):
            out = fold(dot(a_ref[z : z + group].reshape(group * s.length, 2 * s.cols), yf_ref[0]))
            for k in range(group):
                value = out[k * s.length : (k + 1) * s.length]
                re_ref[z + k], im_ref[z + k] = spectrum_of(value[:freqs], value[freqs:])

    def along_z(flip):
        quarter = depth // 4
        order = (lambda z: depth - 1 - z) if flip else (lambda z: z)
        for_re, for_im = (kd_ref, ks_ref) if flip else (ks_ref, kd_ref)

        def parts(x):
            n = len(x) // 2
            return [p + q for p, q in zip(x[:n], x[n:])], x[n:], x[:n]

        def joined(pieces):
            middle, upper, lower = pieces
            return [p + q for p, q in zip(middle, upper)] + [p + q for p, q in zip(middle, lower)]

        def tile(t, carry):
            rows = pl.ds(t * 8, 8)
            real = [re_ref[order(z), rows] for z in range(depth)]
            imag = [im_ref[order(z), rows] for z in range(depth)]
            outer = [parts(x) for x in ([p + q for p, q in zip(real, imag)], imag, real)]
            kept = None
            for part in range(3):
                inner = [parts(x[part]) for x in outer]
                pieces = []
                for piece in range(3):
                    found = []
                    for i in range(quarter):
                        sums = []
                        for table, values in zip((k_ref, for_re, for_im), inner):
                            total = None
                            for j in range(quarter):
                                d = (3 * part + piece) * (2 * quarter - 1) + i - j + quarter - 1
                                term = table[d, rows] * values[piece][j]
                                total = term if total is None else total + term
                            sums.append(total)
                        if flip:
                            found.append((sums[0] + sums[1], sums[0] - sums[2]))
                        else:
                            found.append((sums[0] - sums[1], sums[0] + sums[2]))
                    pieces.append(found)
                value = [joined([[f[k] for f in found] for found in pieces]) for k in (0, 1)]
                if part == 0:
                    kept = value
                else:
                    start = 0 if part == 1 else 2 * quarter
                    for i in range(2 * quarter):
                        pr_ref[order(start + i), rows] = kept[0][i] + value[0][i]
                        pi_ref[order(start + i), rows] = kept[1][i] + value[1][i]
            return carry

        lax.fori_loop(0, freqs // 8, tile, 0)

    def backward(rows, x_table, use):
        half_lanes = lane_iota(freqs, s.cols) < half
        for z in range(0, depth, group):
            pieces = []
            for k in range(group):
                real, imag = pr_ref[z + k], pi_ref[z + k]
                turned_real, turned_imag = turn(real, half), turn(imag, half)
                pieces.append(jnp.where(half_lanes, real + turned_real, imag - turned_imag))
                pieces.append(jnp.where(half_lanes, imag + turned_imag, turned_real - real))
            out = fold(dot(wide_split(jnp.concatenate(pieces, 0)), yi_ref[0]))
            for k in range(group):
                b_ref[z + k] = tall_split(out[k * s.length : (k + 1) * s.length])
        for z in range(0, depth, 2):
            out = fold_rows(dot(x_table[...], jnp.concatenate([b_ref[z], b_ref[z + 1]], 1)))
            for side in (0, 1):
                use(z + side, out[:, side * s.cols : (side + 1) * s.cols])

    forward(s.length, xw_ref)
    along_z(False)

    shape = (s.view_rows, s.cols)
    row = lax.broadcasted_iota(jnp.int32, shape, 0) - s.near
    lane = lane_iota(*shape)
    column = lane + jnp.where(core == 0, jnp.where(lane < s.cols - s.near, 0, -s.cols), jnp.where(lane < s.near, s.cols, 0))
    first_row, last_row = -gx * s.rows, (s.gx - gx) * s.rows
    first_column, last_column = -gy * s.cols, (s.gy - gy) * s.cols
    inside = (row >= first_row) & (row < last_row) & (column >= first_column) & (column < last_column)
    begin = core * half - s.near
    inside = inside & (column >= begin) & (column < begin + half + 2 * s.near)

    def to_ratio(z, blurred):
        safe = jnp.where(inside, blurred, 1.0)
        l_ref[z, : 2 * s.view_rows] = tall_split(jnp.where(inside, v_ref[z] / safe, 0.0))

    backward(s.view_rows, xbn_ref, to_ratio)
    forward(s.view_rows, xn_ref)
    along_z(True)

    lane = lane_iota(s.rows, s.cols)
    owned = (lane // half) == core

    def to_update(z, correction):
        value = jnp.where(owned, e_ref[z] * correction, 0.0)
        u_ref[z] = value

    backward(s.rows, xbo_ref, to_update)

    def three(x):
        high, rest = split(x)
        return high, rest, (x - high.astype(F32) - rest.astype(F32)).astype(BF16)

    def pooled(x, factor, scale):
        count = s.cols // factor
        weights = jnp.where(
            lax.broadcasted_iota(jnp.int32, (s.cols, count), 0) // factor
            == lax.broadcasted_iota(jnp.int32, (s.cols, count), 1),
            scale,
            0.0,
        ).astype(BF16)
        return dot(jnp.concatenate(three(x), 1), jnp.concatenate([weights] * 3, 0))

    u_rows = s.planes * s.rows
    source = u_ref
    planes, rows = depth, s.rows
    sums_of = []
    for level in (1, 2, 3, 4):
        planes, rows = planes // 2, rows // 2
        here = t_ref.at[level - 1]
        for z in range(planes):
            here[z, : 2 * rows] = source[2 * z, : 2 * rows] + source[2 * z + 1, : 2 * rows]
        sums = [
            here[z, pl.ds(0, rows, stride=2)] + here[z, pl.ds(1, rows, stride=2)] for z in range(planes)
        ]
        for z in range(planes):
            here[z, :rows] = sums[z]
        sums_of.append(sums)
        source = here
    levels = []
    for level, sums in enumerate(sums_of, 1):
        factor = 2**level
        value = pooled(jnp.concatenate(sums, 0), factor, 1.0 / factor**3)
        levels.append((value, len(sums), sums[0].shape[0], s.cols // factor))
    top = sums_of[-1][0]
    own_rows = top.shape[0] // 2
    per_chip = s.cols // 32
    line = jnp.concatenate([top[2 * i : 2 * i + 1] + top[2 * i + 1 : 2 * i + 2] for i in range(own_rows)], 1)
    cells = five_ref.shape[2]
    source_lane = lax.broadcasted_iota(jnp.int32, (line.shape[1], cells), 0)
    place = (gx * own_rows + source_lane // s.cols) * (s.gy * per_chip) + gy * per_chip + source_lane % s.cols // 32
    weights = jnp.where(
        place == lax.broadcasted_iota(jnp.int32, place.shape, 1), 1.0 / (32 * 32 * depth), 0.0
    ).astype(BF16)
    five = dot(jnp.concatenate(three(line), 1), jnp.concatenate([weights] * 3, 0))
    five_ref[...] = jnp.broadcast_to(five[None], five_ref.shape)
    for half_index in (0, 1):
        for mine, out_ref in ((True, mine_ref), (False, theirs_ref)):

            @pl.when((core == half_index) == mine)
            def _():
                for z in range(s.planes):
                    out_ref[z * s.rows : (z + 1) * s.rows] = u_ref[half_index * s.planes + z]
                start = u_rows
                for value, planes, rows, columns in levels:
                    count = max(planes * rows // 2, rows)
                    begin = half_index * count if planes > 1 else 0
                    out_ref[start : start + count, :columns] = value[begin : begin + count]
                    start += up8(count)


def last_kernel(s, mine_ref, got_ref, fives_ref, u_ref, one_ref, two_ref, three_ref, four_ref, five_ref):
    for z in range(s.planes):
        part = slice(z * s.rows, (z + 1) * s.rows)
        u_ref[z] = mine_ref[part] + got_ref[part]
    start = s.planes * s.rows
    for out_ref in (one_ref, two_ref, three_ref, four_ref):
        planes, rows, columns = out_ref.shape
        for z in range(planes):
            part = slice(start + z * rows, start + (z + 1) * rows)
            out_ref[z] = mine_ref[part, :columns] + got_ref[part, :columns]
        start += up8(planes * rows)
    rows, columns = five_ref.shape[1:]
    total = jnp.sum(fives_ref[...], axis=0)
    cells = rows * columns
    shape = (rows, cells)
    lane = lane_iota(*shape)
    spread = jnp.where(lane // columns == lax.broadcasted_iota(jnp.int32, shape, 0), jnp.broadcast_to(total, shape), 0.0)
    shape = (cells, columns)
    ones = (lax.broadcasted_iota(jnp.int32, shape, 0) % columns == lane_iota(*shape)).astype(BF16)
    high, rest = split(spread)
    low = (spread - high.astype(F32) - rest.astype(F32)).astype(BF16)
    five_ref[0] = dot(jnp.concatenate([high, rest, low], 1), jnp.concatenate([ones] * 3, 0))


def in_hbm(x):
    return pltpu.with_memory_space_constraint(x, pltpu.HBM)


def whole(shape):
    return pl.BlockSpec(shape, lambda *_: (0,) * len(shape))


def call(body, where, arrays, in_specs, outs, scratch=(), narrow=(), name=None, flops=0, mib=16, copies=()):
    grid_spec = pltpu.PrefetchScalarGridSpec(
        num_scalar_prefetch=1,
        grid=(1,),
        in_specs=in_specs,
        out_specs=[whole(shape) for shape in outs],
        scratch_shapes=[pltpu.VMEM(shape, F32) for shape in scratch] + [pltpu.VMEM(shape, BF16) for shape in narrow] + list(copies),
    )
    return pl.pallas_call(
        body,
        grid_spec=grid_spec,
        out_shape=[jax.ShapeDtypeStruct(shape, F32) for shape in outs],
        compiler_params=pltpu.CompilerParams(vmem_limit_bytes=mib * MIB),
        cost_estimate=pl.CostEstimate(flops=flops, bytes_accessed=0, transcendentals=0) if flops else None,
        name=name,
    )(where, *arrays)


def shift(axis, step):
    count = lax.axis_size(axis)
    return [(i, i + step) for i in range(count) if 0 <= i + step < count]


def to_side(same):
    pairs = []
    for h in range(lax.axis_size("gy")):
        sender_up, sender_down = (0, 1) if same else (1, 0)
        if h + 1 < lax.axis_size("gy"):
            pairs.append((2 * h + sender_up, 2 * (h + 1)))
        if h > 0:
            pairs.append((2 * h + sender_down, 2 * (h - 1) + 1))
    return pairs


def local(estimate, view_data, psf_stack, view_index):
    assert lax.axis_size("gz") == 2
    gx, gy = lax.axis_size("gx"), lax.axis_size("gy")
    s = Sizes(estimate.shape, psf_stack.shape, gx, gy)
    t = {key: jnp.asarray(value) for key, value in tables(s).items()}
    where = jnp.stack(
        [view_index[0], lax.axis_index("gz"), lax.axis_index("gx"), lax.axis_index("gy")]
    ).astype(jnp.int32)

    slab = (s.planes, s.wide + s.near, s.cols)
    outs = [estimate.shape, view_data.shape, slab, slab]
    arrays = (in_hbm(estimate), in_hbm(view_data))
    estimate_here, view_here, up, down = pl.pallas_call(
        functools.partial(send_kernel, s),
        in_specs=[pl.BlockSpec(memory_space=pltpu.HBM)] * 2,
        out_specs=[pl.BlockSpec(memory_space=pltpu.VMEM)] * len(outs),
        out_shape=[jax.ShapeDtypeStruct(shape, F32) for shape in outs],
        scratch_shapes=[pltpu.SemaphoreType.DMA((2,))],
        compiler_params=pltpu.CompilerParams(vmem_limit_bytes=8 * MIB),
        name="send",
    )(*arrays)
    below = lax.ppermute(up, "gx", shift("gx", 1))
    above = lax.ppermute(down, "gx", shift("gx", -1))
    psf_shape = (1,) + psf_stack.shape[1:]
    taps = up8(s.extent)
    k, ks, kd = call(
        functools.partial(kernel_spectrum, s),
        where,
        (in_hbm(psf_stack), in_hbm(t["y_kernel"]), in_hbm(t["x_kernel"])),
        [pl.BlockSpec(memory_space=pltpu.HBM)] * 3,
        [(9 * (s.depth // 2 - 1), s.length // 2, s.cols)] * 3,
        scratch=[((s.extent + 1) // 2 * 2 * taps, s.cols)] * 2 + [(s.extent, s.length // 2, s.cols)] * 2 + [psf_shape],
        narrow=[t["y_kernel"].shape, t["x_kernel"].shape],
        copies=[pltpu.SemaphoreType.DMA((3,))],
        name="kernel_spectrum",
        flops=10**8,
    )
    stack_shape = (s.planes, s.stack_rows, s.cols)
    slab_shape = (s.pack_e + s.pack_v, s.cols)
    arrays = (estimate_here, view_here, below, above)
    stack, same, other = call(
        functools.partial(pack_kernel, s),
        where,
        arrays + (k,),
        [whole(a.shape) for a in arrays] + [pl.BlockSpec(memory_space=pl.ANY)],
        [stack_shape, slab_shape, slab_shape],
        name="pack",
    )
    partner = lax.ppermute(stack, "gz", [(0, 1), (1, 0)])
    same = lax.ppermute(same, ("gy", "gz"), to_side(True))
    other = lax.ppermute(other, ("gy", "gz"), to_side(False))

    u_rows = s.planes * s.rows
    out_rows = u_rows
    level_shapes = []
    planes, rows, columns = s.depth, s.rows, s.cols
    for _ in range(4):
        planes, rows, columns = planes // 2, rows // 2, columns // 2
        level_shapes.append((max(planes // 2, 1), rows, columns))
        out_rows += up8(level_shapes[-1][0] * rows)
    devices = 2 * gx * gy
    five_shape = (rows // 2 * gx, columns // 2 * gy)
    arrays = (
        stack,
        partner,
        same,
        other,
        k,
        ks,
        kd,
        t["y_forward"],
        t["y_inverse"],
        t["x_window"],
        t["x_near"],
        t["x_back_near"],
        t["x_back_own"],
    )
    specs = [whole(a.shape) for a in arrays]
    for k in (7, 8):
        specs[k] = pl.BlockSpec((1,) + arrays[k].shape[1:], lambda i, w: (w[1], 0, 0))
    spectrum = (s.depth, s.length // 2, s.cols)
    mine, theirs, five = call(
        functools.partial(main_kernel, s),
        where,
        arrays,
        specs,
        [(out_rows, s.cols), (out_rows, s.cols), (devices, 1, five_shape[0] * five_shape[1])],
        scratch=[
            (s.depth, s.rows, s.cols),
            (s.depth, s.view_rows, s.cols),
            spectrum,
            spectrum,
            spectrum,
            spectrum,
            (s.depth, s.rows, s.cols),
            (4, s.depth // 2, s.rows, s.cols),
        ],
        narrow=[
            (s.depth, 2 * s.length, s.cols),
            (s.depth, s.length, 2 * s.cols),
            (s.depth, 2 * s.length, s.cols),
        ],
        name="update",
        mib=24,
    )
    got = lax.ppermute(theirs, "gz", [(0, 1), (1, 0)])
    fives = lax.all_to_all(five, ALL, split_axis=0, concat_axis=0, tiled=True)
    outs = [estimate.shape] + level_shapes + [(1,) + five_shape]
    arrays = (mine, got, fives)
    return tuple(
        pl.pallas_call(
            functools.partial(last_kernel, s),
            in_specs=[whole(a.shape) for a in arrays],
            out_specs=[whole(shape) for shape in outs],
            out_shape=[jax.ShapeDtypeStruct(shape, F32) for shape in outs],
            grid=(1,),
            compiler_params=pltpu.CompilerParams(vmem_limit_bytes=8 * MIB),
            name="assemble",
        )(*arrays)
    )


def solution(mesh):
    return jax.shard_map(
        local,
        mesh=mesh,
        in_specs=(P("gz", "gx", "gy"), P("gz", "gx", "gy"), P(), P()),
        out_specs=(
            P("gz", "gx", "gy"),
            P("gz", "gx", "gy"),
            P("gz", "gx", "gy"),
            P("gz", "gx", "gy"),
            P(None, "gx", "gy"),
            P(),
        ),
        check_vma=False,
    )
```

```python
import functools

import jax
import jax.numpy as jnp
import ml_dtypes
import numpy as np
from jax import lax
from jax.experimental import pallas as pl
from jax.experimental.pallas import tpu as pltpu
from jax.sharding import PartitionSpec as P

F32 = jnp.float32
BF16 = jnp.bfloat16
ALL = ("gx", "gy", "gz")
MIB = 1024 * 1024


def up8(count):
    return (count + 7) // 8 * 8


class Sizes:
    def __init__(self, estimate_shape, psf_shape, gx, gy):
        self.planes, self.rows, self.cols = estimate_shape
        self.extent = psf_shape[1]
        self.radius = (self.extent - 1) // 2
        self.depth = 2 * self.planes
        self.half = self.cols // 2
        self.wide = up8(2 * self.radius)
        self.near = up8(self.radius)
        self.length = self.rows + 2 * self.wide
        self.view_rows = self.rows + 2 * self.near
        self.freqs = self.cols // 2
        self.q_wide = self.cols // self.wide
        self.q_near = self.cols // self.near
        self.pack_e = self.depth // self.q_wide * self.length
        self.pack_v = self.depth // self.q_near * self.view_rows
        self.gx, self.gy = gx, gy
        assert self.half + 2 * self.wide == self.cols == 128
        assert self.wide <= self.rows and self.depth % self.q_near == 0
        assert self.depth == 16


def split_np(matrix):
    high = matrix.astype(np.float32).astype(ml_dtypes.bfloat16)
    low = (matrix - high.astype(np.float64)).astype(np.float32).astype(ml_dtypes.bfloat16)
    return high, low


def lane_positions(s, core):
    lanes = np.arange(s.cols)
    return (lanes + s.wide) % s.cols if core == 0 else (lanes - s.wide) % s.cols


def right_pair(matrix):
    high, low = split_np(matrix)
    return np.block([[high, low], [high, np.zeros_like(low)]])


def left_pair(matrix):
    high, low = split_np(matrix)
    return np.block([[high, high], [low, np.zeros_like(low)]])


def tables(s):
    y_freq = 2.0 * np.pi * (np.arange(s.freqs) + 0.5) / s.cols
    x_freq = 2.0 * np.pi * (np.arange(s.length // 2) + 0.5) / s.length
    y_forward, y_inverse = [], []
    for core in (0, 1):
        angle = lane_positions(s, core)[:, None] * y_freq[None, :]
        both = np.concatenate([np.cos(angle), np.sin(angle)], 1)
        y_forward.append(right_pair(both))
        y_inverse.append(right_pair(both.T * (2.0 / s.cols / s.length)))
    offset = np.arange(s.cols) - s.radius
    angle = offset[:, None] * y_freq[None, :]
    y_kernel = np.concatenate([np.cos(angle), np.sin(angle)], 1)
    y_kernel[s.extent :] = 0.0

    def x_forward(positions):
        angle = x_freq[:, None] * positions[None, :]
        return np.concatenate([np.cos(angle), np.sin(angle)], 0)

    def x_inverse(positions):
        angle = positions[:, None] * x_freq[None, :]
        return np.concatenate([np.cos(angle), -np.sin(angle)], 1)

    window = np.arange(s.length) - s.wide
    near = np.arange(s.view_rows) - s.near
    own = np.arange(s.rows)
    taps = np.arange(up8(s.extent)) - s.radius
    high, low = split_np(x_forward(taps))
    x_kernel = np.concatenate([high, high, low], 1)
    return dict(
        y_forward=np.stack(y_forward),
        y_inverse=np.stack(y_inverse),
        y_kernel=right_pair(y_kernel),
        x_window=left_pair(x_forward(window)),
        x_near=left_pair(x_forward(near)),
        x_back_near=left_pair(x_inverse(near)),
        x_back_own=left_pair(x_inverse(own)),
        x_kernel=x_kernel,
    )


def split(x):
    high = x.astype(BF16)
    return high, (x - high.astype(F32)).astype(BF16)


def dot(a, b):
    return lax.dot_general(a, b, (((1,), (0,)), ((), ())), preferred_element_type=F32)


def lane_iota(rows, cols):
    return lax.broadcasted_iota(jnp.int32, (rows, cols), 1)


def turn(x, shift):
    shift %= x.shape[1]
    return pltpu.roll(x, shift, 1) if shift else x


def wide_split(x):
    return jnp.concatenate(split(x), 1)


def tall_split(x):
    return jnp.concatenate(split(x), 0)


def fold(both):
    width = both.shape[1] // 2
    return both[:, :width] + both[:, width:]


def fold_rows(both):
    count = both.shape[0] // 2
    return both[:count] + both[count:]


def spectrum_of(cosine, sine):
    half = cosine.shape[1] // 2
    left = lane_iota(*cosine.shape) < half
    moved = turn(sine, half)
    minus, plus = cosine - moved, turn(cosine + moved, half)
    return jnp.where(left, minus, plus), jnp.where(left, -plus, minus)


def send_kernel(s, e_in, v_in, both_ref, even_ref, odd_ref, sem_ref):
    moves = [
        pltpu.make_async_copy(e_in, both_ref.at[:, : s.rows], sem_ref.at[0]),
        pltpu.make_async_copy(v_in, both_ref.at[:, s.rows :], sem_ref.at[1]),
    ]
    for move in moves:
        move.start()
    even = lax.axis_index("gx") % 2 == 0
    for move in moves:
        move.wait()
    place = 0
    for z in range(s.planes):
        for start, count in ((0, 2 * s.radius), (s.rows, s.radius)):
            low = both_ref[z, start : start + count]
            high = both_ref[z, start + s.rows - count : start + s.rows]
            even_ref[place : place + count] = jnp.where(even, high, low)
            odd_ref[place : place + count] = jnp.where(even, low, high)
            place += count


def pack_kernel(
    s, where_ref, own_ref, partner_ref, even_ref, odd_ref, even2_ref, odd2_ref, k_ref, l_ref, v_ref, e_slab_ref, v_slab_ref, w_ref
):
    core = where_ref[1]
    even = where_ref[2] % 2 == 0
    wide, near = 2 * s.radius, s.radius
    for both_ref, e_x_ref, o_x_ref, base in (
        (own_ref, even_ref, odd_ref, core * s.planes),
        (partner_ref, even2_ref, odd2_ref, (1 - core) * s.planes),
    ):
        for z in range(s.planes):
            here = base + z
            first = z * (wide + near)
            for start, count, pad, rows, out_ref, source in (
                (first, wide, s.wide, s.length, w_ref, 0),
                (first + wide, near, s.near, s.view_rows, v_ref, s.rows),
            ):
                part = slice(start, start + count)
                out_ref[here, :8] = jnp.zeros((8, s.cols), F32)
                out_ref[here, rows - 8 :] = jnp.zeros((8, s.cols), F32)
                out_ref[here, pad - count : pad] = jnp.where(even, o_x_ref[part], e_x_ref[part])
                out_ref[here, pad : pad + s.rows] = both_ref[z, source : source + s.rows]
                out_ref[here, pad + s.rows : pad + s.rows + count] = jnp.where(even, e_x_ref[part], o_x_ref[part])
    for z in range(s.depth):
        l_ref[z] = tall_split(w_ref[z])
    for rows, group, width, slab_ref, source_ref in (
        (s.length, s.q_wide, s.wide, e_slab_ref, w_ref),
        (s.view_rows, s.q_near, s.near, v_slab_ref, v_ref),
    ):
        lanes = (lane_iota(rows, s.cols) // width + core) % group
        for q in range(s.depth // group):
            packed = source_ref[q * group]
            for p in range(1, group):
                packed = jnp.where(lanes == p, turn(source_ref[q * group + p], p * width), packed)
            slab_ref[q * rows : (q + 1) * rows] = packed


def along_x_kernel(s, l_ref, x_ref, t_ref):
    for z in range(0, s.depth, 2):
        out = fold_rows(dot(x_ref[...], jnp.concatenate([l_ref[z], l_ref[z + 1]], 1)))
        for side in (0, 1):
            t_ref[z + side] = out[:, side * s.cols : (side + 1) * s.cols]


def toeplitz_parts(taps):
    middle = len(taps) // 2
    half = (middle + 1) // 2
    centre = taps[middle - half + 1 : middle + half]
    upper = [p - q for p, q in zip(taps[middle - 2 * half + 1 : middle], centre)]
    lower = [p - q for p, q in zip(taps[middle + 1 : middle + 2 * half], centre)]
    return centre, upper, lower


def kernel_spectrum(
    s, where_ref, psf_in, y_in, x_in, k_ref, ks_ref, kd_ref, pad_ref, a_ref, re_ref, im_ref, psf_ref, y_ref, x_ref, sem_ref
):
    taps = up8(s.extent)
    moves = [
        pltpu.make_async_copy(psf_in.at[pl.ds(where_ref[0], 1)], psf_ref, sem_ref.at[0]),
        pltpu.make_async_copy(y_in, y_ref, sem_ref.at[1]),
        pltpu.make_async_copy(x_in, x_ref, sem_ref.at[2]),
    ]
    for move in moves:
        move.start()
    pad_ref[...] = jnp.zeros_like(pad_ref)
    for move in moves:
        move.wait()
    total = jnp.zeros((s.extent, s.extent), F32)
    for a in range(s.extent):
        total = total + psf_ref[0, a]
    total = jnp.sum(total)
    for a in range(s.extent):
        pad_ref[a * taps : a * taps + s.extent, : s.extent] = psf_ref[0, a] / total
    a_ref[...] = fold(dot(wide_split(pad_ref[...]), y_ref[...]))
    for pair in range((s.extent + 1) // 2):
        columns = []
        for side in (0, 1):
            a = 2 * pair + side
            high, low = split(a_ref[a * taps : (a + 1) * taps])
            columns.append(jnp.concatenate([high, low, high], 0))
        out = dot(x_ref[...], jnp.concatenate(columns, 1))
        for side in (0, 1):
            if 2 * pair + side < s.extent:
                value = out[:, side * s.cols : (side + 1) * s.cols]
                re_ref[2 * pair + side], im_ref[2 * pair + side] = spectrum_of(value[: s.length // 2], value[s.length // 2 :])
    first = s.radius - (s.depth - 1)

    def tile(t, carry):
        rows = pl.ds(t * 8, 8)
        real = [re_ref[a, rows] for a in range(first, first + 2 * s.depth - 1)]
        imag = [im_ref[a, rows] for a in range(first, first + 2 * s.depth - 1)]
        total = [p + q for p, q in zip(real, imag)]
        change = [q - p for p, q in zip(real, imag)]
        for out_ref, values in ((k_ref, real), (ks_ref, total), (kd_ref, change)):
            place = 0
            for part in toeplitz_parts(values):
                for inner in toeplitz_parts(part):
                    for value in inner:
                        out_ref[place, rows] = value
                        place += 1
        return carry

    lax.fori_loop(0, s.length // 16, tile, 0)


def from_side(core, rows, cols, width):
    lanes = lane_iota(rows, cols)
    return jnp.where(core == 0, lanes - (cols - width), width - 1 - lanes) >= 0


def stages(s, k_ref, ks_ref, kd_ref, yf_ref, yi_ref, re_ref, im_ref, pr_ref, pi_ref, a_ref, b_ref, l_ref=None):
    half = s.cols // 2
    depth = s.depth
    group = 4
    freqs = s.length // 2

    def forward_x(rows, x_table):
        for z in range(0, depth, 2):
            both = jnp.concatenate([l_ref[z, : 2 * rows], l_ref[z + 1, : 2 * rows]], 1)
            out = fold_rows(dot(x_table[...], both))
            for side in (0, 1):
                a_ref[z + side] = wide_split(out[:, side * s.cols : (side + 1) * s.cols])

    def forward_y():
        for z in range(0, depth, group):
            out = fold(dot(a_ref[z : z + group].reshape(group * s.length, 2 * s.cols), yf_ref[0]))
            for k in range(group):
                value = out[k * s.length : (k + 1) * s.length]
                re_ref[z + k], im_ref[z + k] = spectrum_of(value[:freqs], value[freqs:])

    def along_z(flip):
        quarter = depth // 4
        order = (lambda z: depth - 1 - z) if flip else (lambda z: z)
        for_re, for_im = (kd_ref, ks_ref) if flip else (ks_ref, kd_ref)

        def parts(x):
            n = len(x) // 2
            return [p + q for p, q in zip(x[:n], x[n:])], x[n:], x[:n]

        def joined(pieces):
            middle, upper, lower = pieces
            return [p + q for p, q in zip(middle, upper)] + [p + q for p, q in zip(middle, lower)]

        def tile(t, carry):
            rows = pl.ds(t * 8, 8)
            real = [re_ref[order(z), rows] for z in range(depth)]
            imag = [im_ref[order(z), rows] for z in range(depth)]
            outer = [parts(x) for x in ([p + q for p, q in zip(real, imag)], imag, real)]
            kept = None
            for part in range(3):
                inner = [parts(x[part]) for x in outer]
                pieces = []
                for piece in range(3):
                    found = []
                    for i in range(quarter):
                        sums = []
                        for table, values in zip((k_ref, for_re, for_im), inner):
                            total = None
                            for j in range(quarter):
                                d = (3 * part + piece) * (2 * quarter - 1) + i - j + quarter - 1
                                term = table[d, rows] * values[piece][j]
                                total = term if total is None else total + term
                            sums.append(total)
                        if flip:
                            found.append((sums[0] + sums[1], sums[0] - sums[2]))
                        else:
                            found.append((sums[0] - sums[1], sums[0] + sums[2]))
                    pieces.append(found)
                value = [joined([[f[k] for f in found] for found in pieces]) for k in (0, 1)]
                if part == 0:
                    kept = value
                else:
                    start = 0 if part == 1 else 2 * quarter
                    for i in range(2 * quarter):
                        pr_ref[order(start + i), rows] = kept[0][i] + value[0][i]
                        pi_ref[order(start + i), rows] = kept[1][i] + value[1][i]
            return carry

        lax.fori_loop(0, freqs // 8, tile, 0)

    def backward(rows, x_table, use):
        half_lanes = lane_iota(freqs, s.cols) < half
        for z in range(0, depth, group):
            pieces = []
            for k in range(group):
                real, imag = pr_ref[z + k], pi_ref[z + k]
                turned_real, turned_imag = turn(real, half), turn(imag, half)
                pieces.append(jnp.where(half_lanes, real + turned_real, imag - turned_imag))
                pieces.append(jnp.where(half_lanes, imag + turned_imag, turned_real - real))
            out = fold(dot(wide_split(jnp.concatenate(pieces, 0)), yi_ref[0]))
            for k in range(group):
                b_ref[z + k] = tall_split(out[k * s.length : (k + 1) * s.length])
        for z in range(0, depth, 2):
            out = fold_rows(dot(x_table[...], jnp.concatenate([b_ref[z], b_ref[z + 1]], 1)))
            for side in (0, 1):
                use(z + side, out[:, side * s.cols : (side + 1) * s.cols])

    return forward_x, forward_y, along_z, backward


def first_kernel(
    s, where_ref, t_in_ref, slab_ref, k_ref, ks_ref, kd_ref, yf_ref, yi_ref, xw_ref, xbn_ref, blurred_ref,
    re_ref, im_ref, pr_ref, pi_ref, a_ref, b_ref,
):
    core = where_ref[1]
    _, forward_y, along_z, backward = stages(
        s, k_ref, ks_ref, kd_ref, yf_ref, yi_ref, re_ref, im_ref, pr_ref, pi_ref, a_ref, b_ref
    )
    arrived = from_side(core, s.length, s.cols, s.wide)
    for q in range(0, s.depth // s.q_wide, 2):
        both = jnp.concatenate([slab_ref[(q + k) * s.length : (q + k + 1) * s.length] for k in (0, 1)], 1)
        out = fold_rows(dot(xw_ref[...], tall_split(both)))
        for k in (0, 1):
            side = out[:, k * s.cols : (k + 1) * s.cols]
            for p in range(s.q_wide):
                z = (q + k) * s.q_wide + p
                a_ref[z] = wide_split(jnp.where(arrived, turn(side, -p * s.wide), t_in_ref[z]))
    forward_y()
    along_z(False)

    def keep(z, blurred):
        blurred_ref[z] = blurred

    backward(s.view_rows, xbn_ref, keep)


def second_kernel(
    s, where_ref, blurred_ref, v_in_ref, own_ref, partner_ref, slab_ref, k_ref, ks_ref, kd_ref, yf_ref, yi_ref,
    xn_ref, xbo_ref, mine_ref, theirs_ref, five_ref,
    re_ref, im_ref, pr_ref, pi_ref, u_ref, t_ref, l_ref, a_ref, b_ref,
):
    core, gx, gy = where_ref[1], where_ref[2], where_ref[3]
    half = s.cols // 2
    depth = s.depth
    forward_x, forward_y, along_z, backward = stages(
        s, k_ref, ks_ref, kd_ref, yf_ref, yi_ref, re_ref, im_ref, pr_ref, pi_ref, a_ref, b_ref, l_ref
    )

    shape = (s.view_rows, s.cols)
    row = lax.broadcasted_iota(jnp.int32, shape, 0) - s.near
    lane = lane_iota(*shape)
    column = lane + jnp.where(core == 0, jnp.where(lane < s.cols - s.near, 0, -s.cols), jnp.where(lane < s.near, s.cols, 0))
    first_row, last_row = -gx * s.rows, (s.gx - gx) * s.rows
    first_column, last_column = -gy * s.cols, (s.gy - gy) * s.cols
    inside = (row >= first_row) & (row < last_row) & (column >= first_column) & (column < last_column)
    begin = core * half - s.near
    inside = inside & (column >= begin) & (column < begin + half + 2 * s.near)

    near_arrived = from_side(core, s.view_rows, s.cols, s.near)
    for z in range(depth):
        safe = jnp.where(inside, blurred_ref[z], 1.0)
        first = z // s.q_near * s.view_rows
        side = turn(slab_ref[first : first + s.view_rows], -(z % s.q_near) * s.near)
        recorded = jnp.where(near_arrived, side, v_in_ref[z])
        l_ref[z, : 2 * s.view_rows] = tall_split(jnp.where(inside, recorded / safe, 0.0))
    forward_x(s.view_rows, xn_ref)
    forward_y()
    along_z(True)

    lane = lane_iota(s.rows, s.cols)
    owned = (lane // half) == core

    def to_update(z, correction):
        plane = z % s.planes
        estimate = jnp.where(core == z // s.planes, own_ref[plane, : s.rows], partner_ref[plane, : s.rows])
        u_ref[z] = jnp.where(owned, estimate * correction, 0.0)

    backward(s.rows, xbo_ref, to_update)

    def three(x):
        high, rest = split(x)
        return high, rest, (x - high.astype(F32) - rest.astype(F32)).astype(BF16)

    def pooled(x, factor, scale):
        count = s.cols // factor
        weights = jnp.where(
            lax.broadcasted_iota(jnp.int32, (s.cols, count), 0) // factor
            == lax.broadcasted_iota(jnp.int32, (s.cols, count), 1),
            scale,
            0.0,
        ).astype(BF16)
        return dot(jnp.concatenate(three(x), 1), jnp.concatenate([weights] * 3, 0))

    u_rows = s.planes * s.rows
    source = u_ref
    planes, rows = depth, s.rows
    sums_of = []
    for level in (1, 2, 3, 4):
        planes, rows = planes // 2, rows // 2
        here = t_ref.at[level - 1]
        for z in range(planes):
            here[z, : 2 * rows] = source[2 * z, : 2 * rows] + source[2 * z + 1, : 2 * rows]
        sums = [
            here[z, pl.ds(0, rows, stride=2)] + here[z, pl.ds(1, rows, stride=2)] for z in range(planes)
        ]
        for z in range(planes):
            here[z, :rows] = sums[z]
        sums_of.append(sums)
        source = here
    levels = []
    for level, sums in enumerate(sums_of, 1):
        factor = 2**level
        value = pooled(jnp.concatenate(sums, 0), factor, 1.0 / factor**3)
        levels.append((value, len(sums), sums[0].shape[0], s.cols // factor))
    top = sums_of[-1][0]
    own_rows = top.shape[0] // 2
    per_chip = s.cols // 32
    line = jnp.concatenate([top[2 * i : 2 * i + 1] + top[2 * i + 1 : 2 * i + 2] for i in range(own_rows)], 1)
    cells = five_ref.shape[2]
    source_lane = lax.broadcasted_iota(jnp.int32, (line.shape[1], cells), 0)
    place = (gx * own_rows + source_lane // s.cols) * (s.gy * per_chip) + gy * per_chip + source_lane % s.cols // 32
    weights = jnp.where(
        place == lax.broadcasted_iota(jnp.int32, place.shape, 1), 1.0 / (32 * 32 * depth), 0.0
    ).astype(BF16)
    five = dot(jnp.concatenate(three(line), 1), jnp.concatenate([weights] * 3, 0))
    five_ref[...] = jnp.broadcast_to(five[None], five_ref.shape)
    for half_index in (0, 1):
        for mine, out_ref in ((True, mine_ref), (False, theirs_ref)):

            @pl.when((core == half_index) == mine)
            def _():
                for z in range(s.planes):
                    out_ref[z * s.rows : (z + 1) * s.rows] = u_ref[half_index * s.planes + z]
                start = u_rows
                for value, planes, rows, columns in levels:
                    count = max(planes * rows // 2, rows)
                    begin = half_index * count if planes > 1 else 0
                    out_ref[start : start + count, :columns] = value[begin : begin + count]
                    start += up8(count)


def last_kernel(s, mine_ref, got_ref, fives_ref, u_ref, one_ref, two_ref, three_ref, four_ref, five_ref):
    for z in range(s.planes):
        part = slice(z * s.rows, (z + 1) * s.rows)
        u_ref[z] = mine_ref[part] + got_ref[part]
    start = s.planes * s.rows
    for out_ref in (one_ref, two_ref, three_ref, four_ref):
        planes, rows, columns = out_ref.shape
        for z in range(planes):
            part = slice(start + z * rows, start + (z + 1) * rows)
            out_ref[z] = mine_ref[part, :columns] + got_ref[part, :columns]
        start += up8(planes * rows)
    rows, columns = five_ref.shape[1:]
    total = jnp.sum(fives_ref[...], axis=0)
    cells = rows * columns
    shape = (rows, cells)
    lane = lane_iota(*shape)
    spread = jnp.where(lane // columns == lax.broadcasted_iota(jnp.int32, shape, 0), jnp.broadcast_to(total, shape), 0.0)
    shape = (cells, columns)
    ones = (lax.broadcasted_iota(jnp.int32, shape, 0) % columns == lane_iota(*shape)).astype(BF16)
    high, rest = split(spread)
    low = (spread - high.astype(F32) - rest.astype(F32)).astype(BF16)
    five_ref[0] = dot(jnp.concatenate([high, rest, low], 1), jnp.concatenate([ones] * 3, 0))


def in_hbm(x):
    return pltpu.with_memory_space_constraint(x, pltpu.HBM)


def whole(shape):
    return pl.BlockSpec(shape, lambda *_: (0,) * len(shape))


def call(body, where, arrays, in_specs, outs, scratch=(), narrow=(), name=None, flops=0, mib=16, copies=()):
    outs = [out if isinstance(out[0], tuple) else (out, F32) for out in outs]
    grid_spec = pltpu.PrefetchScalarGridSpec(
        num_scalar_prefetch=1,
        grid=(1,),
        in_specs=in_specs,
        out_specs=[whole(shape) for shape, _ in outs],
        scratch_shapes=[pltpu.VMEM(shape, F32) for shape in scratch] + [pltpu.VMEM(shape, BF16) for shape in narrow] + list(copies),
    )
    return pl.pallas_call(
        body,
        grid_spec=grid_spec,
        out_shape=[jax.ShapeDtypeStruct(*out) for out in outs],
        compiler_params=pltpu.CompilerParams(vmem_limit_bytes=mib * MIB),
        cost_estimate=pl.CostEstimate(flops=flops, bytes_accessed=0, transcendentals=0) if flops else None,
        name=name,
    )(where, *arrays)


def neighbours(first):
    pairs = []
    for i in range(first, lax.axis_size("gx") - 1, 2):
        pairs += [(i, i + 1), (i + 1, i)]
    return pairs


def to_side():
    pairs = []
    for h in range(lax.axis_size("gy") - 1):
        pairs += [(2 * h + 1, 2 * h + 2), (2 * h + 2, 2 * h + 1)]
    return pairs


def local(estimate, view_data, psf_stack, view_index):
    assert lax.axis_size("gz") == 2
    gx, gy = lax.axis_size("gx"), lax.axis_size("gy")
    s = Sizes(estimate.shape, psf_stack.shape, gx, gy)
    t = {key: jnp.asarray(value) for key, value in tables(s).items()}
    where = jnp.stack(
        [view_index[0], lax.axis_index("gz"), lax.axis_index("gx"), lax.axis_index("gy")]
    ).astype(jnp.int32)

    both_shape = (s.planes, 2 * s.rows, s.cols)
    strip = (s.planes * 3 * s.radius, s.cols)
    outs = [both_shape, strip, strip]
    own, to_even, to_odd = pl.pallas_call(
        functools.partial(send_kernel, s),
        in_specs=[pl.BlockSpec(memory_space=pltpu.HBM)] * 2,
        out_specs=[pl.BlockSpec(memory_space=pltpu.VMEM)] * len(outs),
        out_shape=[jax.ShapeDtypeStruct(shape, F32) for shape in outs],
        scratch_shapes=[pltpu.SemaphoreType.DMA((2,))],
        compiler_params=pltpu.CompilerParams(vmem_limit_bytes=8 * MIB),
        name="send",
    )(in_hbm(estimate), in_hbm(view_data))
    across = [(0, 1), (1, 0)]
    partner = lax.ppermute(own, "gz", across)
    even = lax.ppermute(to_even, "gx", neighbours(0))
    odd = lax.ppermute(to_odd, "gx", neighbours(1))
    psf_shape = (1,) + psf_stack.shape[1:]
    taps = up8(s.extent)
    k, ks, kd = call(
        functools.partial(kernel_spectrum, s),
        where,
        (in_hbm(psf_stack), in_hbm(t["y_kernel"]), in_hbm(t["x_kernel"])),
        [pl.BlockSpec(memory_space=pltpu.HBM)] * 3,
        [(9 * (s.depth // 2 - 1), s.length // 2, s.cols)] * 3,
        scratch=[((s.extent + 1) // 2 * 2 * taps, s.cols)] * 2 + [(s.extent, s.length // 2, s.cols)] * 2 + [psf_shape],
        narrow=[t["y_kernel"].shape, t["x_kernel"].shape],
        copies=[pltpu.SemaphoreType.DMA((3,))],
        name="kernel_spectrum",
        flops=10**8,
    )
    even, _ = lax.optimization_barrier((even, k))
    even_partner = lax.ppermute(even, "gz", across)
    odd, _ = lax.optimization_barrier((odd, even_partner))
    odd_partner = lax.ppermute(odd, "gz", across)
    arrays = (own, partner, even, odd, even_partner, odd_partner)
    window = (s.depth, s.length, s.cols)
    view_window = (s.depth, s.view_rows, s.cols)
    split_window, view_here, slab, view_slab = call(
        functools.partial(pack_kernel, s),
        where,
        arrays + (k,),
        [whole(a.shape) for a in arrays] + [pl.BlockSpec(memory_space=pl.ANY)],
        [((s.depth, 2 * s.length, s.cols), BF16), view_window, (s.pack_e, s.cols), (s.pack_v, s.cols)],
        scratch=[window],
        name="pack",
    )
    view_slab = lax.ppermute(view_slab, ("gy", "gz"), to_side())
    slab = lax.ppermute(slab, ("gy", "gz"), to_side())
    along_x = pl.pallas_call(
        functools.partial(along_x_kernel, s),
        out_shape=jax.ShapeDtypeStruct(window, F32),
        compiler_params=pltpu.CompilerParams(vmem_limit_bytes=16 * MIB),
        cost_estimate=pl.CostEstimate(flops=10**8, bytes_accessed=0, transcendentals=0),
        name="along_x",
    )(split_window, t["x_window"])

    u_rows = s.planes * s.rows
    out_rows = u_rows
    level_shapes = []
    planes, rows, columns = s.depth, s.rows, s.cols
    for _ in range(4):
        planes, rows, columns = planes // 2, rows // 2, columns // 2
        level_shapes.append((max(planes // 2, 1), rows, columns))
        out_rows += up8(level_shapes[-1][0] * rows)
    devices = 2 * gx * gy
    five_shape = (rows // 2 * gx, columns // 2 * gy)
    spectra = [(s.depth, s.length // 2, s.cols)] * 4
    halves = [(s.depth, s.length, 2 * s.cols), (s.depth, 2 * s.length, s.cols)]

    def of_core(x):
        return pl.BlockSpec((1,) + x.shape[1:], lambda i, w: (w[1], 0, 0))

    tables_of = (k, ks, kd, t["y_forward"], t["y_inverse"])
    tables_specs = [whole(a.shape) for a in tables_of[:3]] + [of_core(a) for a in tables_of[3:]]
    before, after = (along_x, slab), (t["x_window"], t["x_back_near"])
    (blurred,) = call(
        functools.partial(first_kernel, s),
        where,
        before + tables_of + after,
        [whole(a.shape) for a in before] + tables_specs + [whole(a.shape) for a in after],
        [view_window],
        scratch=spectra,
        narrow=halves,
        name="blur",
        mib=24,
        flops=10**8,
    )
    before, after = (blurred, view_here, own, partner, view_slab), (t["x_near"], t["x_back_own"])
    mine, theirs, five = call(
        functools.partial(second_kernel, s),
        where,
        before + tables_of + after,
        [whole(a.shape) for a in before] + tables_specs + [whole(a.shape) for a in after],
        [(out_rows, s.cols), (out_rows, s.cols), (devices, 1, five_shape[0] * five_shape[1])],
        scratch=spectra + [(s.depth, s.rows, s.cols), (4, s.depth // 2, s.rows, s.cols)],
        narrow=[(s.depth, 2 * s.view_rows, s.cols)] + halves,
        name="update",
        mib=24,
    )
    got = lax.ppermute(theirs, "gz", [(0, 1), (1, 0)])
    fives = lax.all_to_all(five, ALL, split_axis=0, concat_axis=0, tiled=True)
    outs = [estimate.shape] + level_shapes + [(1,) + five_shape]
    arrays = (mine, got, fives)
    return tuple(
        pl.pallas_call(
            functools.partial(last_kernel, s),
            in_specs=[whole(a.shape) for a in arrays],
            out_specs=[whole(shape) for shape in outs],
            out_shape=[jax.ShapeDtypeStruct(shape, F32) for shape in outs],
            grid=(1,),
            compiler_params=pltpu.CompilerParams(vmem_limit_bytes=8 * MIB),
            name="assemble",
        )(*arrays)
    )


def solution(mesh):
    return jax.shard_map(
        local,
        mesh=mesh,
        in_specs=(P("gz", "gx", "gy"), P("gz", "gx", "gy"), P(), P()),
        out_specs=(
            P("gz", "gx", "gy"),
            P("gz", "gx", "gy"),
            P("gz", "gx", "gy"),
            P("gz", "gx", "gy"),
            P(None, "gx", "gy"),
            P(),
        ),
        check_vma=False,
    )
```

```python
import functools

import jax
import jax.numpy as jnp
import ml_dtypes
import numpy as np
from jax import lax
from jax.experimental import pallas as pl
from jax.experimental.pallas import tpu as pltpu
from jax.sharding import PartitionSpec as P


F32 = jnp.float32
BF16 = jnp.bfloat16
ALL = ("gx", "gy", "gz")
MIB = 1024 * 1024


def up8(count):
    return (count + 7) // 8 * 8


class Sizes:
    def __init__(self, estimate_shape, psf_shape, gx, gy):
        self.planes, self.rows, self.cols = estimate_shape
        self.extent = psf_shape[1]
        self.radius = (self.extent - 1) // 2
        self.depth = 2 * self.planes
        self.half = self.cols // 2
        self.wide = up8(2 * self.radius)
        self.near = up8(self.radius)
        self.length = self.rows + 2 * self.wide
        self.view_rows = self.rows + 2 * self.near
        self.freqs = self.cols // 2
        self.q_wide = self.cols // self.wide
        self.q_near = self.cols // self.near
        self.pack_e = self.depth // self.q_wide * self.length
        self.pack_v = self.depth // self.q_near * self.view_rows
        self.gx, self.gy = gx, gy
        assert self.half + 2 * self.wide == self.cols == 128
        assert self.wide <= self.rows and self.depth % self.q_near == 0
        assert self.depth == 16


def split_np(matrix):
    high = matrix.astype(np.float32).astype(ml_dtypes.bfloat16)
    low = (matrix - high.astype(np.float64)).astype(np.float32).astype(ml_dtypes.bfloat16)
    return high, low


def lane_positions(s, core):
    lanes = np.arange(s.cols)
    return (lanes + s.wide) % s.cols if core == 0 else (lanes - s.wide) % s.cols


def right_pair(matrix):
    high, low = split_np(matrix)
    return np.block([[high, low], [high, np.zeros_like(low)]])


def left_pair(matrix):
    high, low = split_np(matrix)
    return np.block([[high, high], [low, np.zeros_like(low)]])


def tables(s):
    y_freq = 2.0 * np.pi * (np.arange(s.freqs) + 0.5) / s.cols
    x_freq = 2.0 * np.pi * (np.arange(s.length // 2) + 0.5) / s.length
    y_forward, y_inverse = [], []
    for core in (0, 1):
        angle = lane_positions(s, core)[:, None] * y_freq[None, :]
        both = np.concatenate([np.cos(angle), np.sin(angle)], 1)
        y_forward.append(right_pair(both))
        y_inverse.append(right_pair(both.T * (2.0 / s.cols / s.length)))
    offset = np.arange(s.cols) - s.radius
    angle = offset[:, None] * y_freq[None, :]
    y_kernel = np.concatenate([np.cos(angle), np.sin(angle)], 1)
    y_kernel[s.extent :] = 0.0

    def x_forward(positions):
        angle = x_freq[:, None] * positions[None, :]
        return np.concatenate([np.cos(angle), np.sin(angle)], 0)

    def x_inverse(positions):
        angle = positions[:, None] * x_freq[None, :]
        return np.concatenate([np.cos(angle), -np.sin(angle)], 1)

    window = np.arange(s.length) - s.wide
    near = np.arange(s.view_rows) - s.near
    own = np.arange(s.rows)
    taps = np.arange(up8(s.extent)) - s.radius
    high, low = split_np(x_forward(taps))
    x_kernel = np.concatenate([high, high, low], 1)
    return dict(
        y_forward=np.stack(y_forward),
        y_inverse=np.stack(y_inverse),
        y_kernel=right_pair(y_kernel),
        x_window=left_pair(x_forward(window)),
        x_near=left_pair(x_forward(near)),
        x_back_near=left_pair(x_inverse(near)),
        x_back_own=left_pair(x_inverse(own)),
        x_kernel=x_kernel,
    )


def split(x):
    high = x.astype(BF16)
    return high, (x - high.astype(F32)).astype(BF16)


def dot(a, b):
    return lax.dot_general(a, b, (((1,), (0,)), ((), ())), preferred_element_type=F32)


def lane_iota(rows, cols):
    return lax.broadcasted_iota(jnp.int32, (rows, cols), 1)


def turn(x, shift):
    shift %= x.shape[1]
    return pltpu.roll(x, shift, 1) if shift else x


def wide_split(x):
    return jnp.concatenate(split(x), 1)


def tall_split(x):
    return jnp.concatenate(split(x), 0)


def fold(both):
    width = both.shape[1] // 2
    return both[:, :width] + both[:, width:]


def fold_rows(both):
    count = both.shape[0] // 2
    return both[:count] + both[count:]


def spectrum_of(cosine, sine):
    half = cosine.shape[1] // 2
    left = lane_iota(*cosine.shape) < half
    moved = turn(sine, half)
    minus, plus = cosine - moved, turn(cosine + moved, half)
    return jnp.where(left, minus, plus), jnp.where(left, -plus, minus)


def send_kernel(s, e_in, v_in, e_ref, v_ref, even_ref, odd_ref, sem_ref):
    moves = [
        pltpu.make_async_copy(e_in, e_ref, sem_ref.at[0]),
        pltpu.make_async_copy(v_in, v_ref, sem_ref.at[1]),
    ]
    for move in moves:
        move.start()
    even = lax.axis_index("gx") % 2 == 0
    for move in moves:
        move.wait()
    for ref, begin, count in ((e_ref, 0, 2 * s.radius), (v_ref, s.planes * 2 * s.radius, s.radius)):
        for z in range(s.planes):
            low, high = ref[z, :count], ref[z, s.rows - count :]
            part = slice(begin + z * count, begin + (z + 1) * count)
            even_ref[part] = jnp.where(even, high, low)
            odd_ref[part] = jnp.where(even, low, high)


def pack(s, begin, count, pad, group, mine, partners, window_ref, slab_ref):
    core = lax.axis_index("gz")
    even = lax.axis_index("gx") % 2 == 0
    rows = s.rows + 2 * pad
    for (body_ref, even_ref, odd_ref), base in ((mine, core * s.planes), (partners, (1 - core) * s.planes)):
        for z in range(s.planes):
            here = base + z
            part = slice(begin + z * count, begin + (z + 1) * count)
            window_ref[here, :8] = jnp.zeros((8, s.cols), F32)
            window_ref[here, rows - 8 :] = jnp.zeros((8, s.cols), F32)
            window_ref[here, pad - count : pad] = jnp.where(even, odd_ref[part], even_ref[part])
            window_ref[here, pad : pad + s.rows] = body_ref[z]
            window_ref[here, pad + s.rows : pad + s.rows + count] = jnp.where(even, even_ref[part], odd_ref[part])
    lanes = (lane_iota(rows, s.cols) // pad + core) % group
    for q in range(s.depth // group):
        packed = window_ref[q * group]
        for p in range(1, group):
            packed = jnp.where(lanes == p, turn(window_ref[q * group + p], p * pad), packed)
        slab_ref[q * rows : (q + 1) * rows] = packed


def pack_estimate(s, e_ref, e2_ref, even_ref, odd_ref, even2_ref, odd2_ref, l_ref, slab_ref, w_ref):
    pack(
        s, 0, 2 * s.radius, s.wide, s.q_wide, (e_ref, even_ref, odd_ref), (e2_ref, even2_ref, odd2_ref), w_ref, slab_ref
    )
    for z in range(s.depth):
        l_ref[z] = tall_split(w_ref[z])


def pack_view(s, v_ref, v2_ref, even_ref, odd_ref, even2_ref, odd2_ref, after_ref, window_ref, slab_ref):
    begin = s.planes * 2 * s.radius
    pack(s, begin, s.radius, s.near, s.q_near, (v_ref, even_ref, odd_ref), (v2_ref, even2_ref, odd2_ref), window_ref, slab_ref)


def along_x_kernel(s, l_ref, x_ref, t_ref):
    for z in range(0, s.depth, 2):
        out = fold_rows(dot(x_ref[...], jnp.concatenate([l_ref[z], l_ref[z + 1]], 1)))
        for side in (0, 1):
            t_ref[z + side] = out[:, side * s.cols : (side + 1) * s.cols]


def toeplitz_parts(taps):
    middle = len(taps) // 2
    half = (middle + 1) // 2
    centre = taps[middle - half + 1 : middle + half]
    upper = [p - q for p, q in zip(taps[middle - 2 * half + 1 : middle], centre)]
    lower = [p - q for p, q in zip(taps[middle + 1 : middle + 2 * half], centre)]
    return centre, upper, lower


def kernel_spectrum(
    s, view_ref, psf_in, y_in, x_in, re_ref, im_ref, pad_ref, a_ref, psf_ref, y_ref, x_ref, sem_ref
):
    taps = up8(s.extent)
    moves = [
        pltpu.make_async_copy(psf_in.at[pl.ds(view_ref[0], 1)], psf_ref, sem_ref.at[0]),
        pltpu.make_async_copy(y_in, y_ref, sem_ref.at[1]),
        pltpu.make_async_copy(x_in, x_ref, sem_ref.at[2]),
    ]
    for move in moves:
        move.start()
    pad_ref[...] = jnp.zeros_like(pad_ref)
    for move in moves:
        move.wait()
    total = jnp.zeros((s.extent, s.extent), F32)
    for a in range(s.extent):
        total = total + psf_ref[0, a]
    total = jnp.sum(total)
    for a in range(s.extent):
        pad_ref[a * taps : a * taps + s.extent, : s.extent] = psf_ref[0, a] / total
    a_ref[...] = fold(dot(wide_split(pad_ref[...]), y_ref[...]))
    for pair in range((s.extent + 1) // 2):
        columns = []
        for side in (0, 1):
            a = 2 * pair + side
            high, low = split(a_ref[a * taps : (a + 1) * taps])
            columns.append(jnp.concatenate([high, low, high], 0))
        out = dot(x_ref[...], jnp.concatenate(columns, 1))
        for side in (0, 1):
            if 2 * pair + side < s.extent:
                value = out[:, side * s.cols : (side + 1) * s.cols]
                re_ref[2 * pair + side], im_ref[2 * pair + side] = spectrum_of(value[: s.length // 2], value[s.length // 2 :])


def kernel_leaves(s, re_ref, im_ref, k_ref, ks_ref, kd_ref):
    first = s.radius - (s.depth - 1)

    def tile(t, carry):
        rows = pl.ds(t * 8, 8)
        real = [re_ref[a, rows] for a in range(first, first + 2 * s.depth - 1)]
        imag = [im_ref[a, rows] for a in range(first, first + 2 * s.depth - 1)]
        total = [p + q for p, q in zip(real, imag)]
        change = [q - p for p, q in zip(real, imag)]
        for out_ref, values in ((k_ref, real), (ks_ref, total), (kd_ref, change)):
            place = 0
            for part in toeplitz_parts(values):
                for inner in toeplitz_parts(part):
                    for value in inner:
                        out_ref[place, rows] = value
                        place += 1
        return carry

    lax.fori_loop(0, s.length // 16, tile, 0)


def from_side(core, rows, cols, width):
    lanes = lane_iota(rows, cols)
    return jnp.where(core == 0, lanes - (cols - width), width - 1 - lanes) >= 0


def stages(s, k_ref, ks_ref, kd_ref, yf_ref, yi_ref, re_ref, im_ref, pr_ref, pi_ref, a_ref, b_ref, l_ref=None):
    half = s.cols // 2
    depth = s.depth
    group = 4
    freqs = s.length // 2

    def forward_x(rows, x_table):
        for z in range(0, depth, 2):
            both = jnp.concatenate([l_ref[z, : 2 * rows], l_ref[z + 1, : 2 * rows]], 1)
            out = fold_rows(dot(x_table[...], both))
            for side in (0, 1):
                a_ref[z + side] = wide_split(out[:, side * s.cols : (side + 1) * s.cols])

    def forward_y():
        for z in range(0, depth, group):
            out = fold(dot(a_ref[z : z + group].reshape(group * s.length, 2 * s.cols), yf_ref[lax.axis_index("gz")]))
            for k in range(group):
                value = out[k * s.length : (k + 1) * s.length]
                re_ref[z + k], im_ref[z + k] = spectrum_of(value[:freqs], value[freqs:])

    def along_z(flip):
        quarter = depth // 4
        order = (lambda z: depth - 1 - z) if flip else (lambda z: z)
        for_re, for_im = (kd_ref, ks_ref) if flip else (ks_ref, kd_ref)

        def parts(x):
            n = len(x) // 2
            return [p + q for p, q in zip(x[:n], x[n:])], x[n:], x[:n]

        def joined(pieces):
            middle, upper, lower = pieces
            return [p + q for p, q in zip(middle, upper)] + [p + q for p, q in zip(middle, lower)]

        def tile(t, carry):
            rows = pl.ds(t * 8, 8)
            real = [re_ref[order(z), rows] for z in range(depth)]
            imag = [im_ref[order(z), rows] for z in range(depth)]
            outer = [parts(x) for x in ([p + q for p, q in zip(real, imag)], imag, real)]
            kept = None
            for part in range(3):
                inner = [parts(x[part]) for x in outer]
                pieces = []
                for piece in range(3):
                    found = []
                    for i in range(quarter):
                        sums = []
                        for table, values in zip((k_ref, for_re, for_im), inner):
                            total = None
                            for j in range(quarter):
                                d = (3 * part + piece) * (2 * quarter - 1) + i - j + quarter - 1
                                term = table[d, rows] * values[piece][j]
                                total = term if total is None else total + term
                            sums.append(total)
                        if flip:
                            found.append((sums[0] + sums[1], sums[0] - sums[2]))
                        else:
                            found.append((sums[0] - sums[1], sums[0] + sums[2]))
                    pieces.append(found)
                value = [joined([[f[k] for f in found] for found in pieces]) for k in (0, 1)]
                if part == 0:
                    kept = value
                else:
                    start = 0 if part == 1 else 2 * quarter
                    for i in range(2 * quarter):
                        pr_ref[order(start + i), rows] = kept[0][i] + value[0][i]
                        pi_ref[order(start + i), rows] = kept[1][i] + value[1][i]
            return carry

        lax.fori_loop(0, freqs // 8, tile, 0)

    def backward(rows, x_table, use):
        half_lanes = lane_iota(freqs, s.cols) < half
        for z in range(0, depth, group):
            pieces = []
            for k in range(group):
                real, imag = pr_ref[z + k], pi_ref[z + k]
                turned_real, turned_imag = turn(real, half), turn(imag, half)
                pieces.append(jnp.where(half_lanes, real + turned_real, imag - turned_imag))
                pieces.append(jnp.where(half_lanes, imag + turned_imag, turned_real - real))
            out = fold(dot(wide_split(jnp.concatenate(pieces, 0)), yi_ref[lax.axis_index("gz")]))
            for k in range(group):
                b_ref[z + k] = tall_split(out[k * s.length : (k + 1) * s.length])
        for z in range(0, depth, 2):
            out = fold_rows(dot(x_table[...], jnp.concatenate([b_ref[z], b_ref[z + 1]], 1)))
            for side in (0, 1):
                use(z + side, out[:, side * s.cols : (side + 1) * s.cols])

    return forward_x, forward_y, along_z, backward


def first_kernel(
    s, t_in_ref, slab_ref, k_ref, ks_ref, kd_ref, yf_ref, yi_ref, xw_ref, xbn_ref, blurred_ref,
    re_ref, im_ref, pr_ref, pi_ref, a_ref, b_ref,
):
    core = lax.axis_index("gz")
    _, forward_y, along_z, backward = stages(
        s, k_ref, ks_ref, kd_ref, yf_ref, yi_ref, re_ref, im_ref, pr_ref, pi_ref, a_ref, b_ref
    )
    arrived = from_side(core, s.length, s.cols, s.wide)
    for q in range(0, s.depth // s.q_wide, 2):
        both = jnp.concatenate([slab_ref[(q + k) * s.length : (q + k + 1) * s.length] for k in (0, 1)], 1)
        out = fold_rows(dot(xw_ref[...], tall_split(both)))
        for k in (0, 1):
            side = out[:, k * s.cols : (k + 1) * s.cols]
            for p in range(s.q_wide):
                z = (q + k) * s.q_wide + p
                a_ref[z] = wide_split(jnp.where(arrived, turn(side, -p * s.wide), t_in_ref[z]))
    forward_y()
    along_z(False)

    def keep(z, blurred):
        blurred_ref[z] = blurred

    backward(s.view_rows, xbn_ref, keep)


def second_kernel(
    s, blurred_ref, v_in_ref, own_ref, partner_ref, slab_ref, k_ref, ks_ref, kd_ref, yf_ref, yi_ref,
    xn_ref, xbo_ref, mine_ref, theirs_ref, five_ref,
    re_ref, im_ref, pr_ref, pi_ref, u_ref, t_ref, l_ref, a_ref, b_ref,
):
    core, gx, gy = lax.axis_index("gz"), lax.axis_index("gx"), lax.axis_index("gy")
    half = s.cols // 2
    depth = s.depth
    forward_x, forward_y, along_z, backward = stages(
        s, k_ref, ks_ref, kd_ref, yf_ref, yi_ref, re_ref, im_ref, pr_ref, pi_ref, a_ref, b_ref, l_ref
    )

    shape = (s.view_rows, s.cols)
    row = lax.broadcasted_iota(jnp.int32, shape, 0) - s.near
    lane = lane_iota(*shape)
    column = lane + jnp.where(core == 0, jnp.where(lane < s.cols - s.near, 0, -s.cols), jnp.where(lane < s.near, s.cols, 0))
    first_row, last_row = -gx * s.rows, (s.gx - gx) * s.rows
    first_column, last_column = -gy * s.cols, (s.gy - gy) * s.cols
    inside = (row >= first_row) & (row < last_row) & (column >= first_column) & (column < last_column)
    begin = core * half - s.near
    inside = inside & (column >= begin) & (column < begin + half + 2 * s.near)

    near_arrived = from_side(core, s.view_rows, s.cols, s.near)
    for z in range(depth):
        safe = jnp.where(inside, blurred_ref[z], 1.0)
        first = z // s.q_near * s.view_rows
        side = turn(slab_ref[first : first + s.view_rows], -(z % s.q_near) * s.near)
        recorded = jnp.where(near_arrived, side, v_in_ref[z])
        l_ref[z, : 2 * s.view_rows] = tall_split(jnp.where(inside, recorded / safe, 0.0))
    forward_x(s.view_rows, xn_ref)
    forward_y()
    along_z(True)

    lane = lane_iota(s.rows, s.cols)
    owned = (lane // half) == core

    def to_update(z, correction):
        plane = z % s.planes
        estimate = jnp.where(core == z // s.planes, own_ref[plane], partner_ref[plane])
        u_ref[z] = jnp.where(owned, estimate * correction, 0.0)

    backward(s.rows, xbo_ref, to_update)

    def three(x):
        high, rest = split(x)
        return high, rest, (x - high.astype(F32) - rest.astype(F32)).astype(BF16)

    def pooled(x, factor, scale):
        count = s.cols // factor
        weights = jnp.where(
            lax.broadcasted_iota(jnp.int32, (s.cols, count), 0) // factor
            == lax.broadcasted_iota(jnp.int32, (s.cols, count), 1),
            scale,
            0.0,
        ).astype(BF16)
        return dot(jnp.concatenate(three(x), 1), jnp.concatenate([weights] * 3, 0))

    u_rows = s.planes * s.rows
    source = u_ref
    planes, rows = depth, s.rows
    sums_of = []
    for level in (1, 2, 3, 4):
        planes, rows = planes // 2, rows // 2
        here = t_ref.at[level - 1]
        for z in range(planes):
            here[z, : 2 * rows] = source[2 * z, : 2 * rows] + source[2 * z + 1, : 2 * rows]
        sums = [
            here[z, pl.ds(0, rows, stride=2)] + here[z, pl.ds(1, rows, stride=2)] for z in range(planes)
        ]
        for z in range(planes):
            here[z, :rows] = sums[z]
        sums_of.append(sums)
        source = here
    levels = []
    for level, sums in enumerate(sums_of, 1):
        factor = 2**level
        value = pooled(jnp.concatenate(sums, 0), factor, 1.0 / factor**3)
        levels.append((value, len(sums), sums[0].shape[0], s.cols // factor))
    top = sums_of[-1][0]
    own_rows = top.shape[0] // 2
    per_chip = s.cols // 32
    line = jnp.concatenate([top[2 * i : 2 * i + 1] + top[2 * i + 1 : 2 * i + 2] for i in range(own_rows)], 1)
    cells = five_ref.shape[2]
    source_lane = lax.broadcasted_iota(jnp.int32, (line.shape[1], cells), 0)
    place = (gx * own_rows + source_lane // s.cols) * (s.gy * per_chip) + gy * per_chip + source_lane % s.cols // 32
    weights = jnp.where(
        place == lax.broadcasted_iota(jnp.int32, place.shape, 1), 1.0 / (32 * 32 * depth), 0.0
    ).astype(BF16)
    five = dot(jnp.concatenate(three(line), 1), jnp.concatenate([weights] * 3, 0))
    five_ref[...] = jnp.broadcast_to(five[None], five_ref.shape)
    for half_index in (0, 1):
        for mine, out_ref in ((True, mine_ref), (False, theirs_ref)):

            @pl.when((core == half_index) == mine)
            def _():
                for z in range(s.planes):
                    out_ref[z * s.rows : (z + 1) * s.rows] = u_ref[half_index * s.planes + z]
                start = u_rows
                for value, planes, rows, columns in levels:
                    count = max(planes * rows // 2, rows)
                    begin = half_index * count if planes > 1 else 0
                    out_ref[start : start + count, :columns] = value[begin : begin + count]
                    start += up8(count)


def last_kernel(s, mine_ref, got_ref, fives_ref, u_ref, one_ref, two_ref, three_ref, four_ref, five_ref):
    for z in range(s.planes):
        part = slice(z * s.rows, (z + 1) * s.rows)
        u_ref[z] = mine_ref[part] + got_ref[part]
    start = s.planes * s.rows
    for out_ref in (one_ref, two_ref, three_ref, four_ref):
        planes, rows, columns = out_ref.shape
        for z in range(planes):
            part = slice(start + z * rows, start + (z + 1) * rows)
            out_ref[z] = mine_ref[part, :columns] + got_ref[part, :columns]
        start += up8(planes * rows)
    rows, columns = five_ref.shape[1:]
    total = jnp.sum(fives_ref[...], axis=0)
    cells = rows * columns
    shape = (rows, cells)
    lane = lane_iota(*shape)
    spread = jnp.where(lane // columns == lax.broadcasted_iota(jnp.int32, shape, 0), jnp.broadcast_to(total, shape), 0.0)
    shape = (cells, columns)
    ones = (lax.broadcasted_iota(jnp.int32, shape, 0) % columns == lane_iota(*shape)).astype(BF16)
    high, rest = split(spread)
    low = (spread - high.astype(F32) - rest.astype(F32)).astype(BF16)
    five_ref[0] = dot(jnp.concatenate([high, rest, low], 1), jnp.concatenate([ones] * 3, 0))


def in_hbm(x):
    return pltpu.with_memory_space_constraint(x, pltpu.HBM)


def call(body, arrays, outs, scratch=(), narrow=(), copies=(), mib=16, flops=10**7, prefetch=(), where=None):
    outs = [out if isinstance(out[0], tuple) else (out, F32) for out in outs]
    return pl.pallas_call(
        body,
        grid_spec=pltpu.PrefetchScalarGridSpec(
            num_scalar_prefetch=len(prefetch),
            in_specs=[pl.BlockSpec(memory_space=where or pltpu.VMEM)] * len(arrays),
            out_specs=[pl.BlockSpec(memory_space=pltpu.VMEM)] * len(outs),
            scratch_shapes=[pltpu.VMEM(shape, F32) for shape in scratch]
            + [pltpu.VMEM(shape, BF16) for shape in narrow]
            + list(copies),
        ),
        out_shape=[jax.ShapeDtypeStruct(*out) for out in outs],
        compiler_params=pltpu.CompilerParams(vmem_limit_bytes=mib * MIB),
        cost_estimate=pl.CostEstimate(flops=flops, bytes_accessed=0, transcendentals=0),
    )(*prefetch, *arrays)


def neighbours(first):
    pairs = []
    for i in range(first, lax.axis_size("gx") - 1, 2):
        pairs += [(i, i + 1), (i + 1, i)]
    return pairs


def to_side():
    pairs = []
    for h in range(lax.axis_size("gy") - 1):
        pairs += [(2 * h + 1, 2 * h + 2), (2 * h + 2, 2 * h + 1)]
    return pairs


def local(estimate, view_data, psf_stack, view_index):
    assert lax.axis_size("gz") == 2
    gx, gy = lax.axis_size("gx"), lax.axis_size("gy")
    s = Sizes(estimate.shape, psf_stack.shape, gx, gy)
    t = {key: jnp.asarray(value) for key, value in tables(s).items()}
    across = [(0, 1), (1, 0)]
    strip = (s.planes * 3 * s.radius, s.cols)
    own, own_view, even, odd = call(
        functools.partial(send_kernel, s),
        (in_hbm(estimate), in_hbm(view_data)),
        [estimate.shape, estimate.shape, strip, strip],
        copies=[pltpu.SemaphoreType.DMA((2,))],
        mib=8,
        where=pltpu.HBM,
    )
    even = lax.ppermute(even, "gx", neighbours(0))
    odd = lax.ppermute(odd, "gx", neighbours(1))
    partner = lax.ppermute(own, "gz", across)
    partner_view = lax.ppermute(own_view, "gz", across)

    taps = up8(s.extent)
    psf_shape = (1,) + psf_stack.shape[1:]
    kernel_planes = (s.extent, s.length // 2, s.cols)
    re, im = call(
        functools.partial(kernel_spectrum, s),
        (in_hbm(psf_stack), in_hbm(t["y_kernel"]), in_hbm(t["x_kernel"])),
        [kernel_planes] * 2,
        scratch=[((s.extent + 1) // 2 * 2 * taps, s.cols)] * 2 + [psf_shape],
        narrow=[t["y_kernel"].shape, t["x_kernel"].shape],
        copies=[pltpu.SemaphoreType.DMA((3,))],
        prefetch=(view_index,),
        where=pltpu.HBM,
    )
    k, ks, kd = call(
        functools.partial(kernel_leaves, s), (re, im), [(9 * (s.depth // 2 - 1), s.length // 2, s.cols)] * 3
    )

    even, _ = lax.optimization_barrier((even, re))
    even2 = lax.ppermute(even, "gz", across)
    odd, _ = lax.optimization_barrier((odd, (even2, k)))
    odd2 = lax.ppermute(odd, "gz", across)
    window = (s.depth, s.length, s.cols)
    view_window = (s.depth, s.view_rows, s.cols)
    split_window, slab = call(
        functools.partial(pack_estimate, s),
        (own, partner, even, odd, even2, odd2),
        [((s.depth, 2 * s.length, s.cols), BF16), (s.pack_e, s.cols)],
        scratch=[window],
    )
    slab_here = slab
    slab = lax.ppermute(slab, ("gy", "gz"), to_side())
    view_here, view_slab = call(
        functools.partial(pack_view, s),
        (own_view, partner_view, even, odd, even2, odd2, slab_here),
        [view_window, (s.pack_v, s.cols)],
    )
    view_slab = lax.ppermute(view_slab, ("gy", "gz"), to_side())
    (along_x,) = call(functools.partial(along_x_kernel, s), (split_window, t["x_window"]), [window])

    u_rows = s.planes * s.rows
    out_rows = u_rows
    level_shapes = []
    planes, rows, columns = s.depth, s.rows, s.cols
    for _ in range(4):
        planes, rows, columns = planes // 2, rows // 2, columns // 2
        level_shapes.append((max(planes // 2, 1), rows, columns))
        out_rows += up8(level_shapes[-1][0] * rows)
    devices = 2 * gx * gy
    five_shape = (rows // 2 * gx, columns // 2 * gy)
    spectra = [(s.depth, s.length // 2, s.cols)] * 4
    halves = [(s.depth, s.length, 2 * s.cols), (s.depth, 2 * s.length, s.cols)]
    shared = (k, ks, kd, t["y_forward"], t["y_inverse"])
    (blurred,) = call(
        functools.partial(first_kernel, s),
        (along_x, slab) + shared + (t["x_window"], t["x_back_near"]),
        [view_window],
        scratch=spectra,
        narrow=halves,
        mib=24,
        flops=10**8,
    )
    mine, theirs, five = call(
        functools.partial(second_kernel, s),
        (blurred, view_here, own, partner, view_slab) + shared + (t["x_near"], t["x_back_own"]),
        [(out_rows, s.cols), (out_rows, s.cols), (devices, 1, five_shape[0] * five_shape[1])],
        scratch=spectra + [(s.depth, s.rows, s.cols), (4, s.depth // 2, s.rows, s.cols)],
        narrow=[(s.depth, 2 * s.view_rows, s.cols)] + halves,
        mib=24,
    )
    got = lax.ppermute(theirs, "gz", across)
    fives = lax.all_to_all(five, ALL, split_axis=0, concat_axis=0, tiled=True)
    return tuple(
        call(
            functools.partial(last_kernel, s),
            (mine, got, fives),
            [estimate.shape] + level_shapes + [(1,) + five_shape],
            mib=8,
        )
    )


def solution(mesh):
    return jax.shard_map(
        local,
        mesh=mesh,
        in_specs=(P("gz", "gx", "gy"), P("gz", "gx", "gy"), P(), P()),
        out_specs=(
            P("gz", "gx", "gy"),
            P("gz", "gx", "gy"),
            P("gz", "gx", "gy"),
            P("gz", "gx", "gy"),
            P(None, "gx", "gy"),
            P(),
        ),
        check_vma=False,
    )
```

```python
import functools

import jax
import jax.numpy as jnp
import ml_dtypes
import numpy as np
from jax import lax
from jax.experimental import pallas as pl
from jax.experimental.pallas import tpu as pltpu
from jax.sharding import PartitionSpec as P


F32 = jnp.float32
BF16 = jnp.bfloat16
ALL = ("gx", "gy", "gz")
MIB = 1024 * 1024


def up8(count):
    return (count + 7) // 8 * 8


class Sizes:
    def __init__(self, estimate_shape, psf_shape, gx, gy):
        self.planes, self.rows, self.cols = estimate_shape
        self.extent = psf_shape[1]
        self.radius = (self.extent - 1) // 2
        self.depth = 2 * self.planes
        self.half = self.cols // 2
        self.wide = up8(2 * self.radius)
        self.near = up8(self.radius)
        self.length = self.rows + 2 * self.wide
        self.view_rows = self.rows + 2 * self.near
        self.freqs = self.cols // 2
        self.q_wide = self.cols // self.wide
        self.q_near = self.cols // self.near
        self.gx, self.gy = gx, gy
        assert self.half + 2 * self.wide == self.cols == 128
        assert self.wide <= self.rows and self.depth % self.q_near == 0
        assert self.depth == 16


def split_np(matrix):
    high = matrix.astype(np.float32).astype(ml_dtypes.bfloat16)
    low = (matrix - high.astype(np.float64)).astype(np.float32).astype(ml_dtypes.bfloat16)
    return high, low


def lane_positions(s, core):
    lanes = np.arange(s.cols)
    return (lanes + s.wide) % s.cols if core == 0 else (lanes - s.wide) % s.cols


def right_pair(matrix):
    high, low = split_np(matrix)
    return np.block([[high, low], [high, np.zeros_like(low)]])


def left_pair(matrix):
    high, low = split_np(matrix)
    return np.block([[high, high], [low, np.zeros_like(low)]])


def tables(s):
    y_freq = 2.0 * np.pi * (np.arange(s.freqs) + 0.5) / s.cols
    x_freq = 2.0 * np.pi * (np.arange(s.length // 2) + 0.5) / s.length
    y_forward, y_inverse = [], []
    for core in (0, 1):
        angle = lane_positions(s, core)[:, None] * y_freq[None, :]
        both = np.concatenate([np.cos(angle), np.sin(angle)], 1)
        y_forward.append(right_pair(both))
        y_inverse.append(right_pair(both.T * (2.0 / s.cols / s.length)))
    offset = np.arange(s.cols) - s.radius
    angle = offset[:, None] * y_freq[None, :]
    y_kernel = np.concatenate([np.cos(angle), np.sin(angle)], 1)
    y_kernel[s.extent :] = 0.0

    def x_forward(positions):
        angle = x_freq[:, None] * positions[None, :]
        return np.concatenate([np.cos(angle), np.sin(angle)], 0)

    def x_inverse(positions):
        angle = positions[:, None] * x_freq[None, :]
        return np.concatenate([np.cos(angle), -np.sin(angle)], 1)

    window = np.arange(s.length) - s.wide
    near = np.arange(s.view_rows) - s.near
    own = np.arange(s.rows)
    taps = np.arange(up8(s.extent)) - s.radius
    high, low = split_np(x_forward(taps))
    x_kernel = np.concatenate([high, high, low], 1)
    return dict(
        y_forward=np.stack(y_forward),
        y_inverse=np.stack(y_inverse),
        y_kernel=right_pair(y_kernel),
        x_window=left_pair(x_forward(window)),
        x_near=left_pair(x_forward(near)),
        x_back_near=left_pair(x_inverse(near)),
        x_back_own=left_pair(x_inverse(own)),
        x_kernel=x_kernel,
    )


def split(x):
    high = x.astype(BF16)
    return high, (x - high.astype(F32)).astype(BF16)


def dot(a, b):
    return lax.dot_general(a, b, (((1,), (0,)), ((), ())), preferred_element_type=F32)


def lane_iota(rows, cols):
    return lax.broadcasted_iota(jnp.int32, (rows, cols), 1)


def turn(x, shift):
    shift %= x.shape[1]
    return pltpu.roll(x, shift, 1) if shift else x


def wide_split(x):
    return jnp.concatenate(split(x), 1)


def tall_split(x):
    return jnp.concatenate(split(x), 0)


def fold(both):
    width = both.shape[1] // 2
    return both[:, :width] + both[:, width:]


def fold_rows(both):
    count = both.shape[0] // 2
    return both[:count] + both[count:]


def spectrum_of(cosine, sine):
    half = cosine.shape[1] // 2
    left = lane_iota(*cosine.shape) < half
    moved = turn(sine, half)
    minus, plus = cosine - moved, turn(cosine + moved, half)
    return jnp.where(left, minus, plus), jnp.where(left, -plus, minus)


def send_kernel(s, e_in, v_in, e_ref, v_ref, even_ref, odd_ref, sem_ref):
    moves = [
        pltpu.make_async_copy(e_in, e_ref, sem_ref.at[0]),
        pltpu.make_async_copy(v_in, v_ref, sem_ref.at[1]),
    ]
    for move in moves:
        move.start()
    even = lax.axis_index("gx") % 2 == 0
    for move in moves:
        move.wait()
    for ref, begin, count in ((e_ref, 0, 2 * s.radius), (v_ref, s.planes * 2 * s.radius, s.radius)):
        for z in range(s.planes):
            low, high = ref[z, :count], ref[z, s.rows - count :]
            part = slice(begin + z * count, begin + (z + 1) * count)
            even_ref[part] = jnp.where(even, high, low)
            odd_ref[part] = jnp.where(even, low, high)


def side_by_side(planes, group, width):
    lanes = (lane_iota(*planes[0].shape) // width + lax.axis_index("gz")) % group
    packed = planes[0]
    for p in range(1, group):
        packed = jnp.where(lanes == p, turn(planes[p], p * width), packed)
    return packed


def of_plane(s, z, mine_ref, partner_ref):
    plane = z % s.planes
    return jnp.where(lax.axis_index("gz") == z // s.planes, mine_ref[plane], partner_ref[plane])


def pack_own(s, e_ref, e2_ref, v_ref, v2_ref, after_ref, slab_ref):
    place = 0
    for mine, partner, group, width in ((e_ref, e2_ref, s.q_wide, s.wide), (v_ref, v2_ref, s.q_near, s.near)):
        for q in range(0, s.depth, group):
            planes = [of_plane(s, z, mine, partner) for z in range(q, q + group)]
            slab_ref[place : place + s.rows] = side_by_side(planes, group, width)
            place += s.rows


def pack_halo(s, even_ref, odd_ref, even2_ref, odd2_ref, e_ref, v_ref, slab_ref):
    core = lax.axis_index("gz")
    even = lax.axis_index("gx") % 2 == 0
    begin = place = 0
    for out_ref, count, pad, group in (
        (e_ref, 2 * s.radius, s.wide, s.q_wide),
        (v_ref, s.radius, s.near, s.q_near),
    ):
        for e_x_ref, o_x_ref, base in (
            (even_ref, odd_ref, core * s.planes),
            (even2_ref, odd2_ref, (1 - core) * s.planes),
        ):
            for z in range(s.planes):
                here = base + z
                part = slice(begin + z * count, begin + (z + 1) * count)
                out_ref[here, :8] = jnp.zeros((8, s.cols), F32)
                out_ref[here, 2 * pad - 8 :] = jnp.zeros((8, s.cols), F32)
                out_ref[here, pad - count : pad] = jnp.where(even, o_x_ref[part], e_x_ref[part])
                out_ref[here, pad : pad + count] = jnp.where(even, e_x_ref[part], o_x_ref[part])
        for q in range(0, s.depth, group):
            slab_ref[place : place + 2 * pad] = side_by_side([out_ref[z] for z in range(q, q + group)], group, pad)
            place += 2 * pad
        begin += s.planes * count


def framed(frame, body):
    pad = frame.shape[0] // 2
    return jnp.concatenate([frame[:pad], body, frame[pad:]], 0)


def along_x_kernel(s, e_ref, e2_ref, halo_ref, x_ref, t_ref):
    for z in range(0, s.depth, 2):
        both = [tall_split(framed(halo_ref[z + side], of_plane(s, z + side, e_ref, e2_ref))) for side in (0, 1)]
        out = fold_rows(dot(x_ref[...], jnp.concatenate(both, 1)))
        for side in (0, 1):
            t_ref[z + side] = out[:, side * s.cols : (side + 1) * s.cols]


def side_slab(s, q, own_ref, halo_ref, pad, own_begin, halo_begin):
    own, halo = own_begin + q * s.rows, halo_begin + q * 2 * pad
    return framed(halo_ref[halo : halo + 2 * pad], own_ref[own : own + s.rows])


def toeplitz_parts(taps):
    middle = len(taps) // 2
    half = (middle + 1) // 2
    centre = taps[middle - half + 1 : middle + half]
    upper = [p - q for p, q in zip(taps[middle - 2 * half + 1 : middle], centre)]
    lower = [p - q for p, q in zip(taps[middle + 1 : middle + 2 * half], centre)]
    return centre, upper, lower


def kernel_spectrum(
    s, view_ref, psf_in, y_in, x_in, re_ref, im_ref, pad_ref, a_ref, psf_ref, y_ref, x_ref, sem_ref
):
    taps = up8(s.extent)
    moves = [
        pltpu.make_async_copy(psf_in.at[pl.ds(view_ref[0], 1)], psf_ref, sem_ref.at[0]),
        pltpu.make_async_copy(y_in, y_ref, sem_ref.at[1]),
        pltpu.make_async_copy(x_in, x_ref, sem_ref.at[2]),
    ]
    for move in moves:
        move.start()
    pad_ref[...] = jnp.zeros_like(pad_ref)
    for move in moves:
        move.wait()
    total = jnp.zeros((s.extent, s.extent), F32)
    for a in range(s.extent):
        total = total + psf_ref[0, a]
    total = jnp.sum(total)
    for a in range(s.extent):
        pad_ref[a * taps : a * taps + s.extent, : s.extent] = psf_ref[0, a] / total
    a_ref[...] = fold(dot(wide_split(pad_ref[...]), y_ref[...]))
    for pair in range((s.extent + 1) // 2):
        columns = []
        for side in (0, 1):
            a = 2 * pair + side
            high, low = split(a_ref[a * taps : (a + 1) * taps])
            columns.append(jnp.concatenate([high, low, high], 0))
        out = dot(x_ref[...], jnp.concatenate(columns, 1))
        for side in (0, 1):
            if 2 * pair + side < s.extent:
                value = out[:, side * s.cols : (side + 1) * s.cols]
                re_ref[2 * pair + side], im_ref[2 * pair + side] = spectrum_of(value[: s.length // 2], value[s.length // 2 :])


def kernel_leaves(s, re_ref, im_ref, after_ref, k_ref, ks_ref, kd_ref):
    first = s.radius - (s.depth - 1)

    def tile(t, carry):
        rows = pl.ds(t * 8, 8)
        real = [re_ref[a, rows] for a in range(first, first + 2 * s.depth - 1)]
        imag = [im_ref[a, rows] for a in range(first, first + 2 * s.depth - 1)]
        total = [p + q for p, q in zip(real, imag)]
        change = [q - p for p, q in zip(real, imag)]
        for out_ref, values in ((k_ref, real), (ks_ref, total), (kd_ref, change)):
            place = 0
            for part in toeplitz_parts(values):
                for inner in toeplitz_parts(part):
                    for value in inner:
                        out_ref[place, rows] = value
                        place += 1
        return carry

    lax.fori_loop(0, s.length // 16, tile, 0)


def from_side(core, rows, cols, width):
    lanes = lane_iota(rows, cols)
    return jnp.where(core == 0, lanes - (cols - width), width - 1 - lanes) >= 0


def stages(s, k_ref, ks_ref, kd_ref, yf_ref, yi_ref, re_ref, im_ref, pr_ref, pi_ref, a_ref, b_ref, l_ref=None):
    half = s.cols // 2
    depth = s.depth
    group = 4
    freqs = s.length // 2

    def forward_x(rows, x_table):
        for z in range(0, depth, 2):
            both = jnp.concatenate([l_ref[z, : 2 * rows], l_ref[z + 1, : 2 * rows]], 1)
            out = fold_rows(dot(x_table[...], both))
            for side in (0, 1):
                a_ref[z + side] = wide_split(out[:, side * s.cols : (side + 1) * s.cols])

    def forward_y():
        for z in range(0, depth, group):
            out = fold(dot(a_ref[z : z + group].reshape(group * s.length, 2 * s.cols), yf_ref[lax.axis_index("gz")]))
            for k in range(group):
                value = out[k * s.length : (k + 1) * s.length]
                re_ref[z + k], im_ref[z + k] = spectrum_of(value[:freqs], value[freqs:])

    def along_z(flip):
        quarter = depth // 4
        order = (lambda z: depth - 1 - z) if flip else (lambda z: z)
        for_re, for_im = (kd_ref, ks_ref) if flip else (ks_ref, kd_ref)

        def parts(x):
            n = len(x) // 2
            return [p + q for p, q in zip(x[:n], x[n:])], x[n:], x[:n]

        def joined(pieces):
            middle, upper, lower = pieces
            return [p + q for p, q in zip(middle, upper)] + [p + q for p, q in zip(middle, lower)]

        def tile(t, carry):
            rows = pl.ds(t * 8, 8)
            real = [re_ref[order(z), rows] for z in range(depth)]
            imag = [im_ref[order(z), rows] for z in range(depth)]
            outer = [parts(x) for x in ([p + q for p, q in zip(real, imag)], imag, real)]
            kept = None
            for part in range(3):
                inner = [parts(x[part]) for x in outer]
                pieces = []
                for piece in range(3):
                    found = []
                    for i in range(quarter):
                        sums = []
                        for table, values in zip((k_ref, for_re, for_im), inner):
                            total = None
                            for j in range(quarter):
                                d = (3 * part + piece) * (2 * quarter - 1) + i - j + quarter - 1
                                term = table[d, rows] * values[piece][j]
                                total = term if total is None else total + term
                            sums.append(total)
                        if flip:
                            found.append((sums[0] + sums[1], sums[0] - sums[2]))
                        else:
                            found.append((sums[0] - sums[1], sums[0] + sums[2]))
                    pieces.append(found)
                value = [joined([[f[k] for f in found] for found in pieces]) for k in (0, 1)]
                if part == 0:
                    kept = value
                else:
                    start = 0 if part == 1 else 2 * quarter
                    for i in range(2 * quarter):
                        pr_ref[order(start + i), rows] = kept[0][i] + value[0][i]
                        pi_ref[order(start + i), rows] = kept[1][i] + value[1][i]
            return carry

        lax.fori_loop(0, freqs // 8, tile, 0, unroll=2)

    def backward(rows, x_table, use):
        half_lanes = lane_iota(freqs, s.cols) < half
        for z in range(0, depth, group):
            pieces = []
            for k in range(group):
                real, imag = pr_ref[z + k], pi_ref[z + k]
                turned_real, turned_imag = turn(real, half), turn(imag, half)
                pieces.append(jnp.where(half_lanes, real + turned_real, imag - turned_imag))
                pieces.append(jnp.where(half_lanes, imag + turned_imag, turned_real - real))
            out = fold(dot(wide_split(jnp.concatenate(pieces, 0)), yi_ref[lax.axis_index("gz")]))
            for k in range(group):
                b_ref[z + k] = tall_split(out[k * s.length : (k + 1) * s.length])
        for z in range(0, depth, 2):
            out = fold_rows(dot(x_table[...], jnp.concatenate([b_ref[z], b_ref[z + 1]], 1)))
            for side in (0, 1):
                use(z + side, out[:, side * s.cols : (side + 1) * s.cols])

    return forward_x, forward_y, along_z, backward


def first_kernel(
    s, t_in_ref, own_slab_ref, halo_slab_ref, k_ref, ks_ref, kd_ref, yf_ref, yi_ref, xw_ref, xbn_ref, blurred_ref,
    re_ref, im_ref, pr_ref, pi_ref, a_ref, b_ref,
):
    core = lax.axis_index("gz")
    _, forward_y, along_z, backward = stages(
        s, k_ref, ks_ref, kd_ref, yf_ref, yi_ref, re_ref, im_ref, pr_ref, pi_ref, a_ref, b_ref
    )
    arrived = from_side(core, s.length, s.cols, s.wide)
    for q in range(0, s.depth // s.q_wide, 2):
        both = jnp.concatenate([side_slab(s, q + k, own_slab_ref, halo_slab_ref, s.wide, 0, 0) for k in (0, 1)], 1)
        out = fold_rows(dot(xw_ref[...], tall_split(both)))
        for k in (0, 1):
            side = out[:, k * s.cols : (k + 1) * s.cols]
            for p in range(s.q_wide):
                z = (q + k) * s.q_wide + p
                a_ref[z] = wide_split(jnp.where(arrived, turn(side, -p * s.wide), t_in_ref[z]))
    forward_y()
    along_z(False)

    def keep(z, blurred):
        blurred_ref[z] = blurred

    backward(s.view_rows, xbn_ref, keep)


def second_kernel(
    s, blurred_ref, own_ref, partner_ref, v_ref, v2_ref, v_halo_ref, own_slab_ref, halo_slab_ref, k_ref, ks_ref, kd_ref, yf_ref, yi_ref,
    xn_ref, xbo_ref, mine_ref, theirs_ref, five_ref,
    re_ref, im_ref, pr_ref, pi_ref, u_ref, t_ref, l_ref, a_ref, b_ref,
):
    core, gx, gy = lax.axis_index("gz"), lax.axis_index("gx"), lax.axis_index("gy")
    half = s.cols // 2
    depth = s.depth
    forward_x, forward_y, along_z, backward = stages(
        s, k_ref, ks_ref, kd_ref, yf_ref, yi_ref, re_ref, im_ref, pr_ref, pi_ref, a_ref, b_ref, l_ref
    )

    shape = (s.view_rows, s.cols)
    row = lax.broadcasted_iota(jnp.int32, shape, 0) - s.near
    lane = lane_iota(*shape)
    column = lane + jnp.where(core == 0, jnp.where(lane < s.cols - s.near, 0, -s.cols), jnp.where(lane < s.near, s.cols, 0))
    first_row, last_row = -gx * s.rows, (s.gx - gx) * s.rows
    first_column, last_column = -gy * s.cols, (s.gy - gy) * s.cols
    inside = (row >= first_row) & (row < last_row) & (column >= first_column) & (column < last_column)
    begin = core * half - s.near
    inside = inside & (column >= begin) & (column < begin + half + 2 * s.near)

    near_arrived = from_side(core, s.view_rows, s.cols, s.near)
    for z in range(depth):
        safe = jnp.where(inside, blurred_ref[z], 1.0)
        side = side_slab(
            s, z // s.q_near, own_slab_ref, halo_slab_ref, s.near,
            s.depth // s.q_wide * s.rows, s.depth // s.q_wide * 2 * s.wide,
        )
        side = turn(side, -(z % s.q_near) * s.near)
        recorded = jnp.where(near_arrived, side, framed(v_halo_ref[z], of_plane(s, z, v_ref, v2_ref)))
        l_ref[z, : 2 * s.view_rows] = tall_split(jnp.where(inside, recorded / safe, 0.0))
    forward_x(s.view_rows, xn_ref)
    forward_y()
    along_z(True)

    lane = lane_iota(s.rows, s.cols)
    owned = (lane // half) == core

    def to_update(z, correction):
        u_ref[z] = jnp.where(owned, of_plane(s, z, own_ref, partner_ref) * correction, 0.0)

    backward(s.rows, xbo_ref, to_update)

    def three(x):
        high, rest = split(x)
        return high, rest, (x - high.astype(F32) - rest.astype(F32)).astype(BF16)

    def pooled(x, factor, scale):
        count = s.cols // factor
        weights = jnp.where(
            lax.broadcasted_iota(jnp.int32, (s.cols, count), 0) // factor
            == lax.broadcasted_iota(jnp.int32, (s.cols, count), 1),
            scale,
            0.0,
        ).astype(BF16)
        return dot(jnp.concatenate(three(x), 1), jnp.concatenate([weights] * 3, 0))

    u_rows = s.planes * s.rows
    source = u_ref
    planes, rows = depth, s.rows
    sums_of = []
    for level in (1, 2, 3, 4):
        planes, rows = planes // 2, rows // 2
        here = t_ref.at[level - 1]
        for z in range(planes):
            here[z, : 2 * rows] = source[2 * z, : 2 * rows] + source[2 * z + 1, : 2 * rows]
        sums = [
            here[z, pl.ds(0, rows, stride=2)] + here[z, pl.ds(1, rows, stride=2)] for z in range(planes)
        ]
        for z in range(planes):
            here[z, :rows] = sums[z]
        sums_of.append(sums)
        source = here
    levels = []
    for level, sums in enumerate(sums_of, 1):
        factor = 2**level
        value = pooled(jnp.concatenate(sums, 0), factor, 1.0 / factor**3)
        levels.append((value, len(sums), sums[0].shape[0], s.cols // factor))
    top = sums_of[-1][0]
    own_rows = top.shape[0] // 2
    per_chip = s.cols // 32
    line = jnp.concatenate([top[2 * i : 2 * i + 1] + top[2 * i + 1 : 2 * i + 2] for i in range(own_rows)], 1)
    cells = five_ref.shape[2]
    source_lane = lax.broadcasted_iota(jnp.int32, (line.shape[1], cells), 0)
    place = (gx * own_rows + source_lane // s.cols) * (s.gy * per_chip) + gy * per_chip + source_lane % s.cols // 32
    weights = jnp.where(
        place == lax.broadcasted_iota(jnp.int32, place.shape, 1), 1.0 / (32 * 32 * depth), 0.0
    ).astype(BF16)
    five = dot(jnp.concatenate(three(line), 1), jnp.concatenate([weights] * 3, 0))
    five_ref[...] = jnp.broadcast_to(five[None], five_ref.shape)
    for half_index in (0, 1):
        for mine, out_ref in ((True, mine_ref), (False, theirs_ref)):

            @pl.when((core == half_index) == mine)
            def _():
                for z in range(s.planes):
                    out_ref[z * s.rows : (z + 1) * s.rows] = u_ref[half_index * s.planes + z]
                start = u_rows
                for value, planes, rows, columns in levels:
                    count = max(planes * rows // 2, rows)
                    begin = half_index * count if planes > 1 else 0
                    out_ref[start : start + count, :columns] = value[begin : begin + count]
                    start += up8(count)


def last_kernel(s, mine_ref, got_ref, fives_ref, u_ref, one_ref, two_ref, three_ref, four_ref, five_ref):
    for z in range(s.planes):
        part = slice(z * s.rows, (z + 1) * s.rows)
        u_ref[z] = mine_ref[part] + got_ref[part]
    start = s.planes * s.rows
    for out_ref in (one_ref, two_ref, three_ref, four_ref):
        planes, rows, columns = out_ref.shape
        for z in range(planes):
            part = slice(start + z * rows, start + (z + 1) * rows)
            out_ref[z] = mine_ref[part, :columns] + got_ref[part, :columns]
        start += up8(planes * rows)
    rows, columns = five_ref.shape[1:]
    total = jnp.sum(fives_ref[...], axis=0)
    cells = rows * columns
    shape = (rows, cells)
    lane = lane_iota(*shape)
    spread = jnp.where(lane // columns == lax.broadcasted_iota(jnp.int32, shape, 0), jnp.broadcast_to(total, shape), 0.0)
    shape = (cells, columns)
    ones = (lax.broadcasted_iota(jnp.int32, shape, 0) % columns == lane_iota(*shape)).astype(BF16)
    high, rest = split(spread)
    low = (spread - high.astype(F32) - rest.astype(F32)).astype(BF16)
    five_ref[0] = dot(jnp.concatenate([high, rest, low], 1), jnp.concatenate([ones] * 3, 0))


def in_hbm(x):
    return pltpu.with_memory_space_constraint(x, pltpu.HBM)


def call(body, arrays, outs, scratch=(), narrow=(), copies=(), mib=16, flops=10**7, prefetch=(), where=None):
    outs = [out if isinstance(out[0], tuple) else (out, F32) for out in outs]
    return pl.pallas_call(
        body,
        grid_spec=pltpu.PrefetchScalarGridSpec(
            num_scalar_prefetch=len(prefetch),
            in_specs=[pl.BlockSpec(memory_space=where or pltpu.VMEM)] * len(arrays),
            out_specs=[pl.BlockSpec(memory_space=pltpu.VMEM)] * len(outs),
            scratch_shapes=[pltpu.VMEM(shape, F32) for shape in scratch]
            + [pltpu.VMEM(shape, BF16) for shape in narrow]
            + list(copies),
        ),
        out_shape=[jax.ShapeDtypeStruct(*out) for out in outs],
        compiler_params=pltpu.CompilerParams(vmem_limit_bytes=mib * MIB),
        cost_estimate=pl.CostEstimate(flops=flops, bytes_accessed=0, transcendentals=0),
    )(*prefetch, *arrays)


def neighbours(first):
    pairs = []
    for i in range(first, lax.axis_size("gx") - 1, 2):
        pairs += [(i, i + 1), (i + 1, i)]
    return pairs


def to_side():
    pairs = []
    for h in range(lax.axis_size("gy") - 1):
        pairs += [(2 * h + 1, 2 * h + 2), (2 * h + 2, 2 * h + 1)]
    return pairs


def local(estimate, view_data, psf_stack, view_index):
    assert lax.axis_size("gz") == 2
    gx, gy = lax.axis_size("gx"), lax.axis_size("gy")
    s = Sizes(estimate.shape, psf_stack.shape, gx, gy)
    t = {key: jnp.asarray(value) for key, value in tables(s).items()}
    across = [(0, 1), (1, 0)]
    strip = (s.planes * 3 * s.radius, s.cols)
    own, own_view, even, odd = call(
        functools.partial(send_kernel, s),
        (in_hbm(estimate), in_hbm(view_data)),
        [estimate.shape, estimate.shape, strip, strip],
        copies=[pltpu.SemaphoreType.DMA((2,))],
        mib=8,
        where=pltpu.HBM,
    )
    even = lax.ppermute(even, "gx", neighbours(0))
    odd = lax.ppermute(odd, "gx", neighbours(1))
    partner = lax.ppermute(own, "gz", across)
    partner_view = lax.ppermute(own_view, "gz", across)

    taps = up8(s.extent)
    psf_shape = (1,) + psf_stack.shape[1:]
    kernel_planes = (s.extent, s.length // 2, s.cols)
    re, im = call(
        functools.partial(kernel_spectrum, s),
        (in_hbm(psf_stack), in_hbm(t["y_kernel"]), in_hbm(t["x_kernel"])),
        [kernel_planes] * 2,
        scratch=[((s.extent + 1) // 2 * 2 * taps, s.cols)] * 2 + [psf_shape],
        narrow=[t["y_kernel"].shape, t["x_kernel"].shape],
        copies=[pltpu.SemaphoreType.DMA((3,))],
        prefetch=(view_index,),
        where=pltpu.HBM,
    )
    own_rows = (s.depth // s.q_wide + s.depth // s.q_near) * s.rows
    (own_slab,) = call(functools.partial(pack_own, s), (own, partner, own_view, partner_view, re), [(own_rows, s.cols)])
    own_slab = lax.ppermute(own_slab, ("gy", "gz"), to_side())
    even, _ = lax.optimization_barrier((even, re))
    even2 = lax.ppermute(even, "gz", across)
    odd, _ = lax.optimization_barrier((odd, even2))
    odd2 = lax.ppermute(odd, "gz", across)
    halo_rows = s.depth // s.q_wide * 2 * s.wide + s.depth // s.q_near * 2 * s.near
    e_halo, v_halo, halo_slab_here = call(
        functools.partial(pack_halo, s),
        (even, odd, even2, odd2),
        [(s.depth, 2 * s.wide, s.cols), (s.depth, 2 * s.near, s.cols), (halo_rows, s.cols)],
    )
    halo_slab = lax.ppermute(halo_slab_here, ("gy", "gz"), to_side())
    k, ks, kd = call(
        functools.partial(kernel_leaves, s),
        (re, im, halo_slab_here),
        [(9 * (s.depth // 2 - 1), s.length // 2, s.cols)] * 3,
    )
    view_window = (s.depth, s.view_rows, s.cols)
    (along_x,) = call(
        functools.partial(along_x_kernel, s), (own, partner, e_halo, t["x_window"]), [(s.depth, s.length, s.cols)]
    )

    u_rows = s.planes * s.rows
    out_rows = u_rows
    level_shapes = []
    planes, rows, columns = s.depth, s.rows, s.cols
    for _ in range(4):
        planes, rows, columns = planes // 2, rows // 2, columns // 2
        level_shapes.append((max(planes // 2, 1), rows, columns))
        out_rows += up8(level_shapes[-1][0] * rows)
    devices = 2 * gx * gy
    five_shape = (rows // 2 * gx, columns // 2 * gy)
    spectra = [(s.depth, s.length // 2, s.cols)] * 4
    halves = [(s.depth, s.length, 2 * s.cols), (s.depth, 2 * s.length, s.cols)]
    shared = (k, ks, kd, t["y_forward"], t["y_inverse"])
    (blurred,) = call(
        functools.partial(first_kernel, s),
        (along_x, own_slab, halo_slab) + shared + (t["x_window"], t["x_back_near"]),
        [view_window],
        scratch=spectra,
        narrow=halves,
        mib=24,
        flops=10**8,
    )
    mine, theirs, five = call(
        functools.partial(second_kernel, s),
        (blurred, own, partner, own_view, partner_view, v_halo, own_slab, halo_slab) + shared + (t["x_near"], t["x_back_own"]),
        [(out_rows, s.cols), (out_rows, s.cols), (devices, 1, five_shape[0] * five_shape[1])],
        scratch=spectra + [(s.depth, s.rows, s.cols), (4, s.depth // 2, s.rows, s.cols)],
        narrow=[(s.depth, 2 * s.view_rows, s.cols)] + halves,
        mib=24,
    )
    got = lax.ppermute(theirs, "gz", across)
    fives = lax.all_to_all(five, ALL, split_axis=0, concat_axis=0, tiled=True)
    return tuple(
        call(
            functools.partial(last_kernel, s),
            (mine, got, fives),
            [estimate.shape] + level_shapes + [(1,) + five_shape],
            mib=8,
        )
    )


def solution(mesh):
    return jax.shard_map(
        local,
        mesh=mesh,
        in_specs=(P("gz", "gx", "gy"), P("gz", "gx", "gy"), P(), P()),
        out_specs=(
            P("gz", "gx", "gy"),
            P("gz", "gx", "gy"),
            P("gz", "gx", "gy"),
            P("gz", "gx", "gy"),
            P(None, "gx", "gy"),
            P(),
        ),
        check_vma=False,
    )
```

```python
import functools

import jax
import jax.numpy as jnp
import ml_dtypes
import numpy as np
from jax import lax
from jax.experimental import pallas as pl
from jax.experimental.pallas import tpu as pltpu
from jax.sharding import PartitionSpec as P


F32 = jnp.float32
BF16 = jnp.bfloat16
ALL = ("gx", "gy", "gz")
MIB = 1024 * 1024


def up8(count):
    return (count + 7) // 8 * 8


class Sizes:
    def __init__(self, estimate_shape, psf_shape, gx, gy):
        self.planes, self.rows, self.cols = estimate_shape
        self.extent = psf_shape[1]
        self.radius = (self.extent - 1) // 2
        self.depth = 2 * self.planes
        self.half = self.cols // 2
        self.wide = up8(2 * self.radius)
        self.near = up8(self.radius)
        self.length = self.rows + 2 * self.wide
        self.view_rows = self.rows + 2 * self.near
        self.freqs = self.cols // 2
        self.q_wide = self.cols // self.wide
        self.q_near = self.cols // self.near
        self.gx, self.gy = gx, gy
        assert self.half + 2 * self.wide == self.cols == 128
        assert self.wide <= self.rows and self.depth % self.q_near == 0
        assert self.depth == 16


def split_np(matrix):
    high = matrix.astype(np.float32).astype(ml_dtypes.bfloat16)
    low = (matrix - high.astype(np.float64)).astype(np.float32).astype(ml_dtypes.bfloat16)
    return high, low


def lane_positions(s, core):
    lanes = np.arange(s.cols)
    return (lanes + s.wide) % s.cols if core == 0 else (lanes - s.wide) % s.cols


def right_pair(matrix):
    high, low = split_np(matrix)
    return np.block([[high, low], [high, np.zeros_like(low)]])


def left_pair(matrix):
    high, low = split_np(matrix)
    return np.block([[high, high], [low, np.zeros_like(low)]])


def tables(s):
    y_freq = 2.0 * np.pi * (np.arange(s.freqs) + 0.5) / s.cols
    x_freq = 2.0 * np.pi * (np.arange(s.length // 2) + 0.5) / s.length
    y_forward, y_inverse = [], []
    for core in (0, 1):
        angle = lane_positions(s, core)[:, None] * y_freq[None, :]
        both = np.concatenate([np.cos(angle), np.sin(angle)], 1)
        y_forward.append(right_pair(both))
        y_inverse.append(right_pair(both.T * (2.0 / s.cols / s.length)))
    offset = np.arange(s.cols) - s.radius
    angle = offset[:, None] * y_freq[None, :]
    y_kernel = np.concatenate([np.cos(angle), np.sin(angle)], 1)
    y_kernel[s.extent :] = 0.0

    def x_forward(positions):
        angle = x_freq[:, None] * positions[None, :]
        return np.concatenate([np.cos(angle), np.sin(angle)], 0)

    def x_inverse(positions):
        angle = positions[:, None] * x_freq[None, :]
        return np.concatenate([np.cos(angle), -np.sin(angle)], 1)

    window = np.arange(s.length) - s.wide
    near = np.arange(s.view_rows) - s.near
    own = np.arange(s.rows)
    taps = np.arange(up8(s.extent)) - s.radius
    high, low = split_np(x_forward(taps))
    x_kernel = np.concatenate([high, high, low], 1)
    return dict(
        y_forward=np.stack(y_forward),
        y_inverse=np.stack(y_inverse),
        y_kernel=right_pair(y_kernel),
        x_window=left_pair(x_forward(window)),
        x_near=left_pair(x_forward(near)),
        x_back_near=left_pair(x_inverse(near)),
        x_back_own=left_pair(x_inverse(own)),
        x_kernel=x_kernel,
    )


def split(x):
    high = x.astype(BF16)
    return high, (x - high.astype(F32)).astype(BF16)


def dot(a, b):
    return lax.dot_general(a, b, (((1,), (0,)), ((), ())), preferred_element_type=F32)


def lane_iota(rows, cols):
    return lax.broadcasted_iota(jnp.int32, (rows, cols), 1)


def turn(x, shift):
    shift %= x.shape[1]
    return pltpu.roll(x, shift, 1) if shift else x


def wide_split(x):
    return jnp.concatenate(split(x), 1)


def tall_split(x):
    return jnp.concatenate(split(x), 0)


def fold(both):
    width = both.shape[1] // 2
    return both[:, :width] + both[:, width:]


def fold_rows(both):
    count = both.shape[0] // 2
    return both[:count] + both[count:]


def spectrum_of(cosine, sine):
    half = cosine.shape[1] // 2
    left = lane_iota(*cosine.shape) < half
    moved = turn(sine, half)
    minus, plus = cosine - moved, turn(cosine + moved, half)
    return jnp.where(left, minus, plus), jnp.where(left, -plus, minus)


def send_kernel(s, e_in, v_in, e_ref, v_ref, even_ref, odd_ref, sem_ref):
    moves = [
        pltpu.make_async_copy(e_in, e_ref, sem_ref.at[0]),
        pltpu.make_async_copy(v_in, v_ref, sem_ref.at[1]),
    ]
    for move in moves:
        move.start()
    even = lax.axis_index("gx") % 2 == 0
    for move in moves:
        move.wait()
    for ref, begin, count in ((e_ref, 0, 2 * s.radius), (v_ref, s.planes * 2 * s.radius, s.radius)):
        for z in range(s.planes):
            low, high = ref[z, :count], ref[z, s.rows - count :]
            part = slice(begin + z * count, begin + (z + 1) * count)
            even_ref[part] = jnp.where(even, high, low)
            odd_ref[part] = jnp.where(even, low, high)


def side_by_side(planes, group, width):
    lanes = (lane_iota(*planes[0].shape) // width + lax.axis_index("gz")) % group
    packed = planes[0]
    for p in range(1, group):
        packed = jnp.where(lanes == p, turn(planes[p], p * width), packed)
    return packed


def of_plane(s, z, mine_ref, partner_ref):
    plane = z % s.planes
    return jnp.where(lax.axis_index("gz") == z // s.planes, mine_ref[plane], partner_ref[plane])


def pack_own(s, e_ref, e2_ref, v_ref, v2_ref, after_ref, slab_ref):
    place = 0
    for mine, partner, group, width in ((e_ref, e2_ref, s.q_wide, s.wide), (v_ref, v2_ref, s.q_near, s.near)):
        for q in range(0, s.depth, group):
            planes = [of_plane(s, z, mine, partner) for z in range(q, q + group)]
            slab_ref[place : place + s.rows] = side_by_side(planes, group, width)
            place += s.rows


def pack_halo(s, even_ref, odd_ref, even2_ref, odd2_ref, e_ref, v_ref, slab_ref):
    core = lax.axis_index("gz")
    even = lax.axis_index("gx") % 2 == 0
    begin = place = 0
    for out_ref, count, pad, group in (
        (e_ref, 2 * s.radius, s.wide, s.q_wide),
        (v_ref, s.radius, s.near, s.q_near),
    ):
        for e_x_ref, o_x_ref, base in (
            (even_ref, odd_ref, core * s.planes),
            (even2_ref, odd2_ref, (1 - core) * s.planes),
        ):
            for z in range(s.planes):
                here = base + z
                part = slice(begin + z * count, begin + (z + 1) * count)
                out_ref[here, :8] = jnp.zeros((8, s.cols), F32)
                out_ref[here, 2 * pad - 8 :] = jnp.zeros((8, s.cols), F32)
                out_ref[here, pad - count : pad] = jnp.where(even, o_x_ref[part], e_x_ref[part])
                out_ref[here, pad : pad + count] = jnp.where(even, e_x_ref[part], o_x_ref[part])
        for q in range(0, s.depth, group):
            slab_ref[place : place + 2 * pad] = side_by_side([out_ref[z] for z in range(q, q + group)], group, pad)
            place += 2 * pad
        begin += s.planes * count


def framed(frame, body):
    pad = frame.shape[0] // 2
    return jnp.concatenate([frame[:pad], body, frame[pad:]], 0)


def along_x_kernel(s, e_ref, e2_ref, halo_ref, x_ref, v_ref, v2_ref, v_halo_ref, t_ref, v_window_ref):
    for z in range(s.depth):
        v_window_ref[z] = framed(v_halo_ref[z], of_plane(s, z, v_ref, v2_ref))
    for z in range(0, s.depth, 2):
        both = [tall_split(framed(halo_ref[z + side], of_plane(s, z + side, e_ref, e2_ref))) for side in (0, 1)]
        out = fold_rows(dot(x_ref[...], jnp.concatenate(both, 1)))
        for side in (0, 1):
            t_ref[z + side] = out[:, side * s.cols : (side + 1) * s.cols]


def side_slab(s, q, own_ref, halo_ref, pad, own_begin, halo_begin):
    own, halo = own_begin + q * s.rows, halo_begin + q * 2 * pad
    return framed(halo_ref[halo : halo + 2 * pad], own_ref[own : own + s.rows])


def toeplitz_parts(taps):
    middle = len(taps) // 2
    half = (middle + 1) // 2
    centre = taps[middle - half + 1 : middle + half]
    upper = [p - q for p, q in zip(taps[middle - 2 * half + 1 : middle], centre)]
    lower = [p - q for p, q in zip(taps[middle + 1 : middle + 2 * half], centre)]
    return centre, upper, lower


def kernel_spectrum(
    s, view_ref, psf_in, y_in, x_in, re_ref, im_ref, pad_ref, a_ref, psf_ref, y_ref, x_ref, sem_ref
):
    taps = up8(s.extent)
    moves = [
        pltpu.make_async_copy(psf_in.at[pl.ds(view_ref[0], 1)], psf_ref, sem_ref.at[0]),
        pltpu.make_async_copy(y_in, y_ref, sem_ref.at[1]),
        pltpu.make_async_copy(x_in, x_ref, sem_ref.at[2]),
    ]
    for move in moves:
        move.start()
    pad_ref[...] = jnp.zeros_like(pad_ref)
    for move in moves:
        move.wait()
    total = jnp.zeros((s.extent, s.extent), F32)
    for a in range(s.extent):
        total = total + psf_ref[0, a]
    total = jnp.sum(total)
    for a in range(s.extent):
        pad_ref[a * taps : a * taps + s.extent, : s.extent] = psf_ref[0, a] / total
    a_ref[...] = fold(dot(wide_split(pad_ref[...]), y_ref[...]))
    for pair in range((s.extent + 1) // 2):
        columns = []
        for side in (0, 1):
            a = 2 * pair + side
            high, low = split(a_ref[a * taps : (a + 1) * taps])
            columns.append(jnp.concatenate([high, low, high], 0))
        out = dot(x_ref[...], jnp.concatenate(columns, 1))
        for side in (0, 1):
            if 2 * pair + side < s.extent:
                value = out[:, side * s.cols : (side + 1) * s.cols]
                re_ref[2 * pair + side], im_ref[2 * pair + side] = spectrum_of(value[: s.length // 2], value[s.length // 2 :])


def kernel_leaves(s, re_ref, im_ref, after_ref, k_ref, ks_ref, kd_ref):
    first = s.radius - (s.depth - 1)

    def tile(t, carry):
        rows = pl.ds(t * 8, 8)
        real = [re_ref[a, rows] for a in range(first, first + 2 * s.depth - 1)]
        imag = [im_ref[a, rows] for a in range(first, first + 2 * s.depth - 1)]
        total = [p + q for p, q in zip(real, imag)]
        change = [q - p for p, q in zip(real, imag)]
        for out_ref, values in ((k_ref, real), (ks_ref, total), (kd_ref, change)):
            place = 0
            for part in toeplitz_parts(values):
                for inner in toeplitz_parts(part):
                    for value in inner:
                        out_ref[place, rows] = value
                        place += 1
        return carry

    lax.fori_loop(0, s.length // 16, tile, 0, unroll=2)


def from_side(core, rows, cols, width):
    lanes = lane_iota(rows, cols)
    return jnp.where(core == 0, lanes - (cols - width), width - 1 - lanes) >= 0


def stages(s, k_ref, ks_ref, kd_ref, yf_ref, yi_ref, re_ref, im_ref, pr_ref, pi_ref, a_ref, b_ref, l_ref=None):
    half = s.cols // 2
    depth = s.depth
    group = 8
    freqs = s.length // 2

    def forward_x(rows, x_table):
        for z in range(0, depth, 2):
            both = jnp.concatenate([l_ref[z, : 2 * rows], l_ref[z + 1, : 2 * rows]], 1)
            out = fold_rows(dot(x_table[...], both))
            for side in (0, 1):
                a_ref[z + side] = wide_split(out[:, side * s.cols : (side + 1) * s.cols])

    def forward_y():
        for z in range(0, depth, group):
            out = fold(dot(a_ref[z : z + group].reshape(group * s.length, 2 * s.cols), yf_ref[lax.axis_index("gz")]))
            for k in range(group):
                value = out[k * s.length : (k + 1) * s.length]
                re_ref[z + k], im_ref[z + k] = spectrum_of(value[:freqs], value[freqs:])

    def along_z(flip):
        quarter = depth // 4
        order = (lambda z: depth - 1 - z) if flip else (lambda z: z)
        for_re, for_im = (kd_ref, ks_ref) if flip else (ks_ref, kd_ref)

        def parts(x):
            n = len(x) // 2
            return [p + q for p, q in zip(x[:n], x[n:])], x[n:], x[:n]

        def joined(pieces):
            middle, upper, lower = pieces
            return [p + q for p, q in zip(middle, upper)] + [p + q for p, q in zip(middle, lower)]

        def tile(t, carry):
            rows = pl.ds(t * 8, 8)
            real = [re_ref[order(z), rows] for z in range(depth)]
            imag = [im_ref[order(z), rows] for z in range(depth)]
            outer = [parts(x) for x in ([p + q for p, q in zip(real, imag)], imag, real)]
            kept = None
            for part in range(3):
                inner = [parts(x[part]) for x in outer]
                pieces = []
                for piece in range(3):
                    found = []
                    for i in range(quarter):
                        sums = []
                        for table, values in zip((k_ref, for_re, for_im), inner):
                            total = None
                            for j in range(quarter):
                                d = (3 * part + piece) * (2 * quarter - 1) + i - j + quarter - 1
                                term = table[d, rows] * values[piece][j]
                                total = term if total is None else total + term
                            sums.append(total)
                        if flip:
                            found.append((sums[0] + sums[1], sums[0] - sums[2]))
                        else:
                            found.append((sums[0] - sums[1], sums[0] + sums[2]))
                    pieces.append(found)
                value = [joined([[f[k] for f in found] for found in pieces]) for k in (0, 1)]
                if part == 0:
                    kept = value
                else:
                    start = 0 if part == 1 else 2 * quarter
                    for i in range(2 * quarter):
                        pr_ref[order(start + i), rows] = kept[0][i] + value[0][i]
                        pi_ref[order(start + i), rows] = kept[1][i] + value[1][i]
            return carry

        lax.fori_loop(0, freqs // 8, tile, 0, unroll=2)

    def backward(rows, x_table, use):
        half_lanes = lane_iota(freqs, s.cols) < half
        for z in range(0, depth, group):
            pieces = []
            for k in range(group):
                real, imag = pr_ref[z + k], pi_ref[z + k]
                turned_real, turned_imag = turn(real, half), turn(imag, half)
                pieces.append(jnp.where(half_lanes, real + turned_real, imag - turned_imag))
                pieces.append(jnp.where(half_lanes, imag + turned_imag, turned_real - real))
            out = fold(dot(wide_split(jnp.concatenate(pieces, 0)), yi_ref[lax.axis_index("gz")]))
            for k in range(group):
                b_ref[z + k] = tall_split(out[k * s.length : (k + 1) * s.length])
        for z in range(0, depth, 2):
            out = fold_rows(dot(x_table[...], jnp.concatenate([b_ref[z], b_ref[z + 1]], 1)))
            for side in (0, 1):
                use(z + side, out[:, side * s.cols : (side + 1) * s.cols])

    return forward_x, forward_y, along_z, backward


def first_kernel(
    s, t_in_ref, own_slab_ref, halo_slab_ref, k_ref, ks_ref, kd_ref, yf_ref, yi_ref, xw_ref, xbn_ref, blurred_ref,
    re_ref, im_ref, pr_ref, pi_ref, a_ref, b_ref,
):
    core = lax.axis_index("gz")
    _, forward_y, along_z, backward = stages(
        s, k_ref, ks_ref, kd_ref, yf_ref, yi_ref, re_ref, im_ref, pr_ref, pi_ref, a_ref, b_ref
    )
    arrived = from_side(core, s.length, s.cols, s.wide)
    for q in range(0, s.depth // s.q_wide, 2):
        both = jnp.concatenate([side_slab(s, q + k, own_slab_ref, halo_slab_ref, s.wide, 0, 0) for k in (0, 1)], 1)
        out = fold_rows(dot(xw_ref[...], tall_split(both)))
        for k in (0, 1):
            side = out[:, k * s.cols : (k + 1) * s.cols]
            for p in range(s.q_wide):
                z = (q + k) * s.q_wide + p
                a_ref[z] = wide_split(jnp.where(arrived, turn(side, -p * s.wide), t_in_ref[z]))
    forward_y()
    along_z(False)

    def keep(z, blurred):
        blurred_ref[z] = blurred

    backward(s.view_rows, xbn_ref, keep)


def second_kernel(
    s, blurred_ref, own_ref, partner_ref, v_window_ref, own_slab_ref, halo_slab_ref, k_ref, ks_ref, kd_ref, yf_ref, yi_ref,
    xn_ref, xbo_ref, mine_ref, theirs_ref, five_ref,
    re_ref, im_ref, pr_ref, pi_ref, u_ref, t_ref, l_ref, a_ref, b_ref,
):
    core, gx, gy = lax.axis_index("gz"), lax.axis_index("gx"), lax.axis_index("gy")
    half = s.cols // 2
    depth = s.depth
    forward_x, forward_y, along_z, backward = stages(
        s, k_ref, ks_ref, kd_ref, yf_ref, yi_ref, re_ref, im_ref, pr_ref, pi_ref, a_ref, b_ref, l_ref
    )

    shape = (s.view_rows, s.cols)
    row = lax.broadcasted_iota(jnp.int32, shape, 0) - s.near
    lane = lane_iota(*shape)
    column = lane + jnp.where(core == 0, jnp.where(lane < s.cols - s.near, 0, -s.cols), jnp.where(lane < s.near, s.cols, 0))
    first_row, last_row = -gx * s.rows, (s.gx - gx) * s.rows
    first_column, last_column = -gy * s.cols, (s.gy - gy) * s.cols
    inside = (row >= first_row) & (row < last_row) & (column >= first_column) & (column < last_column)
    begin = core * half - s.near
    inside = inside & (column >= begin) & (column < begin + half + 2 * s.near)

    near_arrived = from_side(core, s.view_rows, s.cols, s.near)
    for z in range(depth):
        safe = jnp.where(inside, blurred_ref[z], 1.0)
        side = side_slab(
            s, z // s.q_near, own_slab_ref, halo_slab_ref, s.near,
            s.depth // s.q_wide * s.rows, s.depth // s.q_wide * 2 * s.wide,
        )
        side = turn(side, -(z % s.q_near) * s.near)
        recorded = jnp.where(near_arrived, side, v_window_ref[z])
        l_ref[z, : 2 * s.view_rows] = tall_split(jnp.where(inside, recorded / safe, 0.0))
    forward_x(s.view_rows, xn_ref)
    forward_y()
    along_z(True)

    lane = lane_iota(s.rows, s.cols)
    owned = (lane // half) == core

    def to_update(z, correction):
        u_ref[z] = jnp.where(owned, of_plane(s, z, own_ref, partner_ref) * correction, 0.0)

    backward(s.rows, xbo_ref, to_update)

    def three(x):
        high, rest = split(x)
        return high, rest, (x - high.astype(F32) - rest.astype(F32)).astype(BF16)

    def pooled(x, factor, scale):
        count = s.cols // factor
        weights = jnp.where(
            lax.broadcasted_iota(jnp.int32, (s.cols, count), 0) // factor
            == lax.broadcasted_iota(jnp.int32, (s.cols, count), 1),
            scale,
            0.0,
        ).astype(BF16)
        return dot(jnp.concatenate(three(x), 1), jnp.concatenate([weights] * 3, 0))

    u_rows = s.planes * s.rows
    source = u_ref
    planes, rows = depth, s.rows
    sums_of = []
    for level in (1, 2, 3, 4):
        planes, rows = planes // 2, rows // 2
        here = t_ref.at[level - 1]
        for z in range(planes):
            here[z, : 2 * rows] = source[2 * z, : 2 * rows] + source[2 * z + 1, : 2 * rows]
        sums = [
            here[z, pl.ds(0, rows, stride=2)] + here[z, pl.ds(1, rows, stride=2)] for z in range(planes)
        ]
        for z in range(planes):
            here[z, :rows] = sums[z]
        sums_of.append(sums)
        source = here
    levels = []
    for level, sums in enumerate(sums_of, 1):
        factor = 2**level
        value = pooled(jnp.concatenate(sums, 0), factor, 1.0 / factor**3)
        levels.append((value, len(sums), sums[0].shape[0], s.cols // factor))
    top = sums_of[-1][0]
    own_rows = top.shape[0] // 2
    per_chip = s.cols // 32
    line = jnp.concatenate([top[2 * i : 2 * i + 1] + top[2 * i + 1 : 2 * i + 2] for i in range(own_rows)], 1)
    cells = five_ref.shape[2]
    source_lane = lax.broadcasted_iota(jnp.int32, (line.shape[1], cells), 0)
    place = (gx * own_rows + source_lane // s.cols) * (s.gy * per_chip) + gy * per_chip + source_lane % s.cols // 32
    weights = jnp.where(
        place == lax.broadcasted_iota(jnp.int32, place.shape, 1), 1.0 / (32 * 32 * depth), 0.0
    ).astype(BF16)
    five = dot(jnp.concatenate(three(line), 1), jnp.concatenate([weights] * 3, 0))
    five_ref[...] = jnp.broadcast_to(five[None], five_ref.shape)
    for half_index in (0, 1):
        for mine, out_ref in ((True, mine_ref), (False, theirs_ref)):

            @pl.when((core == half_index) == mine)
            def _():
                for z in range(s.planes):
                    out_ref[z * s.rows : (z + 1) * s.rows] = u_ref[half_index * s.planes + z]
                start = u_rows
                for value, planes, rows, columns in levels:
                    count = max(planes * rows // 2, rows)
                    begin = half_index * count if planes > 1 else 0
                    out_ref[start : start + count, :columns] = value[begin : begin + count]
                    start += up8(count)


def last_kernel(s, mine_ref, got_ref, fives_ref, u_ref, one_ref, two_ref, three_ref, four_ref, five_ref):
    for z in range(s.planes):
        part = slice(z * s.rows, (z + 1) * s.rows)
        u_ref[z] = mine_ref[part] + got_ref[part]
    start = s.planes * s.rows
    for out_ref in (one_ref, two_ref, three_ref, four_ref):
        planes, rows, columns = out_ref.shape
        for z in range(planes):
            part = slice(start + z * rows, start + (z + 1) * rows)
            out_ref[z] = mine_ref[part, :columns] + got_ref[part, :columns]
        start += up8(planes * rows)
    rows, columns = five_ref.shape[1:]
    total = jnp.sum(fives_ref[...], axis=0)
    cells = rows * columns
    shape = (rows, cells)
    lane = lane_iota(*shape)
    spread = jnp.where(lane // columns == lax.broadcasted_iota(jnp.int32, shape, 0), jnp.broadcast_to(total, shape), 0.0)
    shape = (cells, columns)
    ones = (lax.broadcasted_iota(jnp.int32, shape, 0) % columns == lane_iota(*shape)).astype(BF16)
    high, rest = split(spread)
    low = (spread - high.astype(F32) - rest.astype(F32)).astype(BF16)
    five_ref[0] = dot(jnp.concatenate([high, rest, low], 1), jnp.concatenate([ones] * 3, 0))


def in_hbm(x):
    return pltpu.with_memory_space_constraint(x, pltpu.HBM)


def call(body, arrays, outs, scratch=(), narrow=(), copies=(), mib=16, flops=10**7, prefetch=(), where=None):
    outs = [out if isinstance(out[0], tuple) else (out, F32) for out in outs]
    return pl.pallas_call(
        body,
        grid_spec=pltpu.PrefetchScalarGridSpec(
            num_scalar_prefetch=len(prefetch),
            in_specs=[pl.BlockSpec(memory_space=where or pltpu.VMEM)] * len(arrays),
            out_specs=[pl.BlockSpec(memory_space=pltpu.VMEM)] * len(outs),
            scratch_shapes=[pltpu.VMEM(shape, F32) for shape in scratch]
            + [pltpu.VMEM(shape, BF16) for shape in narrow]
            + list(copies),
        ),
        out_shape=[jax.ShapeDtypeStruct(*out) for out in outs],
        compiler_params=pltpu.CompilerParams(vmem_limit_bytes=mib * MIB),
        cost_estimate=pl.CostEstimate(flops=flops, bytes_accessed=0, transcendentals=0),
    )(*prefetch, *arrays)


def neighbours(first):
    pairs = []
    for i in range(first, lax.axis_size("gx") - 1, 2):
        pairs += [(i, i + 1), (i + 1, i)]
    return pairs


def to_side():
    pairs = []
    for h in range(lax.axis_size("gy") - 1):
        pairs += [(2 * h + 1, 2 * h + 2), (2 * h + 2, 2 * h + 1)]
    return pairs


def local(estimate, view_data, psf_stack, view_index):
    assert lax.axis_size("gz") == 2
    gx, gy = lax.axis_size("gx"), lax.axis_size("gy")
    s = Sizes(estimate.shape, psf_stack.shape, gx, gy)
    t = {key: jnp.asarray(value) for key, value in tables(s).items()}
    across = [(0, 1), (1, 0)]
    strip = (s.planes * 3 * s.radius, s.cols)
    own, own_view, even, odd = call(
        functools.partial(send_kernel, s),
        (in_hbm(estimate), in_hbm(view_data)),
        [estimate.shape, estimate.shape, strip, strip],
        copies=[pltpu.SemaphoreType.DMA((2,))],
        mib=8,
        where=pltpu.HBM,
    )
    even = lax.ppermute(even, "gx", neighbours(0))
    odd = lax.ppermute(odd, "gx", neighbours(1))
    partner = lax.ppermute(own, "gz", across)
    partner_view = lax.ppermute(own_view, "gz", across)

    taps = up8(s.extent)
    psf_shape = (1,) + psf_stack.shape[1:]
    kernel_planes = (s.extent, s.length // 2, s.cols)
    re, im = call(
        functools.partial(kernel_spectrum, s),
        (in_hbm(psf_stack), in_hbm(t["y_kernel"]), in_hbm(t["x_kernel"])),
        [kernel_planes] * 2,
        scratch=[((s.extent + 1) // 2 * 2 * taps, s.cols)] * 2 + [psf_shape],
        narrow=[t["y_kernel"].shape, t["x_kernel"].shape],
        copies=[pltpu.SemaphoreType.DMA((3,))],
        prefetch=(view_index,),
        where=pltpu.HBM,
    )
    own_rows = (s.depth // s.q_wide + s.depth // s.q_near) * s.rows
    (own_slab,) = call(functools.partial(pack_own, s), (own, partner, own_view, partner_view, re), [(own_rows, s.cols)])
    own_slab = lax.ppermute(own_slab, ("gy", "gz"), to_side())
    even, _ = lax.optimization_barrier((even, re))
    even2 = lax.ppermute(even, "gz", across)
    odd, _ = lax.optimization_barrier((odd, even2))
    odd2 = lax.ppermute(odd, "gz", across)
    halo_rows = s.depth // s.q_wide * 2 * s.wide + s.depth // s.q_near * 2 * s.near
    e_halo, v_halo, halo_slab_here = call(
        functools.partial(pack_halo, s),
        (even, odd, even2, odd2),
        [(s.depth, 2 * s.wide, s.cols), (s.depth, 2 * s.near, s.cols), (halo_rows, s.cols)],
    )
    halo_slab = lax.ppermute(halo_slab_here, ("gy", "gz"), to_side())
    k, ks, kd = call(
        functools.partial(kernel_leaves, s),
        (re, im, halo_slab_here),
        [(9 * (s.depth // 2 - 1), s.length // 2, s.cols)] * 3,
    )
    view_window = (s.depth, s.view_rows, s.cols)
    along_x, v_window = call(
        functools.partial(along_x_kernel, s),
        (own, partner, e_halo, t["x_window"], own_view, partner_view, v_halo),
        [(s.depth, s.length, s.cols), view_window],
    )

    u_rows = s.planes * s.rows
    out_rows = u_rows
    level_shapes = []
    planes, rows, columns = s.depth, s.rows, s.cols
    for _ in range(4):
        planes, rows, columns = planes // 2, rows // 2, columns // 2
        level_shapes.append((max(planes // 2, 1), rows, columns))
        out_rows += up8(level_shapes[-1][0] * rows)
    devices = 2 * gx * gy
    five_shape = (rows // 2 * gx, columns // 2 * gy)
    spectra = [(s.depth, s.length // 2, s.cols)] * 4
    halves = [(s.depth, s.length, 2 * s.cols), (s.depth, 2 * s.length, s.cols)]
    shared = (k, ks, kd, t["y_forward"], t["y_inverse"])
    (blurred,) = call(
        functools.partial(first_kernel, s),
        (along_x, own_slab, halo_slab) + shared + (t["x_window"], t["x_back_near"]),
        [view_window],
        scratch=spectra,
        narrow=halves,
        mib=24,
        flops=10**8,
    )
    mine, theirs, five = call(
        functools.partial(second_kernel, s),
        (blurred, own, partner, v_window, own_slab, halo_slab) + shared + (t["x_near"], t["x_back_own"]),
        [(out_rows, s.cols), (out_rows, s.cols), (devices, 1, five_shape[0] * five_shape[1])],
        scratch=spectra + [(s.depth, s.rows, s.cols), (4, s.depth // 2, s.rows, s.cols)],
        narrow=[(s.depth, 2 * s.view_rows, s.cols)] + halves,
        mib=24,
    )
    got = lax.ppermute(theirs, "gz", across)
    fives = lax.all_to_all(five, ALL, split_axis=0, concat_axis=0, tiled=True)
    return tuple(
        call(
            functools.partial(last_kernel, s),
            (mine, got, fives),
            [estimate.shape] + level_shapes + [(1,) + five_shape],
            mib=8,
        )
    )


def solution(mesh):
    return jax.shard_map(
        local,
        mesh=mesh,
        in_specs=(P("gz", "gx", "gy"), P("gz", "gx", "gy"), P(), P()),
        out_specs=(
            P("gz", "gx", "gy"),
            P("gz", "gx", "gy"),
            P("gz", "gx", "gy"),
            P("gz", "gx", "gy"),
            P(None, "gx", "gy"),
            P(),
        ),
        check_vma=False,
    )
```
